32 devices in a mesh: dap: 4 (over z), dp: 8 (over y, x, core).
Axes of the slice: x: 2, y: 2, z: 4, core: 2. Of those that a mesh axis runs over, the one named last changes fastest.
Arguments:
- pair_z: bfloat16 [24, 96, 96, 128], P('dp', 'dap')
- single_s: bfloat16 [24, 96, 384], P('dp', 'dap')
- token_mask: int32 [24, 96], P('dp')
- dz_out: bfloat16 [24, 96, 96, 128], P('dp', 'dap')
- ds_out: bfloat16 [24, 96, 384], P('dp', 'dap')
- w_pa: bfloat16 [128, 512], replicated
- w_pb: bfloat16 [128, 512], replicated
- w_po: bfloat16 [512, 128], replicated
- w_bias: bfloat16 [128, 16], replicated
- w_q: bfloat16 [384, 384], replicated
- q_bias: bfloat16 [384], replicated
- w_kv: bfloat16 [384, 768], replicated
- w_g: bfloat16 [384, 384], replicated
- w_o: bfloat16 [384, 384], replicated
- w_sa: bfloat16 [384, 1536], replicated
- w_sb: bfloat16 [384, 1536], replicated
- w_so: bfloat16 [1536, 384], replicated
Outputs:
- output 1: bfloat16 [24, 96, 96, 128], P('dp', 'dap')
- output 2: bfloat16 [24, 96, 384], P('dp', 'dap')
- output 3: float32 [128, 512], replicated
- output 4: float32 [128, 512], replicated
- output 5: float32 [512, 128], replicated
- output 6: float32 [128, 16], replicated
- output 7: float32 [384, 384], replicated
- output 8: float32 [384], replicated
- output 9: float32 [384, 768], replicated
- output 10: float32 [384, 384], replicated
- output 11: float32 [384, 384], replicated
- output 12: float32 [384, 1536], replicated
- output 13: float32 [384, 1536], replicated
- output 14: float32 [1536, 384], replicated
All inputs are finite; a program needn't handle non-finite values.
Results may differ from the reference program's by a relative error of at most 0.0175686.
Values are sent between devices in bfloat16 or wider.
A program may use at most 1 GiB of HBM per device.

```python
import jax
import jax.numpy as jnp
from jax import lax

C_S = 384
C_Z = 128
HEADS = 16
HEAD = 24
TRANS = 4
TOKENS = 96
COMPLEXES = 24


def snap_bf16(values):
    return values + lax.stop_gradient(values.astype(jnp.bfloat16).astype(jnp.float32) - values)


def layer_norm(values):
    centred = values - jnp.mean(values, axis=-1, keepdims=True)
    return centred * lax.rsqrt(jnp.mean(centred * centred, axis=-1, keepdims=True) + 1e-5)


def pair_rows(z_rows, w_pa, w_pb, w_po):
    normed = snap_bf16(layer_norm(z_rows))
    hid_a = jnp.einsum('rjc,cf->rjf', normed, w_pa)
    hid_b = jnp.einsum('rjc,cf->rjf', normed, w_pb)
    hidden = snap_bf16(jax.nn.silu(hid_a) * hid_b)
    return snap_bf16(z_rows + jnp.einsum('rjf,fc->rjc', hidden, w_po))


def block_forward(pair_z, single_s, mask_row, w_pa, w_pb, w_po, w_bias, w_q, q_bias, w_kv, w_g, w_o, w_sa, w_sb, w_so):
    attn_width = HEADS * HEAD
    checked_rows = jax.checkpoint(pair_rows)

    def row_step(z_rows):
        return checked_rows(z_rows, w_pa, w_pb, w_po)

    z_new = lax.map(row_step, pair_z.reshape(TOKENS // 16, 16, TOKENS, C_Z)).reshape(TOKENS, TOKENS, C_Z)
    pair_bias = jnp.einsum('ijc,ch->hij', snap_bf16(layer_norm(z_new)), w_bias)
    act_norm = snap_bf16(layer_norm(single_s))
    queries = snap_bf16(jnp.dot(act_norm, w_q, preferred_element_type=jnp.float32) + q_bias).reshape(TOKENS, HEADS, HEAD)
    key_val = snap_bf16(jnp.dot(act_norm, w_kv, preferred_element_type=jnp.float32))
    key_heads = key_val[:, :attn_width].reshape(TOKENS, HEADS, HEAD)
    value_heads = key_val[:, attn_width:].reshape(TOKENS, HEADS, HEAD)
    gate_vals = jax.nn.sigmoid(jnp.dot(act_norm, w_g, preferred_element_type=jnp.float32))
    key_mask = 1e9 * (mask_row.astype(jnp.float32) - 1.0)
    logits = jnp.einsum('ihd,jhd->hij', queries, key_heads) * (HEAD ** -0.5) + pair_bias + key_mask[None, None, :]
    attn_prob = snap_bf16(jax.nn.softmax(logits, axis=-1))
    attended = jnp.einsum('hij,jhd->ihd', attn_prob, value_heads).reshape(TOKENS, attn_width)
    gated = snap_bf16(gate_vals * attended)
    s_mid = snap_bf16(single_s + jnp.dot(gated, w_o, preferred_element_type=jnp.float32))
    mid_act = snap_bf16(layer_norm(s_mid))
    trans_a = jnp.dot(mid_act, w_sa, preferred_element_type=jnp.float32)
    trans_b = jnp.dot(mid_act, w_sb, preferred_element_type=jnp.float32)
    trans_hidden = snap_bf16(jax.nn.silu(trans_a) * trans_b)
    return z_new, s_mid + jnp.dot(trans_hidden, w_so, preferred_element_type=jnp.float32)


def draw_mask(mask_key):
    len_key, full_key = jax.random.split(mask_key)
    lengths = jax.random.randint(len_key, (COMPLEXES,), TOKENS // 4, TOKENS + 1)
    full_at = jax.random.randint(full_key, (), 0, COMPLEXES)
    lengths = jnp.where(jnp.arange(COMPLEXES) == full_at, TOKENS, lengths)
    return (jnp.arange(TOKENS)[None, :] < lengths[:, None]).astype(jnp.int32)


def setup_inputs(seed: int = 0) -> dict:
    sub_keys = jax.random.split(jax.random.key(seed), 17)
    attn_width = HEADS * HEAD

    def draw_normal(key_index, arr_shape, std_scale):
        return (jax.random.normal(sub_keys[key_index], arr_shape, jnp.float32) * std_scale).astype(jnp.bfloat16)

    return {
        'pair_z': draw_normal(0, (COMPLEXES, TOKENS, TOKENS, C_Z), 1.0),
        'single_s': draw_normal(1, (COMPLEXES, TOKENS, C_S), 1.0),
        'token_mask': draw_mask(sub_keys[2]),
        'dz_out': draw_normal(3, (COMPLEXES, TOKENS, TOKENS, C_Z), 1.0),
        'ds_out': draw_normal(4, (COMPLEXES, TOKENS, C_S), 1.0),
        'w_pa': draw_normal(5, (C_Z, TRANS * C_Z), C_Z ** -0.5),
        'w_pb': draw_normal(6, (C_Z, TRANS * C_Z), C_Z ** -0.5),
        'w_po': draw_normal(7, (TRANS * C_Z, C_Z), (TRANS * C_Z) ** -0.5),
        'w_bias': draw_normal(8, (C_Z, HEADS), C_Z ** -0.5),
        'w_q': draw_normal(9, (C_S, attn_width), C_S ** -0.5),
        'q_bias': draw_normal(10, (attn_width,), 0.5),
        'w_kv': draw_normal(11, (C_S, 2 * attn_width), C_S ** -0.5),
        'w_g': draw_normal(12, (C_S, attn_width), C_S ** -0.5),
        'w_o': draw_normal(13, (attn_width, C_S), attn_width ** -0.5),
        'w_sa': draw_normal(14, (C_S, TRANS * C_S), C_S ** -0.5),
        'w_sb': draw_normal(15, (C_S, TRANS * C_S), C_S ** -0.5),
        'w_so': draw_normal(16, (TRANS * C_S, C_S), (TRANS * C_S) ** -0.5),
    }


def reference(pair_z, single_s, token_mask, dz_out, ds_out, w_pa, w_pb, w_po, w_bias, w_q, q_bias, w_kv, w_g, w_o, w_sa, w_sb, w_so):
    weights = tuple(weight.astype(jnp.float32) for weight in (w_pa, w_pb, w_po, w_bias, w_q, q_bias, w_kv, w_g, w_o, w_sa, w_sb, w_so))

    def scan_step(running, per_complex):
        z_one, s_one, mask_one, dz_one, ds_one = per_complex

        def run_block(z_in, s_in, *params):
            return block_forward(z_in, s_in, mask_one, *params)

        _, pullback = jax.vjp(run_block, z_one.astype(jnp.float32), s_one.astype(jnp.float32), *weights)
        all_grads = pullback((dz_one.astype(jnp.float32), ds_one.astype(jnp.float32)))
        summed = tuple(acc_sum + update for acc_sum, update in zip(running, all_grads[2:]))
        return summed, (all_grads[0].astype(jnp.bfloat16), all_grads[1].astype(jnp.bfloat16))

    zero_sums = tuple(jnp.zeros_like(weight) for weight in weights)
    grad_sums, (dz_in, ds_in) = lax.scan(scan_step, zero_sums, (pair_z, single_s, token_mask, dz_out, ds_out))
    return (dz_in, ds_in, grad_sums[0], grad_sums[1], grad_sums[2], grad_sums[3], grad_sums[4], grad_sums[5], grad_sums[6], grad_sums[7], grad_sums[8], grad_sums[9], grad_sums[10], grad_sums[11])
```

```python
import jax
import jax.numpy as jnp
from jax import lax
from jax.experimental import pallas as pl
from jax.experimental.pallas import tpu as pltpu
from jax.sharding import PartitionSpec as P

HEAD_DIM = 24
HEADS = 16
WIDTH = 384
TRANS_S = 1536
PAIR = 128
TRANS_P = 512
TOKENS = 96
ROWS = 24
CPLX = 3
ALL_ROWS = CPLX * ROWS
SCALE = HEAD_DIM ** -0.5
EPSILON = 1e-5
MASK_BIG = 1e9
PEERS = 4
MESH_ID = pl.DeviceIdType.MESH
BF = jnp.bfloat16
F32 = jnp.float32

SLOTS = {
    'so': (0, 1536, 384), 'sa': (288, 384, 1536), 'sb': (576, 384, 1536), 'o': (864, 384, 384),
    'q': (936, 384, 384), 'g': (1008, 384, 384), 'qb': (1080, 16, 128), 'kv': (1088, 384, 768),
    'pa': (1280, 128, 512), 'pb': (1312, 128, 512), 'po': (1344, 512, 128), 'bias': (1376, 16, 128),
}
CHUNKS = ((0, 320), (320, 256), (576, 256), (832, 256), (1088, 192), (1280, 128))
KV_CHUNK, PAIR_CHUNK = 4, 5
TILES = 1408
BLOCK_I = 8
NUM_BLOCKS = ALL_ROWS // BLOCK_I
SEMS_PER_PART = 12


def dot_nn(left, right):
    return lax.dot_general(left, right, (((1,), (0,)), ((), ())), preferred_element_type=F32)


def dot_nt(left, right):
    return lax.dot_general(left, right, (((1,), (1,)), ((), ())), preferred_element_type=F32)


def dot_tn(left, right):
    return lax.dot_general(left, right, (((0,), (0,)), ((), ())), preferred_element_type=F32)


def layer_norm(wide):
    centred = wide - jnp.mean(wide, axis=-1, keepdims=True)
    inv_std = lax.rsqrt(jnp.mean(centred * centred, axis=-1, keepdims=True) + EPSILON)
    return centred * inv_std, inv_std


def norm_grad(normed, inv_std, grad_out):
    mean_grad = jnp.mean(grad_out, axis=-1, keepdims=True)
    mean_proj = jnp.mean(grad_out * normed, axis=-1, keepdims=True)
    return inv_std * (grad_out - mean_grad - normed * mean_proj)


def sigmoid(values):
    return 0.5 * jnp.tanh(0.5 * values) + 0.5


def swiglu_grad(hid_a, hid_b, grad_hidden):
    sig_a = sigmoid(hid_a)
    silu_a = hid_a * sig_a
    grad_a = (grad_hidden * hid_b) * (sig_a + silu_a * (1.0 - sig_a))
    return silu_a * hid_b, grad_a, grad_hidden * silu_a


def put_tiles(grads, name, value, first_col=0):
    base, rows, _ = SLOTS[name]
    per_col = rows // 16
    for col in range(value.shape[1] // 128):
        start = base + (first_col // 128 + col) * per_col
        piece = value[:, col * 128:(col + 1) * 128]
        grads[start:start + per_col] = piece.reshape(per_col, 16, 128).astype(BF)


class Reducer:
    def __init__(self, span, sem_base, refs, place):
        self.base, self.count = span
        self.grads, self.total, self.got1, self.got2, self.got3, self.gotz, self.send_sem, self.recv_sem = refs
        self.place = place
        self.sem_base = sem_base

    def geometry(self, part):
        place = self.place
        half = self.count // 2
        sizes = (half // 2, half // 4, half // 8, half // 32)
        bits = (place['core'], place['x'], place['y']) if part == 0 else (place['core'], place['y'], place['x'])
        names = ('core', 'x', 'y') if part == 0 else ('core', 'y', 'x')
        return self.base + part * half, sizes, bits, names

    def copy(self, part, index):
        first, sizes, bits, names = self.geometry(part)
        peer = self.place['peer']
        my_z = self.place['z']
        keep0 = first + bits[0] * sizes[0]
        keep1 = keep0 + bits[1] * sizes[1]
        keep2 = keep1 + bits[2] * sizes[2]
        keep3 = keep2 + my_z * sizes[3]
        got1, got2, got3 = self.got1.at[part], self.got2.at[part], self.got3.at[part]
        if index == 0:
            src, dst = self.grads.at[pl.ds(first + (1 - bits[0]) * sizes[0], sizes[0])], got1
            device = peer[names[0]]
        elif index == 1:
            src, dst = got1.at[pl.ds((1 - bits[1]) * sizes[1], sizes[1])], got2
            device = peer[names[1]]
        elif index == 2:
            src, dst = got2.at[pl.ds((1 - bits[2]) * sizes[2], sizes[2])], got3
            device = peer[names[2]]
        elif index <= 5:
            other = lax.rem(my_z + index - 2, PEERS)
            src, dst = got3.at[pl.ds(other * sizes[3], sizes[3])], self.gotz.at[part, index - 3]
            device = self.place['z_peer'](other)
        elif index <= 8:
            src = dst = self.total.at[pl.ds(keep3, sizes[3])]
            device = self.place['z_peer'](lax.rem(my_z + index - 5, PEERS))
        else:
            level = 11 - index
            src = dst = self.total.at[pl.ds((keep0, keep1, keep2)[level], sizes[level])]
            device = peer[names[level]]
        slot = self.sem_base + part * SEMS_PER_PART + index
        return pltpu.make_async_remote_copy(
            src_ref=src, dst_ref=dst, send_sem=self.send_sem.at[slot], recv_sem=self.recv_sem.at[slot],
            device_id=device, device_id_type=MESH_ID)

    def advance(self, stage):
        for part in range(2):
            self.step(part, stage)

    def step(self, part, stage):
        first, sizes, bits, _ = self.geometry(part)
        got1, got2, got3 = self.got1.at[part], self.got2.at[part], self.got3.at[part]
        keep0 = first + bits[0] * sizes[0]
        my_z = self.place['z']
        waits = ((), (0,), (1,), (2,), (3, 4, 5), (6, 7, 8), (9,), (10,), (11,))[stage]
        begins = ((0,), (1,), (2,), (3, 4, 5), (6, 7, 8), (9,), (10,), (11,), ())[stage]
        for index in waits:
            self.copy(part, index).wait()
        if stage == 1:
            add_into(got1, self.grads, keep0, sizes[0])
        elif stage == 2:
            add_into(got2, got1, bits[1] * sizes[1], sizes[1])
        elif stage == 3:
            add_into(got3, got2, bits[2] * sizes[2], sizes[2])
        elif stage == 4:
            mine = got3[pl.ds(my_z * sizes[3], sizes[3])].astype(F32)
            for slot in range(PEERS - 1):
                mine = mine + self.gotz[part, slot].astype(F32)
            keep3 = keep0 + bits[1] * sizes[1] + bits[2] * sizes[2] + my_z * sizes[3]
            self.total[pl.ds(keep3, sizes[3])] = mine.astype(BF)
        for index in begins:
            self.copy(part, index).start()


def add_into(dst, src, src_start, count):
    step = 8 if count % 8 == 0 else count

    @pl.loop(0, count // step)
    def _(index):
        at = index * step
        left = dst[pl.ds(at, step)].astype(F32)
        right = src[pl.ds(src_start + at, step)].astype(F32)
        dst[pl.ds(at, step)] = (left + right).astype(BF)


def main_kernel(*refs):
    names = ('pair_z', 'single_s', 'token_mask', 'dz_out', 'ds_out', 'w_pa', 'w_pb', 'w_po', 'w_bias', 'w_q', 'q_bias',
             'w_kv', 'w_g', 'w_o', 'w_sa', 'w_sb', 'w_so')
    hbm = dict(zip(names, refs[:17]))
    dz_in, ds_in, total_out = refs[17:20]
    scratch = refs[20:]
    loaded = dict(zip(names, scratch[:17]))
    (new_rows, bias_rows, grad_bias, kv_buf, gkv_buf, gkv_got, acc_ab, acc_po, acc_bias, wb_t, act_s, norm_s, gq_s, ggp_s,
     gmid_s, inv_s, prob_s, qexp_s, dz_stage, ds_stage, grads, total) = scratch[17:39]
    reduce_refs = scratch[39:39 + 4 * len(CHUNKS)]
    load_sem, kv_send, kv_recv, gkv_send, gkv_recv, ar_send, ar_recv, out_sem, tot_sem = scratch[39 + 4 * len(CHUNKS):]

    order = ('single_s', 'w_kv', 'pair_z', 'w_pa', 'w_pb', 'w_po', 'w_bias', 'w_q', 'q_bias', 'w_g', 'token_mask', 'w_o', 'w_sa',
             'w_sb', 'ds_out', 'w_so', 'dz_out')
    loads = {}
    for index, name in enumerate(order):
        loads[name] = pltpu.make_async_copy(hbm[name], loaded[name], load_sem.at[index])
        loads[name].start()

    my_z = lax.axis_index('dap')
    my_dp = lax.axis_index('dp')
    core = lax.rem(my_dp, 2)
    bit_x = lax.rem(lax.div(my_dp, 2), 2)
    bit_y = lax.div(my_dp, 4)

    def z_peer(other):
        return (other, my_dp)

    peer = {'core': (my_z, my_dp + 1 - 2 * core), 'x': (my_z, my_dp + 2 - 4 * bit_x), 'y': (my_z, my_dp + 4 - 8 * bit_y)}
    place = {'core': core, 'x': bit_x, 'y': bit_y, 'z': my_z, 'peer': peer, 'z_peer': z_peer}

    barrier = pltpu.get_barrier_semaphore()
    for device in list(peer.values()) + [z_peer(lax.rem(my_z + hop, PEERS)) for hop in range(1, PEERS)]:
        pl.semaphore_signal(barrier, inc=1, device_id=device, device_id_type=MESH_ID)
    pl.semaphore_wait(barrier, 6)

    loads['single_s'].wait()
    loads['w_kv'].wait()
    s_wide = loaded['single_s'][...].astype(F32).reshape(ALL_ROWS, WIDTH)
    s_norm, s_inv = layer_norm(s_wide)
    act = s_norm.astype(BF)
    act_s[...] = act
    norm_s[...] = s_norm
    inv_s[...] = s_inv
    kv_local = dot_nn(act, loaded['w_kv'][...])
    kv_buf[my_z] = kv_local.reshape(CPLX, ROWS, 2 * WIDTH).astype(BF)

    def kv_copy(hop):
        return pltpu.make_async_remote_copy(
            src_ref=kv_buf.at[my_z], dst_ref=kv_buf.at[my_z], send_sem=kv_send.at[hop - 1], recv_sem=kv_recv.at[hop - 1],
            device_id=z_peer(lax.rem(my_z + hop, PEERS)), device_id_type=MESH_ID)

    for hop in range(1, PEERS):
        kv_copy(hop).start()

    for name in ('pair_z', 'w_pa', 'w_pb', 'w_po', 'w_bias'):
        loads[name].wait()
    wb_t[...] = jnp.transpose(loaded['w_bias'][...].astype(F32)).astype(BF)
    block_rows = BLOCK_I * TOKENS

    @pl.loop(0, NUM_BLOCKS)
    def _(block):
        at = block * BLOCK_I
        z_wide = loaded['pair_z'][pl.ds(at, BLOCK_I)].reshape(block_rows, PAIR).astype(F32)
        normed, _ = layer_norm(z_wide)
        normed_bf = normed.astype(BF)
        hid_a = dot_nn(normed_bf, loaded['w_pa'][...])
        hid_b = dot_nn(normed_bf, loaded['w_pb'][...])
        hidden = (hid_a * sigmoid(hid_a) * hid_b).astype(BF)
        z_new = (z_wide + dot_nn(hidden, loaded['w_po'][...])).astype(BF)
        new_rows[pl.ds(at, BLOCK_I)] = z_new.reshape(BLOCK_I, TOKENS, PAIR)
        bias_norm, _ = layer_norm(z_new.astype(F32))
        bias_bf = bias_norm.astype(BF)
        for row in range(BLOCK_I):
            bias_rows[at + row] = dot_nt(wb_t[...], bias_bf[row * TOKENS:(row + 1) * TOKENS])

    for name in ('w_q', 'q_bias', 'w_g', 'token_mask', 'w_o', 'w_sa', 'w_sb', 'ds_out', 'w_so'):
        loads[name].wait()
    queries = (dot_nn(act_s[...], loaded['w_q'][...]) + loaded['q_bias'][...].astype(F32)).astype(BF).astype(F32)
    gate = sigmoid(dot_nn(act_s[...], loaded['w_g'][...]))
    lane_head = lax.broadcasted_iota(jnp.int32, (HEADS, WIDTH), 1)
    row_head = lax.broadcasted_iota(jnp.int32, (HEADS, WIDTH), 0)
    head_mask = jnp.where((lane_head >= row_head * HEAD_DIM) & (lane_head < (row_head + 1) * HEAD_DIM), 1.0, 0.0).astype(F32)

    def spread(rows):
        wide = jnp.broadcast_to(rows.reshape(ROWS, 1, WIDTH), (ROWS, HEADS, WIDTH)) * head_mask[None]
        return wide.reshape(ROWS * HEADS, WIDTH).astype(BF)

    def gather_heads(wide):
        return jnp.sum(wide.reshape(ROWS, HEADS, WIDTH) * head_mask[None], axis=1)

    for hop in range(1, PEERS):
        kv_copy(hop).wait()

    def keys_values(cplx):
        both = kv_buf[:, cplx].astype(F32).reshape(TOKENS, 2 * WIDTH).astype(BF)
        return both[:, :WIDTH], both[:, WIDTH:]

    key_mask = MASK_BIG * (loaded['token_mask'][...].astype(F32) - 1.0)
    attended_parts = []
    for cplx in range(CPLX):
        keys, values = keys_values(cplx)
        q_exp = spread(queries[cplx * ROWS:(cplx + 1) * ROWS])
        qexp_s[cplx] = q_exp
        bias = bias_rows[cplx * ROWS:(cplx + 1) * ROWS].reshape(ROWS * HEADS, TOKENS)
        logits = dot_nt(q_exp, keys) * SCALE + bias + key_mask[cplx:cplx + 1]
        top = jnp.max(logits, axis=-1, keepdims=True)
        expd = jnp.exp(logits - top)
        prob = expd / jnp.sum(expd, axis=-1, keepdims=True)
        prob_s[cplx] = prob
        attended_parts.append(gather_heads(dot_nn(prob.astype(BF), values)))
    attended = jnp.concatenate(attended_parts, axis=0)
    gated = (gate * attended).astype(BF)
    s_mid = (s_wide + dot_nn(gated, loaded['w_o'][...])).astype(BF)
    mid_norm, mid_inv = layer_norm(s_mid.astype(F32))
    mid_act = mid_norm.astype(BF)

    reducers = []
    for index, span in enumerate(CHUNKS):
        refs_here = (grads, total) + tuple(reduce_refs[4 * index:4 * index + 4]) + (ar_send, ar_recv)
        reducers.append(Reducer(span, index * 2 * SEMS_PER_PART, refs_here, place))

    ds_wide = loaded['ds_out'][...].astype(F32).reshape(ALL_ROWS, WIDTH)
    ds_bf = ds_wide.astype(BF)
    grad_mid_norm = jnp.zeros((ALL_ROWS, WIDTH), F32)
    piece = 512
    for col in range(0, TRANS_S, piece):
        cols = slice(col, col + piece)
        trans_a = dot_nn(mid_act, loaded['w_sa'][:, cols])
        trans_b = dot_nn(mid_act, loaded['w_sb'][:, cols])
        grad_hidden = dot_nt(ds_bf, loaded['w_so'][cols, :])
        hidden, grad_ta, grad_tb = swiglu_grad(trans_a, trans_b, grad_hidden)
        grad_ta = grad_ta.astype(BF)
        grad_tb = grad_tb.astype(BF)
        d_so = dot_tn(hidden.astype(BF), ds_bf)
        for sub in range(WIDTH // 128):
            start = SLOTS['so'][0] + sub * (TRANS_S // 16) + col // 16
            grads[start:start + piece // 16] = d_so[:, sub * 128:(sub + 1) * 128].reshape(piece // 16, 16, 128).astype(BF)
        put_tiles(grads, 'sa', dot_tn(mid_act, grad_ta), col)
        put_tiles(grads, 'sb', dot_tn(mid_act, grad_tb), col)
        grad_mid_norm = grad_mid_norm + dot_nt(grad_ta, loaded['w_sa'][:, cols]) + dot_nt(grad_tb, loaded['w_sb'][:, cols])
    reducers[0].advance(0)
    reducers[1].advance(0)
    grad_mid = ds_wide + norm_grad(mid_norm, mid_inv, grad_mid_norm)
    gmid_s[...] = grad_mid
    grad_mid_bf = grad_mid.astype(BF)
    put_tiles(grads, 'o', dot_tn(gated, grad_mid_bf))
    grad_gated = dot_nt(grad_mid_bf, loaded['w_o'][...])
    grad_gate_pre = (grad_gated * attended * gate * (1.0 - gate)).astype(BF)
    ggp_s[...] = grad_gate_pre
    grad_att = (grad_gated * gate).astype(BF).astype(F32)
    grad_query_parts = []
    for cplx in range(CPLX):
        keys, values = keys_values(cplx)
        ga_exp = spread(grad_att[cplx * ROWS:(cplx + 1) * ROWS])
        prob = prob_s[cplx]
        grad_prob = dot_nt(ga_exp, values)
        grad_values = dot_tn(prob.astype(BF), ga_exp)
        grad_logits = (prob * (grad_prob - jnp.sum(prob * grad_prob, axis=-1, keepdims=True))).astype(BF)
        grad_bias[cplx * ROWS:(cplx + 1) * ROWS] = grad_logits.reshape(ROWS, HEADS, TOKENS)
        grad_query_parts.append(gather_heads(dot_nn(grad_logits, keys)) * SCALE)
        grad_keys = dot_tn(grad_logits, qexp_s[cplx]) * SCALE
        gkv_buf[:, cplx, :, :WIDTH] = grad_keys.reshape(PEERS, ROWS, WIDTH).astype(BF)
        gkv_buf[:, cplx, :, WIDTH:] = grad_values.reshape(PEERS, ROWS, WIDTH).astype(BF)

    def gkv_copy(hop):
        other = lax.rem(my_z + hop, PEERS)
        return pltpu.make_async_remote_copy(
            src_ref=gkv_buf.at[other], dst_ref=gkv_got.at[hop - 1], send_sem=gkv_send.at[hop - 1],
            recv_sem=gkv_recv.at[hop - 1], device_id=z_peer(other), device_id_type=MESH_ID)

    for hop in range(1, PEERS):
        gkv_copy(hop).start()
    reducers[0].advance(1)
    grad_query = jnp.concatenate(grad_query_parts, axis=0)
    grad_query_bf = grad_query.astype(BF)
    gq_s[...] = grad_query_bf
    put_tiles(grads, 'q', dot_tn(act_s[...], grad_query_bf))
    put_tiles(grads, 'g', dot_tn(act_s[...], grad_gate_pre))
    d_q_bias = jnp.sum(grad_query, axis=0, keepdims=True)
    row_index = lax.broadcasted_iota(jnp.int32, (16, 128), 0)
    bias_tile = jnp.zeros((16, 128), F32)
    for sub in range(3):
        bias_tile = jnp.where(row_index == sub, jnp.broadcast_to(d_q_bias[:, sub * 128:(sub + 1) * 128], (16, 128)), bias_tile)
    grads[1080] = bias_tile.astype(BF)
    grads[1081:1088] = jnp.zeros((7, 16, 128), BF)
    grads[1232:1280] = jnp.zeros((48, 16, 128), BF)
    grads[1377:1408] = jnp.zeros((31, 16, 128), BF)

    def finish_single():
        for hop in range(1, PEERS):
            gkv_copy(hop).wait()
        summed = gkv_buf[my_z].astype(F32)
        for hop in range(1, PEERS):
            summed = summed + gkv_got[hop - 1].astype(F32)
        grad_kv = summed.reshape(ALL_ROWS, 2 * WIDTH).astype(BF)
        put_tiles(grads, 'kv', dot_tn(act_s[...], grad_kv))
        grad_act = (dot_nt(gq_s[...], loaded['w_q'][...]) + dot_nt(grad_kv, loaded['w_kv'][...])
                    + dot_nt(ggp_s[...], loaded['w_g'][...]))
        grad_s = gmid_s[...] + norm_grad(norm_s[...], inv_s[...], grad_act)
        ds_stage[...] = grad_s.reshape(CPLX, ROWS, WIDTH).astype(BF)
        pltpu.make_async_copy(ds_stage, ds_in, out_sem.at[2]).start()

    ticks = []
    starts = {0: -2, 1: -1, 2: 0, 3: 1, 4: 3}
    for tick in range(12):
        todo = []
        for index, start in starts.items():
            stage = tick - start
            if 0 <= stage <= 8 and not (index == 1 and stage == 0):
                todo.append((index, stage))
        ticks.append(todo)

    def run_tick(tick):
        if tick == starts[KV_CHUNK]:
            finish_single()
        for index, stage in ticks[tick]:
            reducers[index].advance(stage)

    loads['dz_out'].wait()
    acc_ab[...] = jnp.zeros_like(acc_ab)
    acc_po[...] = jnp.zeros_like(acc_po)
    acc_bias[...] = jnp.zeros_like(acc_bias)

    @pl.loop(0, NUM_BLOCKS)
    def _(block):
        for tick in range(NUM_BLOCKS):
            @pl.when(block == tick)
            def _():
                run_tick(tick)
        at = block * BLOCK_I
        bias_norm, bias_inv = layer_norm(new_rows[pl.ds(at, BLOCK_I)].reshape(block_rows, PAIR).astype(F32))
        bias_bf = bias_norm.astype(BF)
        bias_acc = acc_bias[...]
        parts = []
        for row in range(BLOCK_I):
            grad_row = grad_bias[at + row]
            bias_acc = bias_acc + dot_nn(grad_row, bias_bf[row * TOKENS:(row + 1) * TOKENS])
            parts.append(dot_tn(grad_row, wb_t[...]))
        acc_bias[...] = bias_acc
        grad_norm = jnp.concatenate(parts, axis=0)
        dz_wide = loaded['dz_out'][pl.ds(at, BLOCK_I)].reshape(block_rows, PAIR).astype(F32)
        grad_new = dz_wide + norm_grad(bias_norm, bias_inv, grad_norm)
        grad_new_bf = grad_new.astype(BF)
        normed, inv_std = layer_norm(loaded['pair_z'][pl.ds(at, BLOCK_I)].reshape(block_rows, PAIR).astype(F32))
        normed_bf = normed.astype(BF)
        hid_a = dot_nn(normed_bf, loaded['w_pa'][...])
        hid_b = dot_nn(normed_bf, loaded['w_pb'][...])
        grad_hidden = dot_nt(grad_new_bf, loaded['w_po'][...])
        hidden, grad_a, grad_b = swiglu_grad(hid_a, hid_b, grad_hidden)
        grad_a = grad_a.astype(BF)
        grad_b = grad_b.astype(BF)
        acc_po[...] += dot_tn(grad_new_bf, hidden.astype(BF))
        acc_ab[:, :TRANS_P] += dot_tn(normed_bf, grad_a)
        acc_ab[:, TRANS_P:] += dot_tn(normed_bf, grad_b)
        grad_normed = dot_nt(grad_a, loaded['w_pa'][...]) + dot_nt(grad_b, loaded['w_pb'][...])
        result = grad_new + norm_grad(normed, inv_std, grad_normed)
        slot = lax.rem(block, 2)

        @pl.when(block >= 2)
        def _():
            pltpu.make_async_copy(dz_stage.at[slot], dz_in.at[pl.ds(0, BLOCK_I)], out_sem.at[slot]).wait()

        dz_stage[slot] = result.reshape(BLOCK_I, TOKENS, PAIR).astype(BF)
        pltpu.make_async_copy(dz_stage.at[slot], dz_in.at[pl.ds(at, BLOCK_I)], out_sem.at[slot]).start()

    put_tiles(grads, 'pa', acc_ab[:, :TRANS_P])
    put_tiles(grads, 'pb', acc_ab[:, TRANS_P:])
    put_tiles(grads, 'po', jnp.transpose(acc_po[...]))
    grads[1376] = acc_bias[...].astype(BF)
    last = reducers[PAIR_CHUNK]
    last.advance(0)
    done_tail = [index for index, start in starts.items() if start + 8 < NUM_BLOCKS]
    copies = []

    def write_out(index):
        base, count = CHUNKS[index]
        made = pltpu.make_async_copy(total.at[pl.ds(base, count)], total_out.at[pl.ds(base, count)], tot_sem.at[index])
        made.start()
        copies.append(made)

    for index in done_tail:
        write_out(index)
    for tick in range(NUM_BLOCKS, 12):
        run_tick(tick)
        for index, start in starts.items():
            if start + 8 == tick:
                write_out(index)
        last.advance(tick - NUM_BLOCKS + 1)
    for stage in range(12 - NUM_BLOCKS + 1, 9):
        last.advance(stage)
    write_out(PAIR_CHUNK)
    pltpu.make_async_copy(ds_stage, ds_in, out_sem.at[2]).wait()
    for slot in range(2):
        pltpu.make_async_copy(dz_stage.at[slot], dz_in.at[pl.ds(0, BLOCK_I)], out_sem.at[slot]).wait()
    for copy in copies:
        copy.wait()


def run_main(inputs):
    any_spec = pl.BlockSpec(memory_space=pl.ANY)
    scratch = [pltpu.VMEM(value.shape, value.dtype) for value in inputs]
    scratch += [
        pltpu.VMEM((ALL_ROWS, TOKENS, PAIR), BF),
        pltpu.VMEM((ALL_ROWS, HEADS, TOKENS), F32),
        pltpu.VMEM((ALL_ROWS, HEADS, TOKENS), BF),
        pltpu.VMEM((PEERS, CPLX, ROWS, 2 * WIDTH), BF),
        pltpu.VMEM((PEERS, CPLX, ROWS, 2 * WIDTH), BF),
        pltpu.VMEM((PEERS - 1, CPLX, ROWS, 2 * WIDTH), BF),
        pltpu.VMEM((PAIR, 2 * TRANS_P), F32),
        pltpu.VMEM((PAIR, TRANS_P), F32),
        pltpu.VMEM((HEADS, PAIR), F32),
        pltpu.VMEM((HEADS, PAIR), BF),
        pltpu.VMEM((ALL_ROWS, WIDTH), BF),
        pltpu.VMEM((ALL_ROWS, WIDTH), F32),
        pltpu.VMEM((ALL_ROWS, WIDTH), BF),
        pltpu.VMEM((ALL_ROWS, WIDTH), BF),
        pltpu.VMEM((ALL_ROWS, WIDTH), F32),
        pltpu.VMEM((ALL_ROWS, 1), F32),
        pltpu.VMEM((CPLX, ROWS * HEADS, TOKENS), F32),
        pltpu.VMEM((CPLX, ROWS * HEADS, WIDTH), BF),
        pltpu.VMEM((2, BLOCK_I, TOKENS, PAIR), BF),
        pltpu.VMEM((CPLX, ROWS, WIDTH), BF),
        pltpu.VMEM((TILES, 16, 128), BF),
        pltpu.VMEM((TILES, 16, 128), BF),
    ]
    for _, count in CHUNKS:
        scratch += [pltpu.VMEM((2, count // 4, 16, 128), BF), pltpu.VMEM((2, count // 8, 16, 128), BF),
                    pltpu.VMEM((2, count // 16, 16, 128), BF), pltpu.VMEM((2, PEERS - 1, count // 64, 16, 128), BF)]
    num_sems = len(CHUNKS) * 2 * SEMS_PER_PART
    dma = pltpu.SemaphoreType.DMA
    scratch += [dma((17,)), dma((3,)), dma((3,)), dma((3,)), dma((3,)), dma((num_sems,)), dma((num_sems,)), dma((3,)),
                dma((len(CHUNKS),))]
    return pl.pallas_call(
        main_kernel,
        out_shape=(jax.ShapeDtypeStruct((ALL_ROWS, TOKENS, PAIR), BF), jax.ShapeDtypeStruct((CPLX, ROWS, WIDTH), BF),
                   jax.ShapeDtypeStruct((TILES, 16, 128), BF)),
        in_specs=[any_spec] * 17,
        out_specs=(any_spec,) * 3,
        scratch_shapes=scratch,
        compiler_params=pltpu.CompilerParams(collective_id=0, has_side_effects=True, vmem_limit_bytes=62 * 1024 * 1024),
        name='pairformer_tail',
    )(*inputs)


UNPACK = ('pa', 'pb', 'po', 'bias', 'q', 'qb', 'kv', 'g', 'o', 'sa', 'sb', 'so')


def unpack_kernel(tiles, *refs):
    outs, stages, sem = refs[:12], refs[12:24], refs[24]
    copies = []
    for index in sorted(range(12), key=lambda i: SLOTS[UNPACK[i]][0]):
        name = UNPACK[index]
        base, rows, cols = SLOTS[name]
        if name == 'bias':
            stages[index][...] = jnp.transpose(tiles[base].astype(F32))
        elif name == 'qb':
            stages[index][...] = tiles[base].astype(F32)
        else:
            per_col = rows // 16
            for col in range(cols // 128):
                part = tiles[base + col * per_col:base + (col + 1) * per_col].astype(F32)
                stages[index][:, col * 128:(col + 1) * 128] = part.reshape(rows, 128)
        made = pltpu.make_async_copy(stages[index], outs[index], sem.at[index])
        made.start()
        copies.append(made)
    for copy in copies:
        copy.wait()


def run_unpack(tiles):
    shapes = []
    for name in UNPACK:
        _, rows, cols = SLOTS[name]
        shapes.append((128, 16) if name == 'bias' else (rows, cols))
    return pl.pallas_call(
        unpack_kernel,
        out_shape=tuple(jax.ShapeDtypeStruct(shape, F32) for shape in shapes),
        in_specs=[pl.BlockSpec(memory_space=pltpu.VMEM)],
        out_specs=(pl.BlockSpec(memory_space=pl.ANY),) * 12,
        scratch_shapes=[pltpu.VMEM(shape, F32) for shape in shapes] + [pltpu.SemaphoreType.DMA((12,))],
        compiler_params=pltpu.CompilerParams(vmem_limit_bytes=48 * 1024 * 1024),
        name='unpack_sums',
    )(tiles)


def solution(mesh):
    pair_spec = P('dp', 'dap', None, None)
    single_spec = P('dp', 'dap', None)

    def body(pair_z, single_s, token_mask, dz_out, ds_out, w_pa, w_pb, w_po, w_bias, w_q, q_bias, w_kv, w_g, w_o, w_sa, w_sb, w_so):
        inputs = (pair_z.reshape(ALL_ROWS, TOKENS, PAIR), single_s, token_mask, dz_out.reshape(ALL_ROWS, TOKENS, PAIR), ds_out,
                  w_pa, w_pb, w_po, w_bias, w_q, q_bias.reshape(1, WIDTH), w_kv, w_g, w_o, w_sa, w_sb, w_so)
        dz_in, ds_in, tiles = run_main(inputs)
        sums = list(run_unpack(tiles))
        sums[5] = sums[5][:3].reshape(WIDTH)
        return (dz_in.reshape(pair_z.shape), ds_in) + tuple(sums)

    in_specs = (pair_spec, single_spec, P('dp', None), pair_spec, single_spec) + (P(),) * 12
    out_specs = (pair_spec, single_spec) + (P(),) * 12
    return jax.shard_map(body, mesh=mesh, in_specs=in_specs, out_specs=out_specs, check_vma=False)
```

```python
import jax
import jax.numpy as jnp
from jax import lax
from jax.experimental import pallas as pl
from jax.experimental.pallas import tpu as pltpu
from jax.sharding import PartitionSpec as P

HEAD_DIM = 24
HEADS = 16
WIDTH = 384
TRANS_S = 1536
PAIR = 128
TRANS_P = 512
TOKENS = 96
ROWS = 24
CPLX = 3
ALL_ROWS = CPLX * ROWS
SCALE = HEAD_DIM ** -0.5
EPSILON = 1e-5
MASK_BIG = 1e9
PEERS = 4
MESH_ID = pl.DeviceIdType.MESH
BF = jnp.bfloat16
F32 = jnp.float32

PIECE = 512
PIECE_TILES = 288
SLOTS = {
    'o': (864, 384, 384),
    'q': (936, 384, 384), 'g': (1008, 384, 384), 'qb': (1080, 16, 128), 'kv': (1088, 384, 768),
    'pa': (1280, 128, 512), 'pb': (1312, 128, 512), 'po': (1344, 512, 128), 'bias': (1376, 16, 128),
}
CHUNK = 128
LOCAL_END, PAIR_START, TILES = 1088, 1280, 1408
CHUNKS = tuple((base, min(CHUNK, LOCAL_END - base)) for base in range(0, LOCAL_END, CHUNK)) + (
    (LOCAL_END, PAIR_START - LOCAL_END), (PAIR_START, TILES - PAIR_START))
KV_CHUNK, PAIR_CHUNK = len(CHUNKS) - 2, len(CHUNKS) - 1
STAGES = 8
BLOCK_I = 8
NUM_BLOCKS = ALL_ROWS // BLOCK_I
SEMS_PER_PART = 12

TILE_US = {'core': 0.0102, 'x': 0.089, 'y': 0.089, 'z': 0.089}
LATENCY_US = {'core': 1.0, 'x': 2.3, 'y': 2.3, 'z': 3.8}
SEGMENT_US = (0.7, 0.7, 0.7, 2.0, 0.4) + (2.6,) * NUM_BLOCKS
SEGMENT_TILES = (288, 576, 864, 936, LOCAL_END)
KV_SEGMENT, KV_US = 3, 13.4


def plan_actions():
    jobs = [(chunk, part) for chunk in range(len(CHUNKS)) for part in range(2)]
    stage = dict.fromkeys(jobs, 0)
    due = {}
    free = dict.fromkeys(TILE_US, 0.0)
    actions = [[] for _ in range(len(SEGMENT_US) + 1)]
    now, segment, kv_due, kv_done = 0.0, 0, None, False

    def ready(job):
        chunk = job[0]
        if stage[job] > STAGES:
            return False
        if stage[job]:
            return due[job] <= now
        if chunk == PAIR_CHUNK:
            return segment == len(SEGMENT_US)
        if chunk == KV_CHUNK:
            return kv_done
        end = sum(CHUNKS[chunk])
        return segment > next(index for index, tiles in enumerate(SEGMENT_TILES) if end <= tiles)

    while True:
        if kv_due is not None and kv_due <= now and not kv_done:
            actions[segment].append((-1, 0, 0))
            now, kv_done = now + 0.9, True
            continue
        waiting = [job for job in jobs if ready(job)]
        if waiting:
            job = min(waiting, key=lambda one: (one[0] != PAIR_CHUNK, one[0], stage[one], one[1]))
            step = stage[job]
            actions[segment].append(job + (step,))
            size = CHUNKS[job[0]][1] // 2
            sizes = (size // 2, size // 4, size // 8, size // 8)
            now += 0.03 + (0.0014 * sizes[step] if 0 < step < 4 else 0.0)
            if step < STAGES:
                level = min(step, STAGES - 1 - step)
                link = ('core', 'yx'[job[1] == 0], 'xy'[job[1] == 0], 'z')[level]
                free[link] = max(free[link], now) + sizes[level] * TILE_US[link]
                due[job] = free[link] + LATENCY_US[link]
            stage[job] = step + 1
        elif segment < len(SEGMENT_US):
            now += SEGMENT_US[segment]
            if segment == KV_SEGMENT:
                kv_due = now + KV_US
            segment += 1
        else:
            later = [due[job] for job in jobs if 0 < stage[job] <= STAGES] + [kv_due] * (not kv_done)
            if not later:
                return actions
            now = max(now, min(later))


ACTIONS = plan_actions()


def dot_nn(left, right):
    return lax.dot_general(left, right, (((1,), (0,)), ((), ())), preferred_element_type=F32)


def dot_nt(left, right):
    return lax.dot_general(left, right, (((1,), (1,)), ((), ())), preferred_element_type=F32)


def dot_tn(left, right):
    return lax.dot_general(left, right, (((0,), (0,)), ((), ())), preferred_element_type=F32)


def layer_norm(wide):
    centred = wide - jnp.mean(wide, axis=-1, keepdims=True)
    inv_std = lax.rsqrt(jnp.mean(centred * centred, axis=-1, keepdims=True) + EPSILON)
    return centred * inv_std, inv_std


def norm_grad(normed, inv_std, grad_out):
    mean_grad = jnp.mean(grad_out, axis=-1, keepdims=True)
    mean_proj = jnp.mean(grad_out * normed, axis=-1, keepdims=True)
    return inv_std * (grad_out - mean_grad - normed * mean_proj)


def sigmoid(values):
    return 0.5 * jnp.tanh(0.5 * values) + 0.5


def swiglu_grad(hid_a, hid_b, grad_hidden):
    sig_a = sigmoid(hid_a)
    silu_a = hid_a * sig_a
    grad_a = (grad_hidden * hid_b) * (sig_a + silu_a * (1.0 - sig_a))
    return silu_a * hid_b, grad_a, grad_hidden * silu_a


def put_at(grads, base, value):
    per_col = value.shape[0] // 16
    for col in range(value.shape[1] // 128):
        start = base + col * per_col
        grads[start:start + per_col] = value[:, col * 128:(col + 1) * 128].reshape(per_col, 16, 128).astype(BF)


def put_tiles(grads, name, value):
    put_at(grads, SLOTS[name][0], value)


class Reducer:
    def __init__(self, span, sem_base, refs, place):
        self.base, self.count = span
        self.grads, self.total, self.got1, self.got2, self.got3, self.gotz, self.send_sem, self.recv_sem = refs
        self.place = place
        self.sem_base = sem_base

    def geometry(self, part):
        place = self.place
        half = self.count // 2
        sizes = (half // 2, half // 4, half // 8, half // 32)
        bits = (place['core'], place['x'], place['y']) if part == 0 else (place['core'], place['y'], place['x'])
        names = ('core', 'x', 'y') if part == 0 else ('core', 'y', 'x')
        return self.base + part * half, sizes, bits, names

    def copy(self, part, index):
        first, sizes, bits, names = self.geometry(part)
        peer = self.place['peer']
        my_z = self.place['z']
        keep0 = first + bits[0] * sizes[0]
        keep1 = keep0 + bits[1] * sizes[1]
        keep2 = keep1 + bits[2] * sizes[2]
        keep3 = keep2 + my_z * sizes[3]
        got1, got2, got3 = self.got1.at[part], self.got2.at[part], self.got3.at[part]
        if index == 0:
            src, dst = self.grads.at[pl.ds(first + (1 - bits[0]) * sizes[0], sizes[0])], got1
            device = peer[names[0]]
        elif index == 1:
            src, dst = got1.at[pl.ds((1 - bits[1]) * sizes[1], sizes[1])], got2
            device = peer[names[1]]
        elif index == 2:
            src, dst = got2.at[pl.ds((1 - bits[2]) * sizes[2], sizes[2])], got3
            device = peer[names[2]]
        elif index <= 5:
            other = lax.rem(my_z + index - 2, PEERS)
            src, dst = got3.at[pl.ds(other * sizes[3], sizes[3])], self.gotz.at[part, index - 3]
            device = self.place['z_peer'](other)
        elif index <= 8:
            src = dst = self.total.at[pl.ds(keep3, sizes[3])]
            device = self.place['z_peer'](lax.rem(my_z + index - 5, PEERS))
        else:
            level = 11 - index
            src = dst = self.total.at[pl.ds((keep0, keep1, keep2)[level], sizes[level])]
            device = peer[names[level]]
        slot = self.sem_base + part * SEMS_PER_PART + index
        return pltpu.make_async_remote_copy(
            src_ref=src, dst_ref=dst, send_sem=self.send_sem.at[slot], recv_sem=self.recv_sem.at[slot],
            device_id=device, device_id_type=MESH_ID)

    def step(self, part, stage):
        first, sizes, bits, _ = self.geometry(part)
        got1, got2, got3 = self.got1.at[part], self.got2.at[part], self.got3.at[part]
        keep0 = first + bits[0] * sizes[0]
        my_z = self.place['z']
        waits = ((), (0,), (1,), (2,), (3, 4, 5), (6, 7, 8), (9,), (10,), (11,))[stage]
        begins = ((0,), (1,), (2,), (3, 4, 5), (6, 7, 8), (9,), (10,), (11,), ())[stage]
        for index in waits:
            self.copy(part, index).wait()
        if stage == 1:
            add_into(got1, self.grads, keep0, sizes[0])
        elif stage == 2:
            add_into(got2, got1, bits[1] * sizes[1], sizes[1])
        elif stage == 3:
            add_into(got3, got2, bits[2] * sizes[2], sizes[2])
        elif stage == 4:
            mine = got3[pl.ds(my_z * sizes[3], sizes[3])].astype(F32)
            for slot in range(PEERS - 1):
                mine = mine + self.gotz[part, slot].astype(F32)
            keep3 = keep0 + bits[1] * sizes[1] + bits[2] * sizes[2] + my_z * sizes[3]
            self.total[pl.ds(keep3, sizes[3])] = mine.astype(BF)
        for index in begins:
            self.copy(part, index).start()


def add_into(dst, src, src_start, count):
    step = 8 if count % 8 == 0 else count

    @pl.loop(0, count // step)
    def _(index):
        at = index * step
        left = dst[pl.ds(at, step)].astype(F32)
        right = src[pl.ds(src_start + at, step)].astype(F32)
        dst[pl.ds(at, step)] = (left + right).astype(BF)


def main_kernel(*refs):
    names = ('pair_z', 'single_s', 'token_mask', 'dz_out', 'ds_out', 'w_pa', 'w_pb', 'w_po', 'w_bias', 'w_q', 'q_bias',
             'w_kv', 'w_g', 'w_o', 'w_sa', 'w_sb', 'w_so')
    hbm = dict(zip(names, refs[:17]))
    dz_in, ds_in, total_out = refs[17:20]
    scratch = refs[20:]
    loaded = dict(zip(names, scratch[:17]))
    (new_rows, bias_rows, grad_bias, kv_buf, gkv_buf, gkv_got, acc_ab, acc_po, acc_bias, act_s, norm_s, gq_s, ggp_s,
     gmid_s, inv_s, prob_s, qexp_s, dz_stage, ds_stage, grads, total) = scratch[17:38]
    reduce_refs = scratch[38:38 + 4 * len(CHUNKS)]
    load_sem, kv_send, kv_recv, gkv_send, gkv_recv, ar_send, ar_recv, out_sem, tot_sem = scratch[38 + 4 * len(CHUNKS):]

    order = ('single_s', 'w_kv', 'pair_z', 'w_pa', 'w_pb', 'w_po', 'w_bias', 'w_q', 'q_bias', 'w_g', 'token_mask', 'w_o', 'w_sa',
             'w_sb', 'ds_out', 'w_so', 'dz_out')
    loads = {}
    for index, name in enumerate(order):
        loads[name] = pltpu.make_async_copy(hbm[name], loaded[name], load_sem.at[index])
        loads[name].start()

    my_z = lax.axis_index('dap')
    my_dp = lax.axis_index('dp')
    core = lax.rem(my_dp, 2)
    bit_x = lax.rem(lax.div(my_dp, 2), 2)
    bit_y = lax.div(my_dp, 4)

    def z_peer(other):
        return (other, my_dp)

    peer = {'core': (my_z, my_dp + 1 - 2 * core), 'x': (my_z, my_dp + 2 - 4 * bit_x), 'y': (my_z, my_dp + 4 - 8 * bit_y)}
    place = {'core': core, 'x': bit_x, 'y': bit_y, 'z': my_z, 'peer': peer, 'z_peer': z_peer}

    barrier = pltpu.get_barrier_semaphore()
    for device in list(peer.values()) + [z_peer(lax.rem(my_z + hop, PEERS)) for hop in range(1, PEERS)]:
        pl.semaphore_signal(barrier, inc=1, device_id=device, device_id_type=MESH_ID)
    pl.semaphore_wait(barrier, 6)

    loads['single_s'].wait()
    loads['w_kv'].wait()
    s_wide = loaded['single_s'][...].astype(F32).reshape(ALL_ROWS, WIDTH)
    s_norm, s_inv = layer_norm(s_wide)
    act = s_norm.astype(BF)
    act_s[...] = act
    norm_s[...] = s_norm
    inv_s[...] = s_inv
    kv_local = dot_nn(act, loaded['w_kv'][...])
    kv_buf[my_z] = kv_local.reshape(CPLX, ROWS, 2 * WIDTH).astype(BF)

    def kv_copy(hop):
        return pltpu.make_async_remote_copy(
            src_ref=kv_buf.at[my_z], dst_ref=kv_buf.at[my_z], send_sem=kv_send.at[hop - 1], recv_sem=kv_recv.at[hop - 1],
            device_id=z_peer(lax.rem(my_z + hop, PEERS)), device_id_type=MESH_ID)

    for hop in range(1, PEERS):
        kv_copy(hop).start()

    for name in ('pair_z', 'w_pa', 'w_pb', 'w_po', 'w_bias'):
        loads[name].wait()
    block_rows = BLOCK_I * TOKENS

    @pl.loop(0, NUM_BLOCKS)
    def _(block):
        at = block * BLOCK_I
        z_wide = loaded['pair_z'][pl.ds(at, BLOCK_I)].reshape(block_rows, PAIR).astype(F32)
        normed, _ = layer_norm(z_wide)
        normed_bf = normed.astype(BF)
        hid_a = dot_nn(normed_bf, loaded['w_pa'][...])
        hid_b = dot_nn(normed_bf, loaded['w_pb'][...])
        hidden = (hid_a * sigmoid(hid_a) * hid_b).astype(BF)
        z_new = (z_wide + dot_nn(hidden, loaded['w_po'][...])).astype(BF)
        new_rows[pl.ds(at, BLOCK_I)] = z_new.reshape(BLOCK_I, TOKENS, PAIR)
        bias_norm, _ = layer_norm(z_new.astype(F32))
        bias_bf = bias_norm.astype(BF)
        for row in range(BLOCK_I):
            bias_rows[at + row] = dot_nt(loaded['w_bias'][...], bias_bf[row * TOKENS:(row + 1) * TOKENS])

    for name in ('w_q', 'q_bias', 'w_g', 'token_mask', 'w_o', 'w_sa', 'w_sb', 'ds_out', 'w_so'):
        loads[name].wait()
    queries = (dot_nn(act_s[...], loaded['w_q'][...]) + loaded['q_bias'][...].astype(F32).reshape(1, WIDTH)).astype(BF).astype(F32)
    gate = sigmoid(dot_nn(act_s[...], loaded['w_g'][...]))
    lane_head = lax.broadcasted_iota(jnp.int32, (HEADS, WIDTH), 1)
    row_head = lax.broadcasted_iota(jnp.int32, (HEADS, WIDTH), 0)
    head_mask = jnp.where((lane_head >= row_head * HEAD_DIM) & (lane_head < (row_head + 1) * HEAD_DIM), 1.0, 0.0).astype(F32)

    def spread(rows):
        wide = jnp.broadcast_to(rows.reshape(ROWS, 1, WIDTH), (ROWS, HEADS, WIDTH)) * head_mask[None]
        return wide.reshape(ROWS * HEADS, WIDTH).astype(BF)

    def gather_heads(wide):
        return jnp.sum(wide.reshape(ROWS, HEADS, WIDTH) * head_mask[None], axis=1)

    for hop in range(1, PEERS):
        kv_copy(hop).wait()

    def keys_values(cplx):
        both = kv_buf[:, cplx].astype(F32).reshape(TOKENS, 2 * WIDTH).astype(BF)
        return both[:, :WIDTH], both[:, WIDTH:]

    key_mask = MASK_BIG * (loaded['token_mask'][...].astype(F32) - 1.0)
    attended_parts = []
    for cplx in range(CPLX):
        keys, values = keys_values(cplx)
        q_exp = spread(queries[cplx * ROWS:(cplx + 1) * ROWS])
        qexp_s[cplx] = q_exp
        bias = bias_rows[cplx * ROWS:(cplx + 1) * ROWS].reshape(ROWS * HEADS, TOKENS)
        logits = dot_nt(q_exp, keys) * SCALE + bias + key_mask[cplx:cplx + 1]
        top = jnp.max(logits, axis=-1, keepdims=True)
        expd = jnp.exp(logits - top)
        prob = expd / jnp.sum(expd, axis=-1, keepdims=True)
        prob_s[cplx] = prob
        attended_parts.append(gather_heads(dot_nn(prob.astype(BF), values)))
    attended = jnp.concatenate(attended_parts, axis=0)
    gated = (gate * attended).astype(BF)
    s_mid = (s_wide + dot_nn(gated, loaded['w_o'][...])).astype(BF)
    mid_norm, mid_inv = layer_norm(s_mid.astype(F32))
    mid_act = mid_norm.astype(BF)

    reducers = []
    for index, span in enumerate(CHUNKS):
        refs_here = (grads, total) + tuple(reduce_refs[4 * index:4 * index + 4]) + (ar_send, ar_recv)
        reducers.append(Reducer(span, index * 2 * SEMS_PER_PART, refs_here, place))

    def act_on(number):
        for chunk, part, step in ACTIONS[number]:
            if chunk < 0:
                finish_single()
            else:
                reducers[chunk].step(part, step)

    ds_wide = loaded['ds_out'][...].astype(F32).reshape(ALL_ROWS, WIDTH)
    ds_bf = ds_wide.astype(BF)
    grad_mid_norm = jnp.zeros((ALL_ROWS, WIDTH), F32)
    for piece in range(TRANS_S // PIECE):
        cols = slice(piece * PIECE, (piece + 1) * PIECE)
        base = piece * PIECE_TILES
        trans_a = dot_nn(mid_act, loaded['w_sa'][:, cols])
        trans_b = dot_nn(mid_act, loaded['w_sb'][:, cols])
        grad_hidden = dot_nt(ds_bf, loaded['w_so'][cols, :])
        hidden, grad_ta, grad_tb = swiglu_grad(trans_a, trans_b, grad_hidden)
        grad_ta = grad_ta.astype(BF)
        grad_tb = grad_tb.astype(BF)
        put_at(grads, base, dot_tn(hidden.astype(BF), ds_bf))
        put_at(grads, base + PIECE_TILES // 3, dot_tn(mid_act, grad_ta))
        put_at(grads, base + 2 * (PIECE_TILES // 3), dot_tn(mid_act, grad_tb))
        act_on(piece + 1)
        grad_mid_norm = grad_mid_norm + dot_nt(grad_ta, loaded['w_sa'][:, cols]) + dot_nt(grad_tb, loaded['w_sb'][:, cols])
    grad_mid = ds_wide + norm_grad(mid_norm, mid_inv, grad_mid_norm)
    gmid_s[...] = grad_mid
    grad_mid_bf = grad_mid.astype(BF)
    put_tiles(grads, 'o', dot_tn(gated, grad_mid_bf))
    grad_gated = dot_nt(grad_mid_bf, loaded['w_o'][...])
    grad_gate_pre = (grad_gated * attended * gate * (1.0 - gate)).astype(BF)
    ggp_s[...] = grad_gate_pre
    grad_att = (grad_gated * gate).astype(BF).astype(F32)
    grad_query_parts = []
    for cplx in range(CPLX):
        keys, values = keys_values(cplx)
        ga_exp = spread(grad_att[cplx * ROWS:(cplx + 1) * ROWS])
        prob = prob_s[cplx]
        grad_prob = dot_nt(ga_exp, values)
        grad_values = dot_tn(prob.astype(BF), ga_exp)
        grad_logits = (prob * (grad_prob - jnp.sum(prob * grad_prob, axis=-1, keepdims=True))).astype(BF)
        grad_bias[cplx * ROWS:(cplx + 1) * ROWS] = grad_logits.reshape(ROWS, HEADS, TOKENS)
        grad_query_parts.append(gather_heads(dot_nn(grad_logits, keys)) * SCALE)
        grad_keys = dot_tn(grad_logits, qexp_s[cplx]) * SCALE
        gkv_buf[:, cplx, :, :WIDTH] = grad_keys.reshape(PEERS, ROWS, WIDTH).astype(BF)
        gkv_buf[:, cplx, :, WIDTH:] = grad_values.reshape(PEERS, ROWS, WIDTH).astype(BF)

    def gkv_copy(hop):
        other = lax.rem(my_z + hop, PEERS)
        return pltpu.make_async_remote_copy(
            src_ref=gkv_buf.at[other], dst_ref=gkv_got.at[hop - 1], send_sem=gkv_send.at[hop - 1],
            recv_sem=gkv_recv.at[hop - 1], device_id=z_peer(other), device_id_type=MESH_ID)

    for hop in range(1, PEERS):
        gkv_copy(hop).start()
    act_on(4)
    grad_query = jnp.concatenate(grad_query_parts, axis=0)
    grad_query_bf = grad_query.astype(BF)
    gq_s[...] = grad_query_bf
    put_tiles(grads, 'q', dot_tn(act_s[...], grad_query_bf))
    put_tiles(grads, 'g', dot_tn(act_s[...], grad_gate_pre))
    d_q_bias = jnp.sum(grad_query, axis=0, keepdims=True)
    row_index = lax.broadcasted_iota(jnp.int32, (16, 128), 0)
    bias_tile = jnp.zeros((16, 128), F32)
    for sub in range(3):
        bias_tile = jnp.where(row_index == sub, jnp.broadcast_to(d_q_bias[:, sub * 128:(sub + 1) * 128], (16, 128)), bias_tile)
    grads[1080] = bias_tile.astype(BF)
    grads[1081:1088] = jnp.zeros((7, 16, 128), BF)
    grads[1232:1280] = jnp.zeros((48, 16, 128), BF)
    grads[1377:1408] = jnp.zeros((31, 16, 128), BF)

    def finish_single():
        for hop in range(1, PEERS):
            gkv_copy(hop).wait()
        summed = gkv_buf[my_z].astype(F32)
        for hop in range(1, PEERS):
            summed = summed + gkv_got[hop - 1].astype(F32)
        grad_kv = summed.reshape(ALL_ROWS, 2 * WIDTH).astype(BF)
        put_tiles(grads, 'kv', dot_tn(act_s[...], grad_kv))
        grad_act = (dot_nt(gq_s[...], loaded['w_q'][...]) + dot_nt(grad_kv, loaded['w_kv'][...])
                    + dot_nt(ggp_s[...], loaded['w_g'][...]))
        grad_s = gmid_s[...] + norm_grad(norm_s[...], inv_s[...], grad_act)
        ds_stage[...] = grad_s.reshape(CPLX, ROWS, WIDTH).astype(BF)
        pltpu.make_async_copy(ds_stage, ds_in, out_sem.at[2]).start()

    loads['dz_out'].wait()
    acc_ab[...] = jnp.zeros_like(acc_ab)
    acc_po[...] = jnp.zeros_like(acc_po)
    acc_bias[...] = jnp.zeros_like(acc_bias)

    @pl.loop(0, NUM_BLOCKS)
    def _(block):
        for tick in range(NUM_BLOCKS):
            @pl.when(block == tick)
            def _():
                act_on(5 + tick)
        at = block * BLOCK_I
        bias_norm, bias_inv = layer_norm(new_rows[pl.ds(at, BLOCK_I)].reshape(block_rows, PAIR).astype(F32))
        bias_bf = bias_norm.astype(BF)
        bias_acc = acc_bias[...]
        parts = []
        for row in range(BLOCK_I):
            grad_row = grad_bias[at + row]
            bias_acc = bias_acc + dot_nn(grad_row, bias_bf[row * TOKENS:(row + 1) * TOKENS])
            parts.append(dot_tn(grad_row, loaded['w_bias'][...]))
        acc_bias[...] = bias_acc
        grad_norm = jnp.concatenate(parts, axis=0)
        dz_wide = loaded['dz_out'][pl.ds(at, BLOCK_I)].reshape(block_rows, PAIR).astype(F32)
        grad_new = dz_wide + norm_grad(bias_norm, bias_inv, grad_norm)
        grad_new_bf = grad_new.astype(BF)
        normed, inv_std = layer_norm(loaded['pair_z'][pl.ds(at, BLOCK_I)].reshape(block_rows, PAIR).astype(F32))
        normed_bf = normed.astype(BF)
        hid_a = dot_nn(normed_bf, loaded['w_pa'][...])
        hid_b = dot_nn(normed_bf, loaded['w_pb'][...])
        grad_hidden = dot_nt(grad_new_bf, loaded['w_po'][...])
        hidden, grad_a, grad_b = swiglu_grad(hid_a, hid_b, grad_hidden)
        grad_a = grad_a.astype(BF)
        grad_b = grad_b.astype(BF)
        acc_po[...] += dot_tn(grad_new_bf, hidden.astype(BF))
        acc_ab[:, :TRANS_P] += dot_tn(normed_bf, grad_a)
        acc_ab[:, TRANS_P:] += dot_tn(normed_bf, grad_b)
        grad_normed = dot_nt(grad_a, loaded['w_pa'][...]) + dot_nt(grad_b, loaded['w_pb'][...])
        result = grad_new + norm_grad(normed, inv_std, grad_normed)
        slot = lax.rem(block, 2)

        @pl.when(block >= 2)
        def _():
            pltpu.make_async_copy(dz_stage.at[slot], dz_in.at[pl.ds(0, BLOCK_I)], out_sem.at[slot]).wait()

        dz_stage[slot] = result.reshape(BLOCK_I, TOKENS, PAIR).astype(BF)
        pltpu.make_async_copy(dz_stage.at[slot], dz_in.at[pl.ds(at, BLOCK_I)], out_sem.at[slot]).start()

    put_tiles(grads, 'pa', acc_ab[:, :TRANS_P])
    put_tiles(grads, 'pb', acc_ab[:, TRANS_P:])
    put_tiles(grads, 'po', jnp.transpose(acc_po[...]))
    grads[1376] = acc_bias[...].astype(BF)
    copies = []

    def write_out(index):
        base, count = CHUNKS[index]
        made = pltpu.make_async_copy(total.at[pl.ds(base, count)], total_out.at[pl.ds(base, count)], tot_sem.at[index])
        made.start()
        copies.append(made)

    left = [action[:2] for action in ACTIONS[-1] if action[2] == STAGES]
    for index in range(len(CHUNKS)):
        if (index, 0) not in left and (index, 1) not in left:
            write_out(index)
    for chunk, part, step in ACTIONS[-1]:
        reducers[chunk].step(part, step)
        if step == STAGES:
            left.remove((chunk, part))
            if (chunk, 1 - part) not in left:
                write_out(chunk)
    pltpu.make_async_copy(ds_stage, ds_in, out_sem.at[2]).wait()
    for slot in range(2):
        pltpu.make_async_copy(dz_stage.at[slot], dz_in.at[pl.ds(0, BLOCK_I)], out_sem.at[slot]).wait()
    for copy in copies:
        copy.wait()


def run_main(inputs):
    any_spec = pl.BlockSpec(memory_space=pl.ANY)
    scratch = [pltpu.VMEM(value.shape, value.dtype) for value in inputs]
    scratch += [
        pltpu.VMEM((ALL_ROWS, TOKENS, PAIR), BF),
        pltpu.VMEM((ALL_ROWS, HEADS, TOKENS), F32),
        pltpu.VMEM((ALL_ROWS, HEADS, TOKENS), BF),
        pltpu.VMEM((PEERS, CPLX, ROWS, 2 * WIDTH), BF),
        pltpu.VMEM((PEERS, CPLX, ROWS, 2 * WIDTH), BF),
        pltpu.VMEM((PEERS - 1, CPLX, ROWS, 2 * WIDTH), BF),
        pltpu.VMEM((PAIR, 2 * TRANS_P), F32),
        pltpu.VMEM((PAIR, TRANS_P), F32),
        pltpu.VMEM((HEADS, PAIR), F32),
        pltpu.VMEM((ALL_ROWS, WIDTH), BF),
        pltpu.VMEM((ALL_ROWS, WIDTH), F32),
        pltpu.VMEM((ALL_ROWS, WIDTH), BF),
        pltpu.VMEM((ALL_ROWS, WIDTH), BF),
        pltpu.VMEM((ALL_ROWS, WIDTH), F32),
        pltpu.VMEM((ALL_ROWS, 1), F32),
        pltpu.VMEM((CPLX, ROWS * HEADS, TOKENS), F32),
        pltpu.VMEM((CPLX, ROWS * HEADS, WIDTH), BF),
        pltpu.VMEM((2, BLOCK_I, TOKENS, PAIR), BF),
        pltpu.VMEM((CPLX, ROWS, WIDTH), BF),
        pltpu.VMEM((TILES, 16, 128), BF),
        pltpu.VMEM((TILES, 16, 128), BF),
    ]
    for _, count in CHUNKS:
        scratch += [pltpu.VMEM((2, count // 4, 16, 128), BF), pltpu.VMEM((2, count // 8, 16, 128), BF),
                    pltpu.VMEM((2, count // 16, 16, 128), BF), pltpu.VMEM((2, PEERS - 1, count // 64, 16, 128), BF)]
    num_sems = len(CHUNKS) * 2 * SEMS_PER_PART
    dma = pltpu.SemaphoreType.DMA
    scratch += [dma((17,)), dma((3,)), dma((3,)), dma((3,)), dma((3,)), dma((num_sems,)), dma((num_sems,)), dma((3,)),
                dma((len(CHUNKS),))]
    return pl.pallas_call(
        main_kernel,
        out_shape=(jax.ShapeDtypeStruct((ALL_ROWS, TOKENS, PAIR), BF), jax.ShapeDtypeStruct((CPLX, ROWS, WIDTH), BF),
                   jax.ShapeDtypeStruct((TILES, 16, 128), BF)),
        in_specs=[any_spec] * 17,
        out_specs=(any_spec,) * 3,
        scratch_shapes=scratch,
        compiler_params=pltpu.CompilerParams(collective_id=0, has_side_effects=True, vmem_limit_bytes=62 * 1024 * 1024),
        name='pairformer_tail',
    )(*inputs)


UNPACK = ('pa', 'pb', 'po', 'bias', 'q', 'qb', 'kv', 'g', 'o', 'sa', 'sb', 'so')


READS = ((0, 288), (288, 288), (576, 288), (864, 224), (1088, 192), (1280, 128))


def unpack_kernel(tiles_hbm, *refs):
    outs = dict(zip(UNPACK, refs[:12]))
    stages = dict(zip(UNPACK, refs[12:24]))
    tiles, read_sem, sem = refs[24:]
    reads = []
    for index, (base, count) in enumerate(READS):
        made = pltpu.make_async_copy(tiles_hbm.at[pl.ds(base, count)], tiles.at[pl.ds(base, count)], read_sem.at[index])
        made.start()
        reads.append(made)

    def widen(stage, base, rows, row, cols, col):
        per_col = rows // 16
        for sub in range(cols // 128):
            part = tiles[base + sub * per_col:base + (sub + 1) * per_col].astype(F32)
            stage[row:row + rows, col + sub * 128:col + (sub + 1) * 128] = part.reshape(rows, 128)

    copies = []

    def send(name):
        made = pltpu.make_async_copy(stages[name], outs[name], sem.at[UNPACK.index(name)])
        made.start()
        copies.append(made)

    for piece in range(TRANS_S // PIECE):
        reads[piece].wait()
        base = piece * PIECE_TILES
        third = PIECE_TILES // 3
        widen(stages['so'], base, PIECE, piece * PIECE, WIDTH, 0)
        widen(stages['sa'], base + third, WIDTH, 0, PIECE, piece * PIECE)
        widen(stages['sb'], base + 2 * third, WIDTH, 0, PIECE, piece * PIECE)
    for name in ('so', 'sa', 'sb'):
        send(name)
    for index, names in ((3, ('o', 'q', 'g', 'qb')), (4, ('kv',)), (5, ('pa', 'pb', 'po', 'bias'))):
        reads[index].wait()
        for name in names:
            base, rows, cols = SLOTS[name]
            if name == 'qb':
                last_tile = tiles[base].astype(F32)
                for sub in range(3):
                    stages[name][pl.ds(sub * 128, 128)] = last_tile[sub]
            else:
                widen(stages[name], base, rows, 0, cols, 0)
            send(name)
    for copy in copies:
        copy.wait()


def run_unpack(tiles):
    shapes = [(WIDTH,) if name == 'qb' else (TRANS_S, WIDTH) if name == 'so' else (WIDTH, TRANS_S) if name in ('sa', 'sb')
              else SLOTS[name][1:] for name in UNPACK]
    any_spec = pl.BlockSpec(memory_space=pl.ANY)
    return pl.pallas_call(
        unpack_kernel,
        out_shape=tuple(jax.ShapeDtypeStruct(shape, F32) for shape in shapes),
        in_specs=[any_spec],
        out_specs=(any_spec,) * 12,
        scratch_shapes=[pltpu.VMEM(shape, F32) for shape in shapes] + [
            pltpu.VMEM((TILES, 16, 128), BF), pltpu.SemaphoreType.DMA((len(READS),)), pltpu.SemaphoreType.DMA((12,))],
        compiler_params=pltpu.CompilerParams(vmem_limit_bytes=62 * 1024 * 1024),
        name='unpack_sums',
    )(tiles)


def solution(mesh):
    pair_spec = P('dp', 'dap', None, None)
    single_spec = P('dp', 'dap', None)

    def body(pair_z, single_s, token_mask, dz_out, ds_out, w_pa, w_pb, w_po, w_bias, w_q, q_bias, w_kv, w_g, w_o, w_sa, w_sb, w_so):
        inputs = (pair_z.reshape(ALL_ROWS, TOKENS, PAIR), single_s, token_mask, dz_out.reshape(ALL_ROWS, TOKENS, PAIR), ds_out,
                  w_pa, w_pb, w_po, w_bias.T, w_q, q_bias, w_kv, w_g, w_o, w_sa, w_sb, w_so)
        dz_in, ds_in, tiles = run_main(inputs)
        sums = list(run_unpack(tiles))
        sums[3] = sums[3].T
        return (dz_in.reshape(pair_z.shape), ds_in) + tuple(sums)

    in_specs = (pair_spec, single_spec, P('dp', None), pair_spec, single_spec) + (P(),) * 12
    out_specs = (pair_spec, single_spec) + (P(),) * 12
    return jax.shard_map(body, mesh=mesh, in_specs=in_specs, out_specs=out_specs, check_vma=False)
```

```python
import math
import jax
import jax.numpy as jnp
from jax import lax
from jax.experimental import pallas as pl
from jax.experimental.pallas import tpu as pltpu
from jax.sharding import PartitionSpec as P

HEAD_DIM = 24
HEADS = 16
WIDTH = 384
TRANS_S = 1536
PAIR = 128
TRANS_P = 512
TOKENS = 96
ROWS = 24
CPLX = 3
ALL_ROWS = CPLX * ROWS
SCALE = HEAD_DIM ** -0.5
EPSILON = 1e-5
MASK_BIG = 1e9
PEERS = 4
MESH_ID = pl.DeviceIdType.MESH
BF = jnp.bfloat16
F32 = jnp.float32

PIECE = 512
PIECE_TILES = 288
SLOTS = {
    'o': (864, 384, 384),
    'q': (936, 384, 384), 'g': (1008, 384, 384), 'qb': (1080, 16, 128), 'kv': (1088, 384, 768),
    'pa': (1280, 128, 512), 'pb': (1312, 128, 512), 'po': (1344, 512, 128), 'bias': (1376, 16, 128),
}
CHUNK = 128
LOCAL_END, PAIR_START, TILES = 1088, 1280, 1408
CHUNKS = tuple((base, min(CHUNK, LOCAL_END - base)) for base in range(0, LOCAL_END, CHUNK)) + (
    (LOCAL_END, PAIR_START - LOCAL_END), (PAIR_START, TILES - PAIR_START))
KV_CHUNK, PAIR_CHUNK = len(CHUNKS) - 2, len(CHUNKS) - 1
BLOCK_I = 8
NUM_BLOCKS = ALL_ROWS // BLOCK_I

CHUNK_KINDS = 'hhpfhapmppp'
LEVELS = {
    'a': (('core', 'x', 'y', 'z'), ('core', 'y', 'x', 'z')),
    'h': (('core', 'x', 'y', 'z0', 'z1'), ('core', 'y', 'x', 'z0', 'z1')),
    'f': (('core', 'z0', 'x', 'y', 'z1'), ('core', 'z0', 'y', 'x', 'z1')),
    'm': (('core', 'x', 'z0', 'y', 'z1'), ('core', 'y', 'z0', 'x', 'z1')),
    'p': (('core', 'xy', 'z'), ('core', 'xy', 'z')),
}
GROUP = {'core': 2, 'x': 2, 'y': 2, 'z': 4, 'z0': 2, 'z1': 2, 'xy': 4}

LINK_US = {
    'core': {'core': 0.0036}, 'x': {'x': 0.0687}, 'y': {'y': 0.0687}, 'xy': {'x': 0.1374, 'y': 0.1374},
    'z': {'mid': 0.3736, 'end': 0.2802}, 'z0': {'end': 0.0934}, 'z1': {'mid': 0.1868, 'end': 0.0934},
}
LATENCY_US = {'core': 0.83, 'x': 3.0, 'y': 3.0, 'z': 4.15, 'z0': 3.0, 'z1': 3.6, 'xy': 3.8}
KV_LINK_US = {'mid': 12.0, 'end': 9.0}
FIRST_BLOCK = 5
SEGMENT_US = (1.0, 1.0, 1.0, 2.1, 0.4) + (2.15,) * NUM_BLOCKS + (0.75,) * NUM_BLOCKS
SEGMENT_TILES = (288, 576, 864, 936, LOCAL_END)
KV_SEGMENT, PAIR_SEGMENT = 3, 4 + NUM_BLOCKS


def level_sizes(chunk):
    sizes = [CHUNKS[chunk][1] // 2]
    for name in LEVELS[CHUNK_KINDS[chunk]][0]:
        sizes.append(sizes[-1] // GROUP[name])
    return sizes


def plan_actions():
    stage = [0] * len(CHUNKS)
    due = {}
    free = {}
    actions = [[] for _ in range(len(SEGMENT_US) + 1)]
    now, segment, kv_due, kv_done = 0.0, 0, None, False

    def steps(chunk):
        return 2 * len(LEVELS[CHUNK_KINDS[chunk]][0])

    def occupy(links, start):
        ends = []
        for link, time in links.items():
            free[link] = max(free.get(link, 0.0), start) + time
            ends.append(free[link])
        return max(ends)

    def ready(chunk):
        if stage[chunk] > steps(chunk):
            return False
        if stage[chunk]:
            return due[chunk] <= now
        if chunk == PAIR_CHUNK:
            return segment > PAIR_SEGMENT
        if chunk == KV_CHUNK:
            return kv_done
        end = sum(CHUNKS[chunk])
        return segment > next(index for index, tiles in enumerate(SEGMENT_TILES) if end <= tiles)

    while True:
        if kv_due is not None and kv_due <= now and not kv_done:
            actions[segment].append((-1, 0))
            now, kv_done = now + 0.8, True
            continue
        waiting = [chunk for chunk in range(len(CHUNKS)) if ready(chunk)]
        if waiting:
            chunk = min(waiting, key=lambda one: (one != PAIR_CHUNK, one))
            step = stage[chunk]
            actions[segment].append((chunk, step))
            half = steps(chunk) // 2
            sizes = level_sizes(chunk)
            now += 0.01 + (0.01 + 0.0034 * sizes[step] if 0 < step <= half else 0.0)
            if step < 2 * half:
                level = min(step, 2 * half - 1 - step)
                for names in LEVELS[CHUNK_KINDS[chunk]]:
                    name = names[level]
                    links = {link: time * sizes[level + 1] for link, time in LINK_US[name].items()}
                    end = occupy(links, now) + LATENCY_US[name]
                    due[chunk] = max(end, due.get(chunk, 0.0))
            stage[chunk] = step + 1
        elif segment < len(SEGMENT_US):
            now += SEGMENT_US[segment]
            if segment == KV_SEGMENT:
                kv_due = occupy(KV_LINK_US, now) + LATENCY_US['z']
            segment += 1
        else:
            later = [due[chunk] for chunk in range(len(CHUNKS)) if 0 < stage[chunk] <= steps(chunk)]
            later += [kv_due] * (not kv_done)
            if not later:
                return actions
            now = max(now, min(later))


ACTIONS = plan_actions()


def dot_nn(left, right):
    return lax.dot_general(left, right, (((1,), (0,)), ((), ())), preferred_element_type=F32)


def dot_nt(left, right):
    return lax.dot_general(left, right, (((1,), (1,)), ((), ())), preferred_element_type=F32)


def dot_tn(left, right):
    return lax.dot_general(left, right, (((0,), (0,)), ((), ())), preferred_element_type=F32)


def layer_norm(wide):
    centred = wide - jnp.mean(wide, axis=-1, keepdims=True)
    inv_std = lax.rsqrt(jnp.mean(centred * centred, axis=-1, keepdims=True) + EPSILON)
    return centred * inv_std, inv_std


def norm_grad(normed, inv_std, grad_out):
    mean_grad = jnp.mean(grad_out, axis=-1, keepdims=True)
    mean_proj = jnp.mean(grad_out * normed, axis=-1, keepdims=True)
    return inv_std * (grad_out - mean_grad - normed * mean_proj)


def sigmoid(values):
    return 0.5 * jnp.tanh(0.5 * values) + 0.5


def swiglu_grad(hid_a, hid_b, grad_hidden):
    sig_a = sigmoid(hid_a)
    silu_a = hid_a * sig_a
    grad_a = (grad_hidden * hid_b) * (sig_a + silu_a * (1.0 - sig_a))
    return silu_a * hid_b, grad_a, grad_hidden * silu_a


def put_at(grads, base, value):
    per_col = value.shape[0] // 16
    for col in range(value.shape[1] // 128):
        start = base + col * per_col
        grads[start:start + per_col] = value[:, col * 128:(col + 1) * 128].reshape(per_col, 16, 128).astype(BF)


def put_tiles(grads, name, value):
    put_at(grads, SLOTS[name][0], value)


class Reducer:
    def __init__(self, chunk, grads, total, total_out, got, send_sem, recv_sem, out_sem, place):
        self.chunk = chunk
        self.grads, self.total, self.total_out, self.got = grads, total, total_out, got
        self.send_sem, self.recv_sem, self.out_sem = send_sem, recv_sem, out_sem
        self.place = place
        self.levels = LEVELS[CHUNK_KINDS[chunk]]
        self.sizes = level_sizes(chunk)
        self.depth = len(self.levels[0])

    def kept(self, part, level):
        at = CHUNKS[self.chunk][0] + part * self.sizes[0]
        for name, size in zip(self.levels[part][:level], self.sizes[1:]):
            at = at + self.place['index'][name] * size
        return at

    def held(self, part, level, start, count):
        if level == 0:
            return self.grads.at[pl.ds(self.kept(part, 0) + start, count)]
        return self.got[level - 1].at[part, 0, pl.ds(start, count)]

    def start(self, step):
        level = min(step, 2 * self.depth - 1 - step)
        size = self.sizes[level + 1]
        for part in range(2):
            name = self.levels[part][level]
            group = GROUP[name]
            for hop in range(1, group):
                other = lax.rem(self.place['index'][name] + hop, group)
                if step < self.depth:
                    src, dst = self.held(part, level, other * size, size), self.got[level].at[part, hop - 1]
                else:
                    src = dst = self.total.at[pl.ds(self.kept(part, level + 1), size)]
                pltpu.make_async_remote_copy(
                    src_ref=src, dst_ref=dst, send_sem=self.send_sem, recv_sem=self.recv_sem.at[step],
                    device_id=self.place['peer'](name, other), device_id_type=MESH_ID).start()

    def moved(self, level):
        return 2 * (GROUP[self.levels[0][level]] - 1) * self.sizes[level + 1]

    def wait_tiles(self, count, sem):
        span = self.grads.at[pl.ds(0, count)]
        pltpu.make_async_copy(span, span, sem).wait()

    def add(self, level):
        size = self.sizes[level + 1]
        for part in range(2):
            name = self.levels[part][level]
            own = self.held(part, level, self.place['index'][name] * size, size)
            slots = [self.got[level].at[part, hop] for hop in range(GROUP[name] - 1)]
            dst = slots[0] if level + 1 < self.depth else self.total.at[pl.ds(self.kept(part, level + 1), size)]
            add_into(dst, [own] + slots, size)

    def step(self, step):
        if step:
            level = min(step - 1, 2 * self.depth - step)
            self.wait_tiles(self.moved(level), self.recv_sem.at[step - 1])
        if 0 < step <= self.depth:
            self.add(step - 1)
        if step < 2 * self.depth:
            self.start(step)
        else:
            base, count = CHUNKS[self.chunk]
            pltpu.make_async_copy(self.total.at[pl.ds(base, count)], self.total_out.at[pl.ds(base, count)], self.out_sem).start()

    def finish_sends(self):
        self.wait_tiles(2 * sum(self.moved(level) for level in range(self.depth)), self.send_sem)


def add_into(dst, terms, count):
    step = math.gcd(count, 8)

    @pl.loop(0, count // step)
    def _(index):
        at = pl.ds(index * step, step)
        total = terms[0][at].astype(F32)
        for term in terms[1:]:
            total = total + term[at].astype(F32)
        dst[at] = total.astype(BF)


def main_kernel(*refs):
    names = ('pair_z', 'single_s', 'token_mask', 'dz_out', 'ds_out', 'w_pa', 'w_pb', 'w_po', 'w_bias', 'w_q', 'q_bias',
             'w_kv', 'w_g', 'w_o', 'w_sa', 'w_sb', 'w_so')
    hbm = dict(zip(names, refs[:17]))
    dz_in, ds_in, total_out = refs[17:20]
    scratch = refs[20:]
    loaded = dict(zip(names, scratch[:17]))
    (new_rows, bias_rows, grad_bias, kv_buf, gkv_buf, gkv_got, acc_ab, acc_po, acc_bias, gab_s, act_s, norm_s, gq_s, ggp_s,
     gmid_s, inv_s, prob_s, qexp_s, dz_stage, ds_stage, grads, total) = scratch[17:39]
    got_refs = list(scratch[39:39 + GOT_COUNT])
    load_sem, kv_send, kv_recv, gkv_send, gkv_recv, ar_send, ar_recv, out_sem, tot_sem = scratch[39 + GOT_COUNT:]

    order = ('single_s', 'w_kv', 'pair_z', 'w_pa', 'w_pb', 'w_po', 'w_bias', 'w_q', 'q_bias', 'w_g', 'token_mask', 'w_o', 'w_sa',
             'w_sb', 'ds_out', 'w_so', 'dz_out')
    loads = {}
    for index, name in enumerate(order):
        loads[name] = pltpu.make_async_copy(hbm[name], loaded[name], load_sem.at[index])
        loads[name].start()

    my_z = lax.axis_index('dap')
    my_dp = lax.axis_index('dp')
    core = lax.rem(my_dp, 2)
    bit_x = lax.rem(lax.div(my_dp, 2), 2)
    bit_y = lax.div(my_dp, 4)

    def z_peer(other):
        return (other, my_dp)

    def peer(name, other):
        if name == 'core':
            return my_z, my_dp + other - core
        if name == 'x':
            return my_z, my_dp + 2 * (other - bit_x)
        if name == 'y':
            return my_z, my_dp + 4 * (other - bit_y)
        if name == 'xy':
            return my_z, 2 * other + core
        if name == 'z':
            return other, my_dp
        low = lax.rem(my_z, 2)
        return (my_z - low + other if name == 'z0' else 2 * other + low), my_dp

    place = {'peer': peer, 'index': {
        'core': core, 'x': bit_x, 'y': bit_y, 'xy': 2 * bit_y + bit_x, 'z': my_z, 'z0': lax.rem(my_z, 2), 'z1': lax.div(my_z, 2)}}

    barrier = pltpu.get_barrier_semaphore()
    for name in ('core', 'xy', 'z'):
        for hop in range(1, GROUP[name]):
            device = peer(name, lax.rem(place['index'][name] + hop, GROUP[name]))
            pl.semaphore_signal(barrier, inc=1, device_id=device, device_id_type=MESH_ID)

    loads['single_s'].wait()
    loads['w_kv'].wait()
    s_wide = loaded['single_s'][...].astype(F32).reshape(ALL_ROWS, WIDTH)
    s_norm, s_inv = layer_norm(s_wide)
    act = s_norm.astype(BF)
    act_s[...] = act
    norm_s[...] = s_norm
    inv_s[...] = s_inv
    kv_local = dot_nn(act, loaded['w_kv'][...])
    pl.semaphore_wait(barrier, 7)
    kv_buf[my_z] = kv_local.reshape(CPLX, ROWS, 2 * WIDTH).astype(BF)

    def kv_copy(hop):
        return pltpu.make_async_remote_copy(
            src_ref=kv_buf.at[my_z], dst_ref=kv_buf.at[my_z], send_sem=kv_send.at[hop - 1], recv_sem=kv_recv.at[hop - 1],
            device_id=z_peer(lax.rem(my_z + hop, PEERS)), device_id_type=MESH_ID)

    for hop in range(1, PEERS):
        kv_copy(hop).start()

    for name in ('pair_z', 'w_pa', 'w_pb', 'w_po', 'w_bias'):
        loads[name].wait()
    block_rows = BLOCK_I * TOKENS

    @pl.loop(0, NUM_BLOCKS)
    def _(block):
        at = block * BLOCK_I
        z_wide = loaded['pair_z'][pl.ds(at, BLOCK_I)].reshape(block_rows, PAIR).astype(F32)
        normed, _ = layer_norm(z_wide)
        normed_bf = normed.astype(BF)
        hid_a = dot_nn(normed_bf, loaded['w_pa'][...])
        hid_b = dot_nn(normed_bf, loaded['w_pb'][...])
        hidden = (hid_a * sigmoid(hid_a) * hid_b).astype(BF)
        z_new = (z_wide + dot_nn(hidden, loaded['w_po'][...])).astype(BF)
        new_rows[pl.ds(at, BLOCK_I)] = z_new.reshape(BLOCK_I, TOKENS, PAIR)
        bias_norm, _ = layer_norm(z_new.astype(F32))
        bias_bf = bias_norm.astype(BF)
        for row in range(BLOCK_I):
            bias_rows[at + row] = dot_nt(loaded['w_bias'][...], bias_bf[row * TOKENS:(row + 1) * TOKENS])

    for name in ('w_q', 'q_bias', 'w_g', 'token_mask', 'w_o', 'w_sa', 'w_sb', 'ds_out', 'w_so'):
        loads[name].wait()
    queries = (dot_nn(act_s[...], loaded['w_q'][...]) + loaded['q_bias'][...].astype(F32).reshape(1, WIDTH)).astype(BF).astype(F32)
    gate = sigmoid(dot_nn(act_s[...], loaded['w_g'][...]))
    lane_head = lax.broadcasted_iota(jnp.int32, (HEADS, WIDTH), 1)
    row_head = lax.broadcasted_iota(jnp.int32, (HEADS, WIDTH), 0)
    head_mask = jnp.where((lane_head >= row_head * HEAD_DIM) & (lane_head < (row_head + 1) * HEAD_DIM), 1.0, 0.0).astype(F32)

    def spread(rows):
        wide = jnp.broadcast_to(rows.reshape(ROWS, 1, WIDTH), (ROWS, HEADS, WIDTH)) * head_mask[None]
        return wide.reshape(ROWS * HEADS, WIDTH).astype(BF)

    def gather_heads(wide):
        return jnp.sum(wide.reshape(ROWS, HEADS, WIDTH) * head_mask[None], axis=1)

    for hop in range(1, PEERS):
        kv_copy(hop).wait()

    def keys_values(cplx):
        both = kv_buf[:, cplx].astype(F32).reshape(TOKENS, 2 * WIDTH).astype(BF)
        return both[:, :WIDTH], both[:, WIDTH:]

    key_mask = MASK_BIG * (loaded['token_mask'][...].astype(F32) - 1.0)
    attended_parts = []
    for cplx in range(CPLX):
        keys, values = keys_values(cplx)
        q_exp = spread(queries[cplx * ROWS:(cplx + 1) * ROWS])
        qexp_s[cplx] = q_exp
        bias = bias_rows[cplx * ROWS:(cplx + 1) * ROWS].reshape(ROWS * HEADS, TOKENS)
        logits = dot_nt(q_exp, keys) * SCALE + bias + key_mask[cplx:cplx + 1]
        top = jnp.max(logits, axis=-1, keepdims=True)
        expd = jnp.exp(logits - top)
        prob = expd / jnp.sum(expd, axis=-1, keepdims=True)
        prob_s[cplx] = prob
        attended_parts.append(gather_heads(dot_nn(prob.astype(BF), values)))
    attended = jnp.concatenate(attended_parts, axis=0)
    gated = (gate * attended).astype(BF)
    s_mid = (s_wide + dot_nn(gated, loaded['w_o'][...])).astype(BF)
    mid_norm, mid_inv = layer_norm(s_mid.astype(F32))
    mid_act = mid_norm.astype(BF)

    reducers = []
    for index in range(len(CHUNKS)):
        depth = len(LEVELS[CHUNK_KINDS[index]][0])
        reducers.append(Reducer(index, grads, total, total_out, got_refs[:depth], ar_send.at[index], ar_recv.at[index], tot_sem, place))
        del got_refs[:depth]

    def act_on(number):
        for chunk, step in ACTIONS[number]:
            if chunk < 0:
                finish_single()
            else:
                reducers[chunk].step(step)

    ds_wide = loaded['ds_out'][...].astype(F32).reshape(ALL_ROWS, WIDTH)
    ds_bf = ds_wide.astype(BF)
    grad_mid_norm = jnp.zeros((ALL_ROWS, WIDTH), F32)
    for piece in range(TRANS_S // PIECE):
        cols = slice(piece * PIECE, (piece + 1) * PIECE)
        base = piece * PIECE_TILES
        trans_a = dot_nn(mid_act, loaded['w_sa'][:, cols])
        trans_b = dot_nn(mid_act, loaded['w_sb'][:, cols])
        grad_hidden = dot_nt(ds_bf, loaded['w_so'][cols, :])
        hidden, grad_ta, grad_tb = swiglu_grad(trans_a, trans_b, grad_hidden)
        grad_ta = grad_ta.astype(BF)
        grad_tb = grad_tb.astype(BF)
        put_at(grads, base, dot_tn(hidden.astype(BF), ds_bf))
        put_at(grads, base + PIECE_TILES // 3, dot_tn(mid_act, grad_ta))
        put_at(grads, base + 2 * (PIECE_TILES // 3), dot_tn(mid_act, grad_tb))
        act_on(piece + 1)
        grad_mid_norm = grad_mid_norm + dot_nt(grad_ta, loaded['w_sa'][:, cols]) + dot_nt(grad_tb, loaded['w_sb'][:, cols])
    grad_mid = ds_wide + norm_grad(mid_norm, mid_inv, grad_mid_norm)
    gmid_s[...] = grad_mid
    grad_mid_bf = grad_mid.astype(BF)
    put_tiles(grads, 'o', dot_tn(gated, grad_mid_bf))
    grad_gated = dot_nt(grad_mid_bf, loaded['w_o'][...])
    grad_gate_pre = (grad_gated * attended * gate * (1.0 - gate)).astype(BF)
    ggp_s[...] = grad_gate_pre
    grad_att = (grad_gated * gate).astype(BF).astype(F32)
    grad_query_parts = []
    for cplx in range(CPLX):
        keys, values = keys_values(cplx)
        ga_exp = spread(grad_att[cplx * ROWS:(cplx + 1) * ROWS])
        prob = prob_s[cplx]
        grad_prob = dot_nt(ga_exp, values)
        grad_values = dot_tn(prob.astype(BF), ga_exp)
        grad_logits = (prob * (grad_prob - jnp.sum(prob * grad_prob, axis=-1, keepdims=True))).astype(BF)
        grad_bias[cplx * ROWS:(cplx + 1) * ROWS] = grad_logits.reshape(ROWS, HEADS, TOKENS)
        grad_query_parts.append(gather_heads(dot_nn(grad_logits, keys)) * SCALE)
        grad_keys = dot_tn(grad_logits, qexp_s[cplx]) * SCALE
        gkv_buf[:, cplx, :, :WIDTH] = grad_keys.reshape(PEERS, ROWS, WIDTH).astype(BF)
        gkv_buf[:, cplx, :, WIDTH:] = grad_values.reshape(PEERS, ROWS, WIDTH).astype(BF)

    def gkv_copy(hop):
        other = lax.rem(my_z + hop, PEERS)
        return pltpu.make_async_remote_copy(
            src_ref=gkv_buf.at[other], dst_ref=gkv_got.at[hop - 1], send_sem=gkv_send.at[hop - 1],
            recv_sem=gkv_recv.at[hop - 1], device_id=z_peer(other), device_id_type=MESH_ID)

    for hop in range(1, PEERS):
        gkv_copy(hop).start()
    act_on(4)
    grad_query = jnp.concatenate(grad_query_parts, axis=0)
    grad_query_bf = grad_query.astype(BF)
    gq_s[...] = grad_query_bf
    put_tiles(grads, 'q', dot_tn(act_s[...], grad_query_bf))
    put_tiles(grads, 'g', dot_tn(act_s[...], grad_gate_pre))
    d_q_bias = jnp.sum(grad_query, axis=0, keepdims=True)
    row_index = lax.broadcasted_iota(jnp.int32, (16, 128), 0)
    bias_tile = jnp.zeros((16, 128), F32)
    for sub in range(3):
        bias_tile = jnp.where(row_index == sub, jnp.broadcast_to(d_q_bias[:, sub * 128:(sub + 1) * 128], (16, 128)), bias_tile)
    grads[1080] = bias_tile.astype(BF)
    grads[1081:1088] = jnp.zeros((7, 16, 128), BF)
    grads[1232:1280] = jnp.zeros((48, 16, 128), BF)
    grads[1377:1408] = jnp.zeros((31, 16, 128), BF)

    def finish_single():
        for hop in range(1, PEERS):
            gkv_copy(hop).wait()
        summed = gkv_buf[my_z].astype(F32)
        for hop in range(1, PEERS):
            summed = summed + gkv_got[hop - 1].astype(F32)
        grad_kv = summed.reshape(ALL_ROWS, 2 * WIDTH).astype(BF)
        put_tiles(grads, 'kv', dot_tn(act_s[...], grad_kv))
        grad_act = (dot_nt(gq_s[...], loaded['w_q'][...]) + dot_nt(grad_kv, loaded['w_kv'][...])
                    + dot_nt(ggp_s[...], loaded['w_g'][...]))
        grad_s = gmid_s[...] + norm_grad(norm_s[...], inv_s[...], grad_act)
        ds_stage[...] = grad_s.reshape(CPLX, ROWS, WIDTH).astype(BF)
        pltpu.make_async_copy(ds_stage, ds_in, out_sem.at[2]).start()

    loads['dz_out'].wait()
    acc_ab[...] = jnp.zeros_like(acc_ab)
    acc_po[...] = jnp.zeros_like(acc_po)
    acc_bias[...] = jnp.zeros_like(acc_bias)

    def act_in_loop(block, first):
        for tick in range(NUM_BLOCKS):
            if ACTIONS[first + tick]:
                @pl.when(block == tick)
                def _():
                    act_on(first + tick)

    @pl.loop(0, NUM_BLOCKS)
    def _(block):
        act_in_loop(block, FIRST_BLOCK)
        at = block * BLOCK_I
        bias_norm, bias_inv = layer_norm(new_rows[pl.ds(at, BLOCK_I)].reshape(block_rows, PAIR).astype(F32))
        bias_bf = bias_norm.astype(BF)
        bias_acc = acc_bias[...]
        parts = []
        for row in range(BLOCK_I):
            grad_row = grad_bias[at + row]
            bias_acc = bias_acc + dot_nn(grad_row, bias_bf[row * TOKENS:(row + 1) * TOKENS])
            parts.append(dot_tn(grad_row, loaded['w_bias'][...]))
        acc_bias[...] = bias_acc
        grad_norm = jnp.concatenate(parts, axis=0)
        dz_wide = loaded['dz_out'][pl.ds(at, BLOCK_I)].reshape(block_rows, PAIR).astype(F32)
        grad_new_bf = (dz_wide + norm_grad(bias_norm, bias_inv, grad_norm)).astype(BF)
        new_rows[pl.ds(at, BLOCK_I)] = grad_new_bf.reshape(BLOCK_I, TOKENS, PAIR)
        normed, _ = layer_norm(loaded['pair_z'][pl.ds(at, BLOCK_I)].reshape(block_rows, PAIR).astype(F32))
        normed_bf = normed.astype(BF)
        hid_a = dot_nn(normed_bf, loaded['w_pa'][...])
        hid_b = dot_nn(normed_bf, loaded['w_pb'][...])
        grad_hidden = dot_nt(grad_new_bf, loaded['w_po'][...])
        hidden, grad_a, grad_b = swiglu_grad(hid_a, hid_b, grad_hidden)
        grad_a = grad_a.astype(BF)
        grad_b = grad_b.astype(BF)
        gab_s[block, :, :TRANS_P] = grad_a
        gab_s[block, :, TRANS_P:] = grad_b
        acc_po[...] += dot_tn(grad_new_bf, hidden.astype(BF))
        acc_ab[:, :TRANS_P] += dot_tn(normed_bf, grad_a)
        acc_ab[:, TRANS_P:] += dot_tn(normed_bf, grad_b)

    put_tiles(grads, 'pa', acc_ab[:, :TRANS_P])
    put_tiles(grads, 'pb', acc_ab[:, TRANS_P:])
    put_tiles(grads, 'po', jnp.transpose(acc_po[...]))
    grads[1376] = acc_bias[...].astype(BF)

    @pl.loop(0, NUM_BLOCKS)
    def _(block):
        act_in_loop(block, FIRST_BLOCK + NUM_BLOCKS)
        at = block * BLOCK_I
        normed, inv_std = layer_norm(loaded['pair_z'][pl.ds(at, BLOCK_I)].reshape(block_rows, PAIR).astype(F32))
        grad_normed = dot_nt(gab_s[block, :, :TRANS_P], loaded['w_pa'][...]) + dot_nt(gab_s[block, :, TRANS_P:], loaded['w_pb'][...])
        grad_new = new_rows[pl.ds(at, BLOCK_I)].reshape(block_rows, PAIR).astype(F32)
        result = grad_new + norm_grad(normed, inv_std, grad_normed)
        slot = lax.rem(block, 2)

        @pl.when(block >= 2)
        def _():
            pltpu.make_async_copy(dz_stage.at[slot], dz_in.at[pl.ds(0, BLOCK_I)], out_sem.at[slot]).wait()

        dz_stage[slot] = result.reshape(BLOCK_I, TOKENS, PAIR).astype(BF)
        pltpu.make_async_copy(dz_stage.at[slot], dz_in.at[pl.ds(at, BLOCK_I)], out_sem.at[slot]).start()

    act_on(FIRST_BLOCK + 2 * NUM_BLOCKS)
    for reducer in reducers:
        reducer.finish_sends()
    pltpu.make_async_copy(ds_stage, ds_in, out_sem.at[2]).wait()
    for slot in range(2):
        pltpu.make_async_copy(dz_stage.at[slot], dz_in.at[pl.ds(0, BLOCK_I)], out_sem.at[slot]).wait()
    pltpu.make_async_copy(total, total_out, tot_sem).wait()


GOT_COUNT = sum(len(LEVELS[kind][0]) for kind in CHUNK_KINDS)
MAX_STEPS = 2 * max(len(LEVELS[kind][0]) for kind in CHUNK_KINDS)


def run_main(inputs):
    any_spec = pl.BlockSpec(memory_space=pl.ANY)
    scratch = [pltpu.VMEM(value.shape, value.dtype) for value in inputs]
    scratch += [
        pltpu.VMEM((ALL_ROWS, TOKENS, PAIR), BF),
        pltpu.VMEM((ALL_ROWS, HEADS, TOKENS), F32),
        pltpu.VMEM((ALL_ROWS, HEADS, TOKENS), BF),
        pltpu.VMEM((PEERS, CPLX, ROWS, 2 * WIDTH), BF),
        pltpu.VMEM((PEERS, CPLX, ROWS, 2 * WIDTH), BF),
        pltpu.VMEM((PEERS - 1, CPLX, ROWS, 2 * WIDTH), BF),
        pltpu.VMEM((PAIR, 2 * TRANS_P), F32),
        pltpu.VMEM((PAIR, TRANS_P), F32),
        pltpu.VMEM((HEADS, PAIR), F32),
        pltpu.VMEM((NUM_BLOCKS, BLOCK_I * TOKENS, 2 * TRANS_P), BF),
        pltpu.VMEM((ALL_ROWS, WIDTH), BF),
        pltpu.VMEM((ALL_ROWS, WIDTH), F32),
        pltpu.VMEM((ALL_ROWS, WIDTH), BF),
        pltpu.VMEM((ALL_ROWS, WIDTH), BF),
        pltpu.VMEM((ALL_ROWS, WIDTH), F32),
        pltpu.VMEM((ALL_ROWS, 1), F32),
        pltpu.VMEM((CPLX, ROWS * HEADS, TOKENS), F32),
        pltpu.VMEM((CPLX, ROWS * HEADS, WIDTH), BF),
        pltpu.VMEM((2, BLOCK_I, TOKENS, PAIR), BF),
        pltpu.VMEM((CPLX, ROWS, WIDTH), BF),
        pltpu.VMEM((TILES, 16, 128), BF),
        pltpu.VMEM((TILES, 16, 128), BF),
    ]
    for chunk, kind in enumerate(CHUNK_KINDS):
        for name, size in zip(LEVELS[kind][0], level_sizes(chunk)[1:]):
            scratch.append(pltpu.VMEM((2, GROUP[name] - 1, size, 16, 128), BF))
    dma = pltpu.SemaphoreType.DMA
    scratch += [dma((17,)), dma((3,)), dma((3,)), dma((3,)), dma((3,)), dma((len(CHUNKS),)), dma((len(CHUNKS), MAX_STEPS)), dma((3,)),
                dma]
    return pl.pallas_call(
        main_kernel,
        out_shape=(jax.ShapeDtypeStruct((ALL_ROWS, TOKENS, PAIR), BF), jax.ShapeDtypeStruct((CPLX, ROWS, WIDTH), BF),
                   jax.ShapeDtypeStruct((TILES, 16, 128), BF)),
        in_specs=[any_spec] * 17,
        out_specs=(any_spec,) * 3,
        scratch_shapes=scratch,
        compiler_params=pltpu.CompilerParams(collective_id=0, has_side_effects=True, vmem_limit_bytes=62 * 1024 * 1024),
        name='pairformer_tail',
    )(*inputs)


UNPACK = ('pa', 'pb', 'po', 'bias', 'q', 'qb', 'kv', 'g', 'o', 'sa', 'sb', 'so')


READS = ((0, 288), (288, 288), (576, 288), (864, 224), (1088, 192), (1280, 128))


def unpack_kernel(tiles_hbm, dz_hbm, ds_hbm, *refs):
    outs = dict(zip(UNPACK, refs[:12]))
    dz_out, ds_out = refs[12:14]
    stages = dict(zip(UNPACK, refs[14:26]))
    tiles, dz_buf, ds_buf, read_sem, sem, pass_sem = refs[26:]
    reads = []
    for index, (base, count) in enumerate(READS):
        made = pltpu.make_async_copy(tiles_hbm.at[pl.ds(base, count)], tiles.at[pl.ds(base, count)], read_sem.at[index])
        made.start()
        reads.append(made)
    passes = ((dz_hbm, dz_buf, dz_out), (ds_hbm, ds_buf, ds_out))
    for index, (src, buf, _) in enumerate(passes):
        pltpu.make_async_copy(src, buf, pass_sem.at[index]).start()

    def widen(stage, base, rows, row, cols, col):
        per_col = rows // 16
        for sub in range(cols // 128):
            part = tiles[base + sub * per_col:base + (sub + 1) * per_col].astype(F32)
            stage[row:row + rows, col + sub * 128:col + (sub + 1) * 128] = part.reshape(rows, 128)

    copies = []

    def send(name):
        made = pltpu.make_async_copy(stages[name], outs[name], sem.at[UNPACK.index(name)])
        made.start()
        copies.append(made)

    for piece in range(TRANS_S // PIECE):
        reads[piece].wait()
        base = piece * PIECE_TILES
        third = PIECE_TILES // 3
        widen(stages['so'], base, PIECE, piece * PIECE, WIDTH, 0)
        widen(stages['sa'], base + third, WIDTH, 0, PIECE, piece * PIECE)
        widen(stages['sb'], base + 2 * third, WIDTH, 0, PIECE, piece * PIECE)
    for name in ('so', 'sa', 'sb'):
        send(name)
    for index, names in ((3, ('o', 'q', 'g', 'qb')), (4, ('kv',)), (5, ('pa', 'pb', 'po', 'bias'))):
        reads[index].wait()
        for name in names:
            base, rows, cols = SLOTS[name]
            if name == 'qb':
                last_tile = tiles[base].astype(F32)
                for sub in range(3):
                    stages[name][pl.ds(sub * 128, 128)] = last_tile[sub]
            else:
                widen(stages[name], base, rows, 0, cols, 0)
            send(name)
    for index, (src, buf, dst) in enumerate(passes):
        pltpu.make_async_copy(src, buf, pass_sem.at[index]).wait()
        made = pltpu.make_async_copy(buf, dst, pass_sem.at[index])
        made.start()
        copies.append(made)
    for copy in copies:
        copy.wait()


def run_unpack(tiles, dz_in, ds_in):
    shapes = [(WIDTH,) if name == 'qb' else (TRANS_S, WIDTH) if name == 'so' else (WIDTH, TRANS_S) if name in ('sa', 'sb')
              else SLOTS[name][1:] for name in UNPACK]
    any_spec = pl.BlockSpec(memory_space=pl.ANY)
    return pl.pallas_call(
        unpack_kernel,
        out_shape=tuple(jax.ShapeDtypeStruct(shape, F32) for shape in shapes) + (
            jax.ShapeDtypeStruct(dz_in.shape, BF), jax.ShapeDtypeStruct(ds_in.shape, BF)),
        in_specs=[any_spec] * 3,
        out_specs=(any_spec,) * 14,
        scratch_shapes=[pltpu.VMEM(shape, F32) for shape in shapes] + [
            pltpu.VMEM((TILES, 16, 128), BF), pltpu.VMEM(dz_in.shape, BF), pltpu.VMEM(ds_in.shape, BF),
            pltpu.SemaphoreType.DMA((len(READS),)), pltpu.SemaphoreType.DMA((12,)), pltpu.SemaphoreType.DMA((2,))],
        compiler_params=pltpu.CompilerParams(vmem_limit_bytes=62 * 1024 * 1024),
        name='unpack_sums',
    )(tiles, dz_in, ds_in)


def solution(mesh):
    pair_spec = P('dp', 'dap', None, None)
    single_spec = P('dp', 'dap', None)

    def body(pair_z, single_s, token_mask, dz_out, ds_out, w_pa, w_pb, w_po, w_bias, w_q, q_bias, w_kv, w_g, w_o, w_sa, w_sb, w_so):
        inputs = (pair_z.reshape(ALL_ROWS, TOKENS, PAIR), single_s, token_mask, dz_out.reshape(ALL_ROWS, TOKENS, PAIR), ds_out,
                  w_pa, w_pb, w_po, w_bias.T, w_q, q_bias, w_kv, w_g, w_o, w_sa, w_sb, w_so)
        dz_in, ds_in, tiles = run_main(inputs)
        *sums, dz_in, ds_in = run_unpack(tiles, dz_in, ds_in)
        sums[3] = sums[3].T
        return (dz_in.reshape(pair_z.shape), ds_in) + tuple(sums)

    in_specs = (pair_spec, single_spec, P('dp', None), pair_spec, single_spec) + (P(),) * 12
    out_specs = (pair_spec, single_spec) + (P(),) * 12
    return jax.shard_map(body, mesh=mesh, in_specs=in_specs, out_specs=out_specs, check_vma=False)
```

```python
import math
import jax
import jax.numpy as jnp
from jax import lax
from jax.experimental import pallas as pl
from jax.experimental.pallas import tpu as pltpu
from jax.sharding import PartitionSpec as P

HEAD_DIM = 24
HEADS = 16
WIDTH = 384
TRANS_S = 1536
PAIR = 128
TRANS_P = 512
TOKENS = 96
ROWS = 24
CPLX = 3
ALL_ROWS = CPLX * ROWS
SCALE = HEAD_DIM ** -0.5
EPSILON = 1e-5
MASK_BIG = 1e9
PEERS = 4
MESH_ID = pl.DeviceIdType.MESH
BF = jnp.bfloat16
F32 = jnp.float32

PIECE = 512
PIECE_TILES = 288
SLOTS = {
    'o': (864, 384, 384),
    'q': (936, 384, 384), 'g': (1008, 384, 384), 'qb': (1080, 16, 128), 'kv': (1088, 384, 768),
    'pa': (1280, 128, 512), 'pb': (1312, 128, 512), 'po': (1344, 512, 128), 'bias': (1376, 16, 128),
}
CHUNK = 128
LOCAL_END, PAIR_START, TILES = 1088, 1280, 1408
CHUNKS = tuple((base, min(CHUNK, LOCAL_END - base)) for base in range(0, LOCAL_END, CHUNK)) + (
    (LOCAL_END, PAIR_START - LOCAL_END), (PAIR_START, TILES - PAIR_START))
KV_CHUNK, PAIR_CHUNK = len(CHUNKS) - 2, len(CHUNKS) - 1
BLOCK_I = 8
NUM_BLOCKS = ALL_ROWS // BLOCK_I
FWD_BLOCK_I = 12

CHUNK_KINDS = 'haaaahaaapp'
LEVELS = {
    'a': (('core', 'x', 'y', 'z'), ('core', 'y', 'x', 'z')),
    'h': (('core', 'x', 'y', 'z0', 'z1'), ('core', 'y', 'x', 'z0', 'z1')),
    'f': (('core', 'z0', 'x', 'y', 'z1'), ('core', 'z0', 'y', 'x', 'z1')),
    'm': (('core', 'x', 'z0', 'y', 'z1'), ('core', 'y', 'z0', 'x', 'z1')),
    'p': (('core', 'xy', 'z'), ('core', 'xy', 'z')),
}
GROUP = {'core': 2, 'x': 2, 'y': 2, 'z': 4, 'z0': 2, 'z1': 2, 'xy': 4}

LINK_US = {
    'core': {'core': 0.003}, 'x': {'x': 0.0757}, 'y': {'y': 0.0757}, 'xy': {'x': 0.1514, 'y': 0.1514},
    'z': {'mid': 0.3024, 'end': 0.2268}, 'z0': {'end': 0.0756}, 'z1': {'mid': 0.1512, 'end': 0.0756},
}
LATENCY_US = {'core': 0.85, 'x': 3.5, 'y': 3.2, 'z': 4.15, 'z0': 3.4, 'z1': 3.9, 'xy': 3.8}
KV_LINK_US = {'mid': 13.2, 'end': 9.9}
BACKLOG_US = 2.0
FIRST_BLOCK = 5
SEGMENT_US = (1.0, 1.0, 1.0, 2.1, 0.4) + (2.3,) * NUM_BLOCKS + (0.75,) * NUM_BLOCKS
SEGMENT_TILES = (288, 576, 864, 936, LOCAL_END)
KV_SEGMENT, PAIR_SEGMENT = 3, 4 + NUM_BLOCKS


def level_sizes(chunk):
    sizes = [CHUNKS[chunk][1] // 2]
    for name in LEVELS[CHUNK_KINDS[chunk]][0]:
        sizes.append(sizes[-1] // GROUP[name])
    return sizes


def plan_actions():
    stage = [0] * len(CHUNKS)
    due = {}
    free = {}
    actions = [[] for _ in range(len(SEGMENT_US) + 1)]
    now, segment, kv_due, kv_done = 0.0, 0, None, False

    def steps(chunk):
        return 2 * len(LEVELS[CHUNK_KINDS[chunk]][0])

    def occupy(links, start):
        ends = []
        for link, time in links.items():
            free[link] = max(free.get(link, 0.0), start) + time
            ends.append(free[link])
        return max(ends)

    def when(chunk):
        step, half = stage[chunk], steps(chunk) // 2
        if step > 2 * half:
            return None
        time = due.get(chunk, 0.0)
        if step == 0:
            if chunk == PAIR_CHUNK:
                able = segment > PAIR_SEGMENT
            elif chunk == KV_CHUNK:
                able = kv_done
            else:
                end = sum(CHUNKS[chunk])
                able = segment > next(index for index, tiles in enumerate(SEGMENT_TILES) if end <= tiles)
            if not able:
                return None
        if step < 2 * half and chunk != PAIR_CHUNK:
            for names in LEVELS[CHUNK_KINDS[chunk]]:
                for link in LINK_US[names[min(step, 2 * half - 1 - step)]]:
                    time = max(time, free.get(link, 0.0) - BACKLOG_US)
        return time

    while True:
        if kv_due is not None and kv_due <= now and not kv_done:
            actions[segment].append((-1, 0))
            now, kv_done = now + 0.8, True
            continue
        times = {chunk: when(chunk) for chunk in range(len(CHUNKS))}
        times = {chunk: time for chunk, time in times.items() if time is not None}
        waiting = [chunk for chunk, time in times.items() if time <= now]
        if waiting:
            chunk = min(waiting, key=lambda one: (one != PAIR_CHUNK, one))
            step = stage[chunk]
            actions[segment].append((chunk, step))
            half = steps(chunk) // 2
            sizes = level_sizes(chunk)
            now += 0.015 + (0.0034 * sizes[step] if 0 < step <= half else 0.0)
            if step < 2 * half:
                level = min(step, 2 * half - 1 - step)
                ends = []
                for names in LEVELS[CHUNK_KINDS[chunk]]:
                    name = names[level]
                    links = {link: time * sizes[level + 1] for link, time in LINK_US[name].items()}
                    ends.append(occupy(links, now) + LATENCY_US[name])
                due[chunk] = max(ends)
            stage[chunk] = step + 1
        elif segment < len(SEGMENT_US):
            now += SEGMENT_US[segment]
            if segment == KV_SEGMENT:
                kv_due = occupy(KV_LINK_US, now) + LATENCY_US['z']
            segment += 1
        else:
            later = list(times.values()) + [kv_due] * (not kv_done)
            if not later:
                return actions
            now = max(now, min(later))


ACTIONS = plan_actions()


def dot_nn(left, right):
    return lax.dot_general(left, right, (((1,), (0,)), ((), ())), preferred_element_type=F32)


def dot_nt(left, right):
    return lax.dot_general(left, right, (((1,), (1,)), ((), ())), preferred_element_type=F32)


def dot_tn(left, right):
    return lax.dot_general(left, right, (((0,), (0,)), ((), ())), preferred_element_type=F32)


def layer_norm(wide):
    centred = wide - jnp.mean(wide, axis=-1, keepdims=True)
    inv_std = lax.rsqrt(jnp.mean(centred * centred, axis=-1, keepdims=True) + EPSILON)
    return centred * inv_std, inv_std


def norm_grad(normed, inv_std, grad_out):
    mean_grad = jnp.mean(grad_out, axis=-1, keepdims=True)
    mean_proj = jnp.mean(grad_out * normed, axis=-1, keepdims=True)
    return inv_std * (grad_out - mean_grad - normed * mean_proj)


def sigmoid(values):
    return 0.5 * jnp.tanh(0.5 * values) + 0.5


def swiglu_grad(hid_a, hid_b, grad_hidden):
    half_a = 0.5 * hid_a
    tanh_a = jnp.tanh(half_a)
    sig_a = 0.5 * tanh_a + 0.5
    silu_a = half_a * tanh_a + half_a
    grad_a = (grad_hidden * hid_b) * (sig_a + silu_a * (1.0 - sig_a))
    return silu_a * hid_b, grad_a, grad_hidden * silu_a


def put_at(grads, base, value):
    per_col = value.shape[0] // 16
    for col in range(value.shape[1] // 128):
        start = base + col * per_col
        grads[start:start + per_col] = value[:, col * 128:(col + 1) * 128].reshape(per_col, 16, 128).astype(BF)


def put_tiles(grads, name, value):
    put_at(grads, SLOTS[name][0], value)


class Reducer:
    def __init__(self, chunk, grads, total, got, send_sem, recv_sem, place):
        self.chunk = chunk
        self.grads, self.total, self.got = grads, total, got
        self.send_sem, self.recv_sem = send_sem, recv_sem
        self.place = place
        self.levels = LEVELS[CHUNK_KINDS[chunk]]
        self.sizes = level_sizes(chunk)
        self.depth = len(self.levels[0])

    def kept(self, part, level):
        at = CHUNKS[self.chunk][0] + part * self.sizes[0]
        for name, size in zip(self.levels[part][:level], self.sizes[1:]):
            at = at + self.place['index'][name] * size
        return at

    def held(self, part, level, start, count):
        if level == 0:
            return self.grads.at[pl.ds(self.kept(part, 0) + start, count)]
        return self.got[level - 1].at[part, 0, pl.ds(start, count)]

    def start(self, step):
        level = min(step, 2 * self.depth - 1 - step)
        size = self.sizes[level + 1]
        for part in range(2):
            name = self.levels[part][level]
            group = GROUP[name]
            for hop in range(1, group):
                other = lax.rem(self.place['index'][name] + hop, group)
                if step < self.depth:
                    src, dst = self.held(part, level, other * size, size), self.got[level].at[part, hop - 1]
                else:
                    src = dst = self.total.at[pl.ds(self.kept(part, level + 1), size)]
                pltpu.make_async_remote_copy(
                    src_ref=src, dst_ref=dst, send_sem=self.send_sem, recv_sem=self.recv_sem.at[step],
                    device_id=self.place['peer'](name, other), device_id_type=MESH_ID).start()

    def moved(self, level):
        return 2 * (GROUP[self.levels[0][level]] - 1) * self.sizes[level + 1]

    def wait_tiles(self, count, sem):
        span = self.grads.at[pl.ds(0, count)]
        pltpu.make_async_copy(span, span, sem).wait()

    def add(self, level):
        size = self.sizes[level + 1]
        for part in range(2):
            name = self.levels[part][level]
            own = self.held(part, level, self.place['index'][name] * size, size)
            slots = [self.got[level].at[part, hop] for hop in range(GROUP[name] - 1)]
            dst = slots[0] if level + 1 < self.depth else self.total.at[pl.ds(self.kept(part, level + 1), size)]
            add_into(dst, [own] + slots, size)

    def step(self, step):
        if step:
            level = min(step - 1, 2 * self.depth - step)
            self.wait_tiles(self.moved(level), self.recv_sem.at[step - 1])
        if 0 < step <= self.depth:
            self.add(step - 1)
        if step < 2 * self.depth:
            self.start(step)

    def finish_sends(self):
        self.wait_tiles(2 * sum(self.moved(level) for level in range(self.depth)), self.send_sem)


def add_into(dst, terms, count):
    step = math.gcd(count, 8)

    @pl.loop(0, count // step)
    def _(index):
        at = pl.ds(index * step, step)
        total = terms[0][at].astype(F32)
        for term in terms[1:]:
            total = total + term[at].astype(F32)
        dst[at] = total.astype(BF)


def main_kernel(*refs):
    names = ('pair_z', 'single_s', 'token_mask', 'dz_out', 'ds_out', 'w_pa', 'w_pb', 'w_po', 'w_bias', 'w_q', 'q_bias',
             'w_kv', 'w_g', 'w_o', 'w_sa', 'w_sb', 'w_so')
    hbm = dict(zip(names, refs[:17]))
    dz_in, ds_in, total = refs[17:20]
    scratch = refs[20:]
    loaded = dict(zip(names, scratch[:17]))
    (new_rows, bias_rows, grad_bias, kv_buf, gkv_buf, gkv_got, acc_ab, acc_po, acc_bias, gab_s, act_s, norm_s, gq_s, ggp_s,
     gmid_s, inv_s, prob_s, qexp_s, grads) = scratch[17:36]
    got_refs = list(scratch[36:36 + GOT_COUNT])
    load_sem, kv_send, kv_recv, gkv_send, gkv_recv, ar_send, ar_recv = scratch[36 + GOT_COUNT:]

    order = ('single_s', 'w_kv', 'pair_z', 'w_pa', 'w_pb', 'w_po', 'w_bias', 'w_q', 'q_bias', 'w_g', 'token_mask', 'w_o', 'w_sa',
             'w_sb', 'ds_out', 'w_so', 'dz_out')
    loads = {}
    for index, name in enumerate(order):
        loads[name] = pltpu.make_async_copy(hbm[name], loaded[name], load_sem.at[index])
        loads[name].start()

    my_z = lax.axis_index('dap')
    my_dp = lax.axis_index('dp')
    core = lax.rem(my_dp, 2)
    bit_x = lax.rem(lax.div(my_dp, 2), 2)
    bit_y = lax.div(my_dp, 4)

    def z_peer(other):
        return (other, my_dp)

    def peer(name, other):
        if name == 'core':
            return my_z, my_dp + other - core
        if name == 'x':
            return my_z, my_dp + 2 * (other - bit_x)
        if name == 'y':
            return my_z, my_dp + 4 * (other - bit_y)
        if name == 'xy':
            return my_z, 2 * other + core
        if name == 'z':
            return other, my_dp
        low = lax.rem(my_z, 2)
        return (my_z - low + other if name == 'z0' else 2 * other + low), my_dp

    place = {'peer': peer, 'index': {
        'core': core, 'x': bit_x, 'y': bit_y, 'xy': 2 * bit_y + bit_x, 'z': my_z, 'z0': lax.rem(my_z, 2), 'z1': lax.div(my_z, 2)}}

    barrier = pltpu.get_barrier_semaphore()
    for name in ('core', 'xy', 'z'):
        for hop in range(1, GROUP[name]):
            device = peer(name, lax.rem(place['index'][name] + hop, GROUP[name]))
            pl.semaphore_signal(barrier, inc=1, device_id=device, device_id_type=MESH_ID)

    loads['single_s'].wait()
    loads['w_kv'].wait()
    s_wide = loaded['single_s'][...].astype(F32).reshape(ALL_ROWS, WIDTH)
    s_norm, s_inv = layer_norm(s_wide)
    act = s_norm.astype(BF)
    act_s[...] = act
    norm_s[...] = s_norm
    inv_s[...] = s_inv
    kv_local = dot_nn(act, loaded['w_kv'][...])
    pl.semaphore_wait(barrier, 7)
    kv_buf[my_z] = kv_local.reshape(CPLX, ROWS, 2 * WIDTH).astype(BF)

    def kv_copy(hop):
        return pltpu.make_async_remote_copy(
            src_ref=kv_buf.at[my_z], dst_ref=kv_buf.at[my_z], send_sem=kv_send.at[hop - 1], recv_sem=kv_recv.at[hop - 1],
            device_id=z_peer(lax.rem(my_z + hop, PEERS)), device_id_type=MESH_ID)

    for hop in range(1, PEERS):
        kv_copy(hop).start()

    for name in ('pair_z', 'w_pa', 'w_pb', 'w_po', 'w_bias'):
        loads[name].wait()
    block_rows = BLOCK_I * TOKENS
    fwd_rows = FWD_BLOCK_I * TOKENS

    @pl.loop(0, ALL_ROWS // FWD_BLOCK_I)
    def _(block):
        at = block * FWD_BLOCK_I
        z_wide = loaded['pair_z'][pl.ds(at, FWD_BLOCK_I)].reshape(fwd_rows, PAIR).astype(F32)
        normed, _ = layer_norm(z_wide)
        normed_bf = normed.astype(BF)
        half_a = 0.5 * dot_nn(normed_bf, loaded['w_pa'][...])
        hid_b = dot_nn(normed_bf, loaded['w_pb'][...])
        hidden = ((half_a * jnp.tanh(half_a) + half_a) * hid_b).astype(BF)
        z_new = (z_wide + dot_nn(hidden, loaded['w_po'][...])).astype(BF)
        new_rows[pl.ds(at, FWD_BLOCK_I)] = z_new.reshape(FWD_BLOCK_I, TOKENS, PAIR)
        bias_norm, _ = layer_norm(z_new.astype(F32))
        bias_bf = bias_norm.astype(BF)
        for row in range(FWD_BLOCK_I):
            bias_rows[at + row] = dot_nt(loaded['w_bias'][...], bias_bf[row * TOKENS:(row + 1) * TOKENS])

    for name in ('w_q', 'q_bias', 'w_g', 'token_mask', 'w_o', 'w_sa', 'w_sb', 'ds_out', 'w_so'):
        loads[name].wait()
    queries = (dot_nn(act_s[...], loaded['w_q'][...]) + loaded['q_bias'][...].astype(F32).reshape(1, WIDTH)).astype(BF).astype(F32)
    gate = sigmoid(dot_nn(act_s[...], loaded['w_g'][...]))
    lane_head = lax.broadcasted_iota(jnp.int32, (HEADS, WIDTH), 1)
    row_head = lax.broadcasted_iota(jnp.int32, (HEADS, WIDTH), 0)
    head_mask = jnp.where((lane_head >= row_head * HEAD_DIM) & (lane_head < (row_head + 1) * HEAD_DIM), 1.0, 0.0).astype(F32)

    def spread(rows):
        wide = jnp.broadcast_to(rows.reshape(ROWS, 1, WIDTH), (ROWS, HEADS, WIDTH)) * head_mask[None]
        return wide.reshape(ROWS * HEADS, WIDTH).astype(BF)

    def gather_heads(wide):
        return jnp.sum(wide.reshape(ROWS, HEADS, WIDTH) * head_mask[None], axis=1)

    for hop in range(1, PEERS):
        kv_copy(hop).wait()

    def keys_values(cplx):
        both = kv_buf[:, cplx].astype(F32).reshape(TOKENS, 2 * WIDTH).astype(BF)
        return both[:, :WIDTH], both[:, WIDTH:]

    key_mask = MASK_BIG * (loaded['token_mask'][...].astype(F32) - 1.0)
    attended_parts = []
    for cplx in range(CPLX):
        keys, values = keys_values(cplx)
        q_exp = spread(queries[cplx * ROWS:(cplx + 1) * ROWS])
        qexp_s[cplx] = q_exp
        bias = bias_rows[cplx * ROWS:(cplx + 1) * ROWS].reshape(ROWS * HEADS, TOKENS)
        logits = dot_nt(q_exp, keys) * SCALE + bias + key_mask[cplx:cplx + 1]
        top = jnp.max(logits, axis=-1, keepdims=True)
        expd = jnp.exp(logits - top)
        prob = expd / jnp.sum(expd, axis=-1, keepdims=True)
        prob_s[cplx] = prob
        attended_parts.append(gather_heads(dot_nn(prob.astype(BF), values)))
    attended = jnp.concatenate(attended_parts, axis=0)
    gated = (gate * attended).astype(BF)
    s_mid = (s_wide + dot_nn(gated, loaded['w_o'][...])).astype(BF)
    mid_norm, mid_inv = layer_norm(s_mid.astype(F32))
    mid_act = mid_norm.astype(BF)

    reducers = []
    for index in range(len(CHUNKS)):
        depth = len(LEVELS[CHUNK_KINDS[index]][0])
        reducers.append(Reducer(index, grads, total, got_refs[:depth], ar_send.at[index], ar_recv.at[index], place))
        del got_refs[:depth]

    def act_on(number):
        for chunk, step in ACTIONS[number]:
            if chunk < 0:
                finish_single()
            else:
                reducers[chunk].step(step)

    ds_wide = loaded['ds_out'][...].astype(F32).reshape(ALL_ROWS, WIDTH)
    ds_bf = ds_wide.astype(BF)
    grad_mid_norm = jnp.zeros((ALL_ROWS, WIDTH), F32)
    for piece in range(TRANS_S // PIECE):
        cols = slice(piece * PIECE, (piece + 1) * PIECE)
        base = piece * PIECE_TILES
        trans_a = dot_nn(mid_act, loaded['w_sa'][:, cols])
        trans_b = dot_nn(mid_act, loaded['w_sb'][:, cols])
        grad_hidden = dot_nt(ds_bf, loaded['w_so'][cols, :])
        hidden, grad_ta, grad_tb = swiglu_grad(trans_a, trans_b, grad_hidden)
        grad_ta = grad_ta.astype(BF)
        grad_tb = grad_tb.astype(BF)
        put_at(grads, base, dot_tn(hidden.astype(BF), ds_bf))
        put_at(grads, base + PIECE_TILES // 3, dot_tn(mid_act, grad_ta))
        put_at(grads, base + 2 * (PIECE_TILES // 3), dot_tn(mid_act, grad_tb))
        act_on(piece + 1)
        grad_mid_norm = grad_mid_norm + dot_nt(grad_ta, loaded['w_sa'][:, cols]) + dot_nt(grad_tb, loaded['w_sb'][:, cols])
    grad_mid = ds_wide + norm_grad(mid_norm, mid_inv, grad_mid_norm)
    gmid_s[...] = grad_mid
    grad_mid_bf = grad_mid.astype(BF)
    put_tiles(grads, 'o', dot_tn(gated, grad_mid_bf))
    grad_gated = dot_nt(grad_mid_bf, loaded['w_o'][...])
    grad_gate_pre = (grad_gated * attended * gate * (1.0 - gate)).astype(BF)
    ggp_s[...] = grad_gate_pre
    grad_att = (grad_gated * gate).astype(BF).astype(F32)
    grad_query_parts = []
    for cplx in range(CPLX):
        keys, values = keys_values(cplx)
        ga_exp = spread(grad_att[cplx * ROWS:(cplx + 1) * ROWS])
        prob = prob_s[cplx]
        grad_prob = dot_nt(ga_exp, values)
        grad_values = dot_tn(prob.astype(BF), ga_exp)
        grad_logits = (prob * (grad_prob - jnp.sum(prob * grad_prob, axis=-1, keepdims=True))).astype(BF)
        grad_bias[cplx * ROWS:(cplx + 1) * ROWS] = grad_logits.reshape(ROWS, HEADS, TOKENS)
        grad_query_parts.append(gather_heads(dot_nn(grad_logits, keys)) * SCALE)
        grad_keys = dot_tn(grad_logits, qexp_s[cplx]) * SCALE
        gkv_buf[:, cplx, :, :WIDTH] = grad_keys.reshape(PEERS, ROWS, WIDTH).astype(BF)
        gkv_buf[:, cplx, :, WIDTH:] = grad_values.reshape(PEERS, ROWS, WIDTH).astype(BF)

    def gkv_copy(hop):
        other = lax.rem(my_z + hop, PEERS)
        return pltpu.make_async_remote_copy(
            src_ref=gkv_buf.at[other], dst_ref=gkv_got.at[hop - 1], send_sem=gkv_send.at[hop - 1],
            recv_sem=gkv_recv.at[hop - 1], device_id=z_peer(other), device_id_type=MESH_ID)

    for hop in range(1, PEERS):
        gkv_copy(hop).start()
    act_on(4)
    grad_query = jnp.concatenate(grad_query_parts, axis=0)
    grad_query_bf = grad_query.astype(BF)
    gq_s[...] = grad_query_bf
    put_tiles(grads, 'q', dot_tn(act_s[...], grad_query_bf))
    put_tiles(grads, 'g', dot_tn(act_s[...], grad_gate_pre))
    d_q_bias = jnp.sum(grad_query, axis=0, keepdims=True)
    row_index = lax.broadcasted_iota(jnp.int32, (16, 128), 0)
    bias_tile = jnp.zeros((16, 128), F32)
    for sub in range(3):
        bias_tile = jnp.where(row_index == sub, jnp.broadcast_to(d_q_bias[:, sub * 128:(sub + 1) * 128], (16, 128)), bias_tile)
    grads[1080] = bias_tile.astype(BF)
    grads[1081:1088] = jnp.zeros((7, 16, 128), BF)
    grads[1232:1280] = jnp.zeros((48, 16, 128), BF)
    grads[1377:1408] = jnp.zeros((31, 16, 128), BF)

    def finish_single():
        for hop in range(1, PEERS):
            gkv_copy(hop).wait()
        summed = gkv_buf[my_z].astype(F32)
        for hop in range(1, PEERS):
            summed = summed + gkv_got[hop - 1].astype(F32)
        grad_kv = summed.reshape(ALL_ROWS, 2 * WIDTH).astype(BF)
        put_tiles(grads, 'kv', dot_tn(act_s[...], grad_kv))
        grad_act = (dot_nt(gq_s[...], loaded['w_q'][...]) + dot_nt(grad_kv, loaded['w_kv'][...])
                    + dot_nt(ggp_s[...], loaded['w_g'][...]))
        grad_s = gmid_s[...] + norm_grad(norm_s[...], inv_s[...], grad_act)
        ds_in[...] = grad_s.reshape(CPLX, ROWS, WIDTH).astype(BF)

    loads['dz_out'].wait()
    acc_ab[...] = jnp.zeros_like(acc_ab)
    acc_po[...] = jnp.zeros_like(acc_po)
    acc_bias[...] = jnp.zeros_like(acc_bias)

    def act_in_loop(block, first):
        for tick in range(NUM_BLOCKS):
            if ACTIONS[first + tick]:
                @pl.when(block == tick)
                def _():
                    act_on(first + tick)

    @pl.loop(0, NUM_BLOCKS)
    def _(block):
        act_in_loop(block, FIRST_BLOCK)
        at = block * BLOCK_I
        bias_norm, bias_inv = layer_norm(new_rows[pl.ds(at, BLOCK_I)].reshape(block_rows, PAIR).astype(F32))
        bias_bf = bias_norm.astype(BF)
        bias_acc = acc_bias[...]
        parts = []
        for row in range(BLOCK_I):
            grad_row = grad_bias[at + row]
            bias_acc = bias_acc + dot_nn(grad_row, bias_bf[row * TOKENS:(row + 1) * TOKENS])
            parts.append(dot_tn(grad_row, loaded['w_bias'][...]))
        acc_bias[...] = bias_acc
        grad_norm = jnp.concatenate(parts, axis=0)
        dz_wide = loaded['dz_out'][pl.ds(at, BLOCK_I)].reshape(block_rows, PAIR).astype(F32)
        grad_new_bf = (dz_wide + norm_grad(bias_norm, bias_inv, grad_norm)).astype(BF)
        new_rows[pl.ds(at, BLOCK_I)] = grad_new_bf.reshape(BLOCK_I, TOKENS, PAIR)
        normed, _ = layer_norm(loaded['pair_z'][pl.ds(at, BLOCK_I)].reshape(block_rows, PAIR).astype(F32))
        normed_bf = normed.astype(BF)
        hid_a = dot_nn(normed_bf, loaded['w_pa'][...])
        hid_b = dot_nn(normed_bf, loaded['w_pb'][...])
        grad_hidden = dot_nt(grad_new_bf, loaded['w_po'][...])
        hidden, grad_a, grad_b = swiglu_grad(hid_a, hid_b, grad_hidden)
        grad_a = grad_a.astype(BF)
        grad_b = grad_b.astype(BF)
        gab_s[block, :, :TRANS_P] = grad_a
        gab_s[block, :, TRANS_P:] = grad_b
        acc_po[...] += dot_tn(grad_new_bf, hidden.astype(BF))
        acc_ab[:, :TRANS_P] += dot_tn(normed_bf, grad_a)
        acc_ab[:, TRANS_P:] += dot_tn(normed_bf, grad_b)

    put_tiles(grads, 'pa', acc_ab[:, :TRANS_P])
    put_tiles(grads, 'pb', acc_ab[:, TRANS_P:])
    put_tiles(grads, 'po', jnp.transpose(acc_po[...]))
    grads[1376] = acc_bias[...].astype(BF)

    @pl.loop(0, NUM_BLOCKS)
    def _(block):
        act_in_loop(block, FIRST_BLOCK + NUM_BLOCKS)
        at = block * BLOCK_I
        normed, inv_std = layer_norm(loaded['pair_z'][pl.ds(at, BLOCK_I)].reshape(block_rows, PAIR).astype(F32))
        grad_normed = dot_nt(gab_s[block, :, :TRANS_P], loaded['w_pa'][...]) + dot_nt(gab_s[block, :, TRANS_P:], loaded['w_pb'][...])
        grad_new = new_rows[pl.ds(at, BLOCK_I)].reshape(block_rows, PAIR).astype(F32)
        result = grad_new + norm_grad(normed, inv_std, grad_normed)
        dz_in[pl.ds(at, BLOCK_I)] = result.reshape(BLOCK_I, TOKENS, PAIR).astype(BF)

    act_on(FIRST_BLOCK + 2 * NUM_BLOCKS)
    for reducer in reducers:
        reducer.finish_sends()


GOT_COUNT = sum(len(LEVELS[kind][0]) for kind in CHUNK_KINDS)
MAX_STEPS = 2 * max(len(LEVELS[kind][0]) for kind in CHUNK_KINDS)


def run_main(inputs):
    any_spec = pl.BlockSpec(memory_space=pl.ANY)
    scratch = [pltpu.VMEM(value.shape, value.dtype) for value in inputs]
    scratch += [
        pltpu.VMEM((ALL_ROWS, TOKENS, PAIR), BF),
        pltpu.VMEM((ALL_ROWS, HEADS, TOKENS), F32),
        pltpu.VMEM((ALL_ROWS, HEADS, TOKENS), BF),
        pltpu.VMEM((PEERS, CPLX, ROWS, 2 * WIDTH), BF),
        pltpu.VMEM((PEERS, CPLX, ROWS, 2 * WIDTH), BF),
        pltpu.VMEM((PEERS - 1, CPLX, ROWS, 2 * WIDTH), BF),
        pltpu.VMEM((PAIR, 2 * TRANS_P), F32),
        pltpu.VMEM((PAIR, TRANS_P), F32),
        pltpu.VMEM((HEADS, PAIR), F32),
        pltpu.VMEM((NUM_BLOCKS, BLOCK_I * TOKENS, 2 * TRANS_P), BF),
        pltpu.VMEM((ALL_ROWS, WIDTH), BF),
        pltpu.VMEM((ALL_ROWS, WIDTH), F32),
        pltpu.VMEM((ALL_ROWS, WIDTH), BF),
        pltpu.VMEM((ALL_ROWS, WIDTH), BF),
        pltpu.VMEM((ALL_ROWS, WIDTH), F32),
        pltpu.VMEM((ALL_ROWS, 1), F32),
        pltpu.VMEM((CPLX, ROWS * HEADS, TOKENS), F32),
        pltpu.VMEM((CPLX, ROWS * HEADS, WIDTH), BF),
        pltpu.VMEM((TILES, 16, 128), BF),
    ]
    for chunk, kind in enumerate(CHUNK_KINDS):
        for name, size in zip(LEVELS[kind][0], level_sizes(chunk)[1:]):
            scratch.append(pltpu.VMEM((2, GROUP[name] - 1, size, 16, 128), BF))
    dma = pltpu.SemaphoreType.DMA
    scratch += [dma((17,)), dma((3,)), dma((3,)), dma((3,)), dma((3,)), dma((len(CHUNKS),)), dma((len(CHUNKS), MAX_STEPS))]
    return pl.pallas_call(
        main_kernel,
        out_shape=(pltpu.VMEM((ALL_ROWS, TOKENS, PAIR), BF), pltpu.VMEM((CPLX, ROWS, WIDTH), BF), pltpu.VMEM((TILES, 16, 128), BF)),
        in_specs=[any_spec] * 17,
        out_specs=(pl.BlockSpec(memory_space=pltpu.VMEM),) * 3,
        scratch_shapes=scratch,
        compiler_params=pltpu.CompilerParams(collective_id=0, has_side_effects=True, vmem_limit_bytes=48 * 1024 * 1024),
        name='pairformer_tail',
    )(*(pltpu.with_memory_space_constraint(value, pltpu.HBM) for value in inputs))


UNPACK = ('pa', 'pb', 'po', 'bias', 'q', 'qb', 'kv', 'g', 'o', 'sa', 'sb', 'so')


def unpack_kernel(tiles, dz_buf, ds_buf, *refs):
    outs = dict(zip(UNPACK, refs[:12]))
    dz_out, ds_out = refs[12:14]
    stages = dict(zip(UNPACK, refs[14:26]))
    sem, pass_sem = refs[26:]
    copies = []
    for index, (buf, dst) in enumerate(((dz_buf, dz_out), (ds_buf, ds_out))):
        made = pltpu.make_async_copy(buf, dst, pass_sem.at[index])
        made.start()
        copies.append(made)

    def widen(stage, base, rows, row, cols, col):
        per_col = rows // 16
        for sub in range(cols // 128):
            part = tiles[base + sub * per_col:base + (sub + 1) * per_col].astype(F32)
            stage[row:row + rows, col + sub * 128:col + (sub + 1) * 128] = part.reshape(rows, 128)

    def send(name):
        made = pltpu.make_async_copy(stages[name], outs[name], sem.at[UNPACK.index(name)])
        made.start()
        copies.append(made)

    for piece in range(TRANS_S // PIECE):
        base = piece * PIECE_TILES
        third = PIECE_TILES // 3
        widen(stages['so'], base, PIECE, piece * PIECE, WIDTH, 0)
        widen(stages['sa'], base + third, WIDTH, 0, PIECE, piece * PIECE)
        widen(stages['sb'], base + 2 * third, WIDTH, 0, PIECE, piece * PIECE)
    for name in ('so', 'sa', 'sb'):
        send(name)
    for name in ('kv', 'o', 'q', 'g', 'pa', 'pb', 'po', 'bias', 'qb'):
        base, rows, cols = SLOTS[name]
        if name == 'qb':
            last_tile = tiles[base].astype(F32)
            for sub in range(3):
                stages[name][pl.ds(sub * 128, 128)] = last_tile[sub]
        else:
            widen(stages[name], base, rows, 0, cols, 0)
        send(name)
    for copy in copies:
        copy.wait()


def run_unpack(tiles, dz_in, ds_in):
    shapes = [(WIDTH,) if name == 'qb' else (TRANS_S, WIDTH) if name == 'so' else (WIDTH, TRANS_S) if name in ('sa', 'sb')
              else SLOTS[name][1:] for name in UNPACK]
    any_spec = pl.BlockSpec(memory_space=pl.ANY)
    return pl.pallas_call(
        unpack_kernel,
        out_shape=tuple(jax.ShapeDtypeStruct(shape, F32) for shape in shapes) + (
            jax.ShapeDtypeStruct(dz_in.shape, BF), jax.ShapeDtypeStruct(ds_in.shape, BF)),
        in_specs=[pl.BlockSpec(memory_space=pltpu.VMEM)] * 3,
        out_specs=(any_spec,) * 14,
        scratch_shapes=[pltpu.VMEM(shape, F32) for shape in shapes] + [
            pltpu.SemaphoreType.DMA((12,)), pltpu.SemaphoreType.DMA((2,))],
        compiler_params=pltpu.CompilerParams(vmem_limit_bytes=24 * 1024 * 1024),
        name='unpack_sums',
    )(*(pltpu.with_memory_space_constraint(value, pltpu.VMEM) for value in (tiles, dz_in, ds_in)))


def solution(mesh):
    pair_spec = P('dp', 'dap', None, None)
    single_spec = P('dp', 'dap', None)

    def body(pair_z, single_s, token_mask, dz_out, ds_out, w_pa, w_pb, w_po, w_bias, w_q, q_bias, w_kv, w_g, w_o, w_sa, w_sb, w_so):
        inputs = (pair_z.reshape(ALL_ROWS, TOKENS, PAIR), single_s, token_mask, dz_out.reshape(ALL_ROWS, TOKENS, PAIR), ds_out,
                  w_pa, w_pb, w_po, w_bias.T, w_q, q_bias, w_kv, w_g, w_o, w_sa, w_sb, w_so)
        dz_in, ds_in, tiles = run_main(inputs)
        *sums, dz_in, ds_in = run_unpack(tiles, dz_in, ds_in)
        sums[3] = sums[3].T
        return (dz_in.reshape(pair_z.shape), ds_in) + tuple(sums)

    in_specs = (pair_spec, single_spec, P('dp', None), pair_spec, single_spec) + (P(),) * 12
    out_specs = (pair_spec, single_spec) + (P(),) * 12
    return jax.shard_map(body, mesh=mesh, in_specs=in_specs, out_specs=out_specs, check_vma=False)
```

```python
import math
import jax
import jax.numpy as jnp
from jax import lax
from jax.experimental import pallas as pl
from jax.experimental.pallas import tpu as pltpu
from jax.sharding import PartitionSpec as P

HEAD_DIM = 24
HEADS = 16
WIDTH = 384
TRANS_S = 1536
PAIR = 128
TRANS_P = 512
TOKENS = 96
ROWS = 24
CPLX = 3
ALL_ROWS = CPLX * ROWS
SCALE = HEAD_DIM ** -0.5
EPSILON = 1e-5
MASK_BIG = 1e9
PEERS = 4
MESH_ID = pl.DeviceIdType.MESH
BF = jnp.bfloat16
F32 = jnp.float32

PIECE = 512
PIECE_TILES = 288
SLOTS = {
    'o': (864, 384, 384),
    'q': (936, 384, 384), 'g': (1008, 384, 384), 'qb': (1080, 16, 128), 'kv': (1088, 384, 768),
    'pa': (1280, 128, 512), 'pb': (1312, 128, 512), 'po': (1344, 512, 128), 'bias': (1232, 16, 128),
}
CHUNK = 128
LOCAL_END, PAIR_START, TILES = 1088, 1280, 1376
CHUNKS = tuple((base, min(CHUNK, LOCAL_END - base)) for base in range(0, LOCAL_END, CHUNK)) + (
    (LOCAL_END, PAIR_START - LOCAL_END), (PAIR_START, TILES - PAIR_START))
KV_CHUNK, PAIR_CHUNK = len(CHUNKS) - 2, len(CHUNKS) - 1
BLOCK_I = 8
NUM_BLOCKS = ALL_ROWS // BLOCK_I
FWD_BLOCK_I = 12

CHUNK_KINDS = 'hhafafhaaap'
LEVELS = {
    'a': (('core', 'x', 'y', 'z'), ('core', 'y', 'x', 'z')),
    'h': (('core', 'x', 'y', 'z0', 'z1'), ('core', 'y', 'x', 'z0', 'z1')),
    'f': (('core', 'z0', 'x', 'y', 'z1'), ('core', 'z0', 'y', 'x', 'z1')),
    'm': (('core', 'x', 'z0', 'y', 'z1'), ('core', 'y', 'z0', 'x', 'z1')),
    'n': (('core', 'x', 'z0', 'z1', 'y'), ('core', 'y', 'z0', 'z1', 'x')),
    'p': (('core', 'xy', 'z'),),
}
GROUP = {'core': 2, 'x': 2, 'y': 2, 'z': 4, 'z0': 2, 'z1': 2, 'xy': 4}

LINK_US = {
    'core': {'core': 0.003}, 'x': {'x': 0.0757}, 'y': {'y': 0.0757}, 'xy': {'x': 0.1514, 'y': 0.1514},
    'z': {'mid': 0.3024, 'end': 0.2268}, 'z0': {'end': 0.0756}, 'z1': {'mid': 0.1512, 'end': 0.0756},
}
LATENCY_US = {'core': 0.85, 'x': 3.5, 'y': 3.2, 'z': 4.15, 'z0': 3.4, 'z1': 3.9, 'xy': 3.8}
KV_LINK_US = ({'end': 4.1}, {'mid': 4.1, 'end': 2.05})
BACKLOG_US = 2.0
FIRST_BLOCK = 5
MAIN_BLOCK = FIRST_BLOCK + NUM_BLOCKS
SINGLE_END = MAIN_BLOCK + NUM_BLOCKS
DZ_BLOCK = SINGLE_END + 1
SEGMENT_US = (1.0, 1.0, 1.0, 2.1, 0.4) + (0.55,) * NUM_BLOCKS + (1.85,) * NUM_BLOCKS + (0.6,) + (0.75,) * NUM_BLOCKS
SEGMENT_TILES = (288, 576, 864, 936, LOCAL_END)
KV_SEGMENT = 3


def level_sizes(chunk):
    sizes = [CHUNKS[chunk][1] // len(LEVELS[CHUNK_KINDS[chunk]])]
    for name in LEVELS[CHUNK_KINDS[chunk]][0]:
        sizes.append(sizes[-1] // GROUP[name])
    return sizes


def plan_actions():
    stage = [0] * len(CHUNKS)
    due = {}
    free = {}
    actions = [[] for _ in range(len(SEGMENT_US) + 1)]
    now, segment, kv_due, kv_step = 0.0, 0, None, 0

    def steps(chunk):
        return 2 * len(LEVELS[CHUNK_KINDS[chunk]][0])

    def occupy(links, start):
        ends = []
        for link, time in links.items():
            free[link] = max(free.get(link, 0.0), start) + time
            ends.append(free[link])
        return max(ends)

    def when(chunk):
        step, half = stage[chunk], steps(chunk) // 2
        if step > 2 * half:
            return None
        time = due.get(chunk, 0.0)
        if step == 0:
            if chunk == PAIR_CHUNK:
                able = segment >= SINGLE_END
            elif chunk == KV_CHUNK:
                able = kv_step == 2
            else:
                end = sum(CHUNKS[chunk])
                able = segment > next(index for index, tiles in enumerate(SEGMENT_TILES) if end <= tiles)
            if not able:
                return None
        if step < 2 * half and chunk != PAIR_CHUNK:
            for names in LEVELS[CHUNK_KINDS[chunk]]:
                for link in LINK_US[names[min(step, 2 * half - 1 - step)]]:
                    time = max(time, free.get(link, 0.0) - BACKLOG_US)
        return time

    while True:
        if kv_due is not None and kv_due <= now and (kv_step == 0 or segment >= MAIN_BLOCK):
            actions[segment].append((-1, kv_step))
            kv_step += 1
            now += 0.3
            kv_due = occupy(KV_LINK_US[1], now) + LATENCY_US['z1'] if kv_step == 1 else None
            continue
        times = {chunk: when(chunk) for chunk in range(len(CHUNKS))}
        times = {chunk: time for chunk, time in times.items() if time is not None}
        waiting = [chunk for chunk, time in times.items() if time <= now]
        if waiting:
            chunk = min(waiting, key=lambda one: (one != PAIR_CHUNK, one))
            step = stage[chunk]
            actions[segment].append((chunk, step))
            half = steps(chunk) // 2
            sizes = level_sizes(chunk)
            now += 0.015 + (0.0017 * len(LEVELS[CHUNK_KINDS[chunk]]) * sizes[step] if 0 < step <= half else 0.0)
            if step < 2 * half:
                level = min(step, 2 * half - 1 - step)
                ends = []
                for names in LEVELS[CHUNK_KINDS[chunk]]:
                    name = names[level]
                    links = {link: time * sizes[level + 1] for link, time in LINK_US[name].items()}
                    ends.append(occupy(links, now) + LATENCY_US[name])
                due[chunk] = max(ends)
            stage[chunk] = step + 1
        elif segment < len(SEGMENT_US):
            now += SEGMENT_US[segment]
            if segment == KV_SEGMENT:
                kv_due = occupy(KV_LINK_US[0], now) + LATENCY_US['z0']
            segment += 1
        else:
            later = list(times.values()) + [kv_due] * (kv_due is not None)
            if not later:
                return actions
            now = max(now, min(later))


ACTIONS = plan_actions()


def dot_nn(left, right):
    return lax.dot_general(left, right, (((1,), (0,)), ((), ())), preferred_element_type=F32)


def dot_nt(left, right):
    return lax.dot_general(left, right, (((1,), (1,)), ((), ())), preferred_element_type=F32)


def dot_tn(left, right):
    return lax.dot_general(left, right, (((0,), (0,)), ((), ())), preferred_element_type=F32)


def layer_norm(wide):
    centred = wide - jnp.mean(wide, axis=-1, keepdims=True)
    inv_std = lax.rsqrt(jnp.mean(centred * centred, axis=-1, keepdims=True) + EPSILON)
    return centred * inv_std, inv_std


def norm_grad(normed, inv_std, grad_out):
    mean_grad = jnp.mean(grad_out, axis=-1, keepdims=True)
    mean_proj = jnp.mean(grad_out * normed, axis=-1, keepdims=True)
    return inv_std * (grad_out - mean_grad - normed * mean_proj)


def sigmoid(values):
    return 0.5 * jnp.tanh(0.5 * values) + 0.5


def swiglu_grad(hid_a, hid_b, grad_hidden):
    half_a = 0.5 * hid_a
    tanh_a = jnp.tanh(half_a)
    sig_a = 0.5 * tanh_a + 0.5
    silu_a = half_a * tanh_a + half_a
    grad_a = (grad_hidden * hid_b) * (sig_a + silu_a * (1.0 - sig_a))
    return silu_a * hid_b, grad_a, grad_hidden * silu_a


def put_at(grads, base, value):
    per_col = value.shape[0] // 16
    for col in range(value.shape[1] // 128):
        start = base + col * per_col
        grads[start:start + per_col] = value[:, col * 128:(col + 1) * 128].reshape(per_col, 16, 128).astype(BF)


def put_tiles(grads, name, value):
    put_at(grads, SLOTS[name][0], value)


class Reducer:
    def __init__(self, chunk, grads, total, got, send_sem, recv_sem, place):
        self.chunk = chunk
        self.grads, self.total, self.got = grads, total, got
        self.send_sem, self.recv_sem = send_sem, recv_sem
        self.place = place
        self.levels = LEVELS[CHUNK_KINDS[chunk]]
        self.sizes = level_sizes(chunk)
        self.depth = len(self.levels[0])

    def kept(self, part, level):
        at = CHUNKS[self.chunk][0] + part * self.sizes[0]
        for name, size in zip(self.levels[part][:level], self.sizes[1:]):
            at = at + self.place['index'][name] * size
        return at

    def held(self, part, level, start, count):
        if level == 0:
            return self.grads.at[pl.ds(self.kept(part, 0) + start, count)]
        return self.got[level - 1].at[part, 0, pl.ds(start, count)]

    def start(self, step):
        level = min(step, 2 * self.depth - 1 - step)
        size = self.sizes[level + 1]
        for part in range(len(self.levels)):
            name = self.levels[part][level]
            group = GROUP[name]
            for hop in range(1, group):
                other = lax.rem(self.place['index'][name] + hop, group)
                if step < self.depth:
                    src, dst = self.held(part, level, other * size, size), self.got[level].at[part, hop - 1]
                else:
                    src = dst = self.total.at[pl.ds(self.kept(part, level + 1), size)]
                pltpu.make_async_remote_copy(
                    src_ref=src, dst_ref=dst, send_sem=self.send_sem, recv_sem=self.recv_sem.at[step],
                    device_id=self.place['peer'](name, other), device_id_type=MESH_ID).start()

    def moved(self, level):
        return len(self.levels) * (GROUP[self.levels[0][level]] - 1) * self.sizes[level + 1]

    def wait_tiles(self, count, sem):
        span = self.grads.at[pl.ds(0, count)]
        pltpu.make_async_copy(span, span, sem).wait()

    def add(self, level):
        size = self.sizes[level + 1]
        for part in range(len(self.levels)):
            name = self.levels[part][level]
            own = self.held(part, level, self.place['index'][name] * size, size)
            slots = [self.got[level].at[part, hop] for hop in range(GROUP[name] - 1)]
            dst = slots[0] if level + 1 < self.depth else self.total.at[pl.ds(self.kept(part, level + 1), size)]
            add_into(dst, [own] + slots, size)

    def step(self, step):
        if step:
            level = min(step - 1, 2 * self.depth - step)
            self.wait_tiles(self.moved(level), self.recv_sem.at[step - 1])
        if 0 < step <= self.depth:
            self.add(step - 1)
        if step < 2 * self.depth:
            self.start(step)

    def finish_sends(self):
        self.wait_tiles(2 * sum(self.moved(level) for level in range(self.depth)), self.send_sem)


def add_into(dst, terms, count):
    step = math.gcd(count, 8)

    @pl.loop(0, count // step)
    def _(index):
        at = pl.ds(index * step, step)
        total = terms[0][at].astype(F32)
        for term in terms[1:]:
            total = total + term[at].astype(F32)
        dst[at] = total.astype(BF)


def main_kernel(*refs):
    names = ('pair_z', 'single_s', 'token_mask', 'dz_out', 'ds_out', 'w_pa', 'w_pb', 'w_po', 'w_bias', 'w_q', 'q_bias',
             'w_kv', 'w_g', 'w_o', 'w_sa', 'w_sb', 'w_so')
    hbm = dict(zip(names, refs[:17]))
    dz_in, ds_in, total = refs[17:20]
    scratch = refs[20:]
    loaded = dict(zip(names, scratch[:17]))
    (new_rows, bias_rows, grad_bias, kv_buf, gkv_buf, gkv_got1, gkv_got2, gkv_s, acc_ab, acc_po, acc_bias, gab_s, act_s, norm_s, gq_s, ggp_s,
     gmid_s, inv_s, prob_s, qexp_s, grads) = scratch[17:38]
    got_refs = list(scratch[38:38 + GOT_COUNT])
    load_sem, kv_send, kv_recv, gkv_send, gkv_recv, ar_send, ar_recv = scratch[38 + GOT_COUNT:]

    order = ('single_s', 'w_kv', 'pair_z', 'w_pa', 'w_pb', 'w_po', 'w_bias', 'w_q', 'q_bias', 'w_g', 'token_mask', 'w_o', 'w_sa',
             'w_sb', 'ds_out', 'w_so', 'dz_out')
    loads = {}
    for index, name in enumerate(order):
        loads[name] = pltpu.make_async_copy(hbm[name], loaded[name], load_sem.at[index])
        loads[name].start()

    my_z = lax.axis_index('dap')
    my_dp = lax.axis_index('dp')
    core = lax.rem(my_dp, 2)
    bit_x = lax.rem(lax.div(my_dp, 2), 2)
    bit_y = lax.div(my_dp, 4)

    def z_peer(other):
        return (other, my_dp)

    def peer(name, other):
        if name == 'core':
            return my_z, my_dp + other - core
        if name == 'x':
            return my_z, my_dp + 2 * (other - bit_x)
        if name == 'y':
            return my_z, my_dp + 4 * (other - bit_y)
        if name == 'xy':
            return my_z, 2 * other + core
        if name == 'z':
            return other, my_dp
        low = lax.rem(my_z, 2)
        return (my_z - low + other if name == 'z0' else 2 * other + low), my_dp

    place = {'peer': peer, 'index': {
        'core': core, 'x': bit_x, 'y': bit_y, 'xy': 2 * bit_y + bit_x, 'z': my_z, 'z0': lax.rem(my_z, 2), 'z1': lax.div(my_z, 2)}}

    barrier = pltpu.get_barrier_semaphore()
    for name in ('core', 'xy', 'z'):
        for hop in range(1, GROUP[name]):
            device = peer(name, lax.rem(place['index'][name] + hop, GROUP[name]))
            pl.semaphore_signal(barrier, inc=1, device_id=device, device_id_type=MESH_ID)

    loads['single_s'].wait()
    loads['w_kv'].wait()
    s_wide = loaded['single_s'][...].astype(F32).reshape(ALL_ROWS, WIDTH)
    s_norm, s_inv = layer_norm(s_wide)
    act = s_norm.astype(BF)
    act_s[...] = act
    norm_s[...] = s_norm
    inv_s[...] = s_inv
    kv_local = dot_nn(act, loaded['w_kv'][...])
    pl.semaphore_wait(barrier, 7)
    kv_buf[my_z] = kv_local.reshape(CPLX, ROWS, 2 * WIDTH).astype(BF)

    def kv_copy(hop):
        return pltpu.make_async_remote_copy(
            src_ref=kv_buf.at[my_z], dst_ref=kv_buf.at[my_z], send_sem=kv_send.at[hop - 1], recv_sem=kv_recv.at[hop - 1],
            device_id=z_peer(lax.rem(my_z + hop, PEERS)), device_id_type=MESH_ID)

    for hop in range(1, PEERS):
        kv_copy(hop).start()

    for name in ('pair_z', 'w_pa', 'w_pb', 'w_po', 'w_bias'):
        loads[name].wait()
    block_rows = BLOCK_I * TOKENS
    fwd_rows = FWD_BLOCK_I * TOKENS

    @pl.loop(0, ALL_ROWS // FWD_BLOCK_I)
    def _(block):
        at = block * FWD_BLOCK_I
        z_wide = loaded['pair_z'][pl.ds(at, FWD_BLOCK_I)].reshape(fwd_rows, PAIR).astype(F32)
        normed, _ = layer_norm(z_wide)
        normed_bf = normed.astype(BF)
        half_a = 0.5 * dot_nn(normed_bf, loaded['w_pa'][...])
        hid_b = dot_nn(normed_bf, loaded['w_pb'][...])
        hidden = ((half_a * jnp.tanh(half_a) + half_a) * hid_b).astype(BF)
        z_new = (z_wide + dot_nn(hidden, loaded['w_po'][...])).astype(BF)
        new_rows[pl.ds(at, FWD_BLOCK_I)] = z_new.reshape(FWD_BLOCK_I, TOKENS, PAIR)
        bias_norm, _ = layer_norm(z_new.astype(F32))
        bias_bf = bias_norm.astype(BF)
        for row in range(FWD_BLOCK_I):
            bias_rows[at + row] = dot_nt(loaded['w_bias'][...], bias_bf[row * TOKENS:(row + 1) * TOKENS])

    for name in ('w_q', 'q_bias', 'w_g', 'token_mask', 'w_o', 'w_sa', 'w_sb', 'ds_out', 'w_so'):
        loads[name].wait()
    queries = (dot_nn(act_s[...], loaded['w_q'][...]) + loaded['q_bias'][...].astype(F32).reshape(1, WIDTH)).astype(BF).astype(F32)
    gate = sigmoid(dot_nn(act_s[...], loaded['w_g'][...]))
    lane_head = lax.broadcasted_iota(jnp.int32, (HEADS, WIDTH), 1)
    row_head = lax.broadcasted_iota(jnp.int32, (HEADS, WIDTH), 0)
    head_mask = jnp.where((lane_head >= row_head * HEAD_DIM) & (lane_head < (row_head + 1) * HEAD_DIM), 1.0, 0.0).astype(F32)

    def spread(rows):
        wide = jnp.broadcast_to(rows.reshape(ROWS, 1, WIDTH), (ROWS, HEADS, WIDTH)) * head_mask[None]
        return wide.reshape(ROWS * HEADS, WIDTH).astype(BF)

    def gather_heads(wide):
        return jnp.sum(wide.reshape(ROWS, HEADS, WIDTH) * head_mask[None], axis=1)

    for hop in range(1, PEERS):
        kv_copy(hop).wait()

    def keys_values(cplx):
        both = kv_buf[:, cplx].astype(F32).reshape(TOKENS, 2 * WIDTH).astype(BF)
        return both[:, :WIDTH], both[:, WIDTH:]

    key_mask = MASK_BIG * (loaded['token_mask'][...].astype(F32) - 1.0)
    attended_parts = []
    for cplx in range(CPLX):
        keys, values = keys_values(cplx)
        q_exp = spread(queries[cplx * ROWS:(cplx + 1) * ROWS])
        qexp_s[cplx] = q_exp
        bias = bias_rows[cplx * ROWS:(cplx + 1) * ROWS].reshape(ROWS * HEADS, TOKENS)
        logits = dot_nt(q_exp, keys) * SCALE + bias + key_mask[cplx:cplx + 1]
        top = jnp.max(logits, axis=-1, keepdims=True)
        expd = jnp.exp(logits - top)
        prob = expd / jnp.sum(expd, axis=-1, keepdims=True)
        prob_s[cplx] = prob
        attended_parts.append(gather_heads(dot_nn(prob.astype(BF), values)))
    attended = jnp.concatenate(attended_parts, axis=0)
    gated = (gate * attended).astype(BF)
    s_mid = (s_wide + dot_nn(gated, loaded['w_o'][...])).astype(BF)
    mid_norm, mid_inv = layer_norm(s_mid.astype(F32))
    mid_act = mid_norm.astype(BF)

    reducers = []
    for index in range(len(CHUNKS)):
        depth = len(LEVELS[CHUNK_KINDS[index]][0])
        reducers.append(Reducer(index, grads, total, got_refs[:depth], ar_send.at[index], ar_recv.at[index], place))
        del got_refs[:depth]

    def act_on(number):
        for chunk, step in ACTIONS[number]:
            if chunk < 0:
                (forward_kv_grad, finish_kv_grad)[step]()
            else:
                reducers[chunk].step(step)

    ds_wide = loaded['ds_out'][...].astype(F32).reshape(ALL_ROWS, WIDTH)
    ds_bf = ds_wide.astype(BF)
    grad_mid_norm = jnp.zeros((ALL_ROWS, WIDTH), F32)
    for piece in range(TRANS_S // PIECE):
        cols = slice(piece * PIECE, (piece + 1) * PIECE)
        base = piece * PIECE_TILES
        trans_a = dot_nn(mid_act, loaded['w_sa'][:, cols])
        trans_b = dot_nn(mid_act, loaded['w_sb'][:, cols])
        grad_hidden = dot_nt(ds_bf, loaded['w_so'][cols, :])
        hidden, grad_ta, grad_tb = swiglu_grad(trans_a, trans_b, grad_hidden)
        grad_ta = grad_ta.astype(BF)
        grad_tb = grad_tb.astype(BF)
        put_at(grads, base, dot_tn(hidden.astype(BF), ds_bf))
        put_at(grads, base + PIECE_TILES // 3, dot_tn(mid_act, grad_ta))
        put_at(grads, base + 2 * (PIECE_TILES // 3), dot_tn(mid_act, grad_tb))
        act_on(piece + 1)
        grad_mid_norm = grad_mid_norm + dot_nt(grad_ta, loaded['w_sa'][:, cols]) + dot_nt(grad_tb, loaded['w_sb'][:, cols])
    grad_mid = ds_wide + norm_grad(mid_norm, mid_inv, grad_mid_norm)
    gmid_s[...] = grad_mid
    grad_mid_bf = grad_mid.astype(BF)
    put_tiles(grads, 'o', dot_tn(gated, grad_mid_bf))
    grad_gated = dot_nt(grad_mid_bf, loaded['w_o'][...])
    grad_gate_pre = (grad_gated * attended * gate * (1.0 - gate)).astype(BF)
    ggp_s[...] = grad_gate_pre
    grad_att = (grad_gated * gate).astype(BF).astype(F32)
    grad_query_parts = []
    for cplx in range(CPLX):
        keys, values = keys_values(cplx)
        ga_exp = spread(grad_att[cplx * ROWS:(cplx + 1) * ROWS])
        prob = prob_s[cplx]
        grad_prob = dot_nt(ga_exp, values)
        grad_values = dot_tn(prob.astype(BF), ga_exp)
        grad_logits = (prob * (grad_prob - jnp.sum(prob * grad_prob, axis=-1, keepdims=True))).astype(BF)
        grad_bias[cplx * ROWS:(cplx + 1) * ROWS] = grad_logits.reshape(ROWS, HEADS, TOKENS)
        grad_query_parts.append(gather_heads(dot_nn(grad_logits, keys)) * SCALE)
        grad_keys = dot_tn(grad_logits, qexp_s[cplx]) * SCALE
        grad_keys = grad_keys.reshape(PEERS, ROWS, WIDTH).astype(BF)
        grad_values = grad_values.reshape(PEERS, ROWS, WIDTH).astype(BF)
        for owner in range(PEERS):
            gkv_buf[owner % 2, owner // 2, cplx, :, :WIDTH] = grad_keys[owner]
            gkv_buf[owner % 2, owner // 2, cplx, :, WIDTH:] = grad_values[owner]

    low, high = place['index']['z0'], place['index']['z1']

    def gkv_copy(step):
        src, dst = ((gkv_buf.at[1 - low], gkv_got1), (gkv_got1.at[1 - high], gkv_got2))[step]
        return pltpu.make_async_remote_copy(
            src_ref=src, dst_ref=dst, send_sem=gkv_send.at[step], recv_sem=gkv_recv.at[step],
            device_id=peer(*(('z0', 1 - low), ('z1', 1 - high))[step]), device_id_type=MESH_ID)

    gkv_copy(0).start()
    act_on(4)
    grad_query = jnp.concatenate(grad_query_parts, axis=0)
    grad_query_bf = grad_query.astype(BF)
    gq_s[...] = grad_query_bf
    put_tiles(grads, 'q', dot_tn(act_s[...], grad_query_bf))
    put_tiles(grads, 'g', dot_tn(act_s[...], grad_gate_pre))
    d_q_bias = jnp.sum(grad_query, axis=0, keepdims=True)
    row_index = lax.broadcasted_iota(jnp.int32, (16, 128), 0)
    bias_tile = jnp.zeros((16, 128), F32)
    for sub in range(3):
        bias_tile = jnp.where(row_index == sub, jnp.broadcast_to(d_q_bias[:, sub * 128:(sub + 1) * 128], (16, 128)), bias_tile)
    grads[1080] = bias_tile.astype(BF)
    grads[1081:1088] = jnp.zeros((7, 16, 128), BF)
    grads[1233:1280] = jnp.zeros((47, 16, 128), BF)

    def forward_kv_grad():
        gkv_copy(0).wait()
        gkv_got1[...] = (gkv_got1[...].astype(F32) + gkv_buf[low].astype(F32)).astype(BF)
        gkv_copy(1).start()

    def finish_kv_grad():
        gkv_copy(1).wait()
        summed = gkv_got1[high].astype(F32) + gkv_got2[...].astype(F32)
        grad_kv = summed.reshape(ALL_ROWS, 2 * WIDTH).astype(BF)
        gkv_s[...] = grad_kv
        put_tiles(grads, 'kv', dot_tn(act_s[...], grad_kv))

    def finish_single():
        grad_act = (dot_nt(gq_s[...], loaded['w_q'][...]) + dot_nt(gkv_s[...], loaded['w_kv'][...])
                    + dot_nt(ggp_s[...], loaded['w_g'][...]))
        grad_s = gmid_s[...] + norm_grad(norm_s[...], inv_s[...], grad_act)
        ds_in[...] = grad_s.reshape(CPLX, ROWS, WIDTH).astype(BF)

    loads['dz_out'].wait()
    acc_ab[...] = jnp.zeros_like(acc_ab)
    acc_po[...] = jnp.zeros_like(acc_po)
    acc_bias[...] = jnp.zeros_like(acc_bias)

    def act_in_loop(block, first):
        for tick in range(NUM_BLOCKS):
            if ACTIONS[first + tick]:
                @pl.when(block == tick)
                def _():
                    act_on(first + tick)

    @pl.loop(0, NUM_BLOCKS)
    def _(block):
        act_in_loop(block, FIRST_BLOCK)
        at = block * BLOCK_I
        bias_norm, bias_inv = layer_norm(new_rows[pl.ds(at, BLOCK_I)].reshape(block_rows, PAIR).astype(F32))
        bias_bf = bias_norm.astype(BF)
        bias_acc = acc_bias[...]
        parts = []
        for row in range(BLOCK_I):
            grad_row = grad_bias[at + row]
            bias_acc = bias_acc + dot_nn(grad_row, bias_bf[row * TOKENS:(row + 1) * TOKENS])
            parts.append(dot_tn(grad_row, loaded['w_bias'][...]))
        acc_bias[...] = bias_acc
        grad_norm = jnp.concatenate(parts, axis=0)
        dz_wide = loaded['dz_out'][pl.ds(at, BLOCK_I)].reshape(block_rows, PAIR).astype(F32)
        grad_new_bf = (dz_wide + norm_grad(bias_norm, bias_inv, grad_norm)).astype(BF)
        new_rows[pl.ds(at, BLOCK_I)] = grad_new_bf.reshape(BLOCK_I, TOKENS, PAIR)

    grads[SLOTS['bias'][0]] = acc_bias[...].astype(BF)

    @pl.loop(0, NUM_BLOCKS)
    def _(block):
        act_in_loop(block, MAIN_BLOCK)
        at = block * BLOCK_I
        grad_new_bf = new_rows[pl.ds(at, BLOCK_I)].reshape(block_rows, PAIR)
        normed, _ = layer_norm(loaded['pair_z'][pl.ds(at, BLOCK_I)].reshape(block_rows, PAIR).astype(F32))
        normed_bf = normed.astype(BF)
        hid_a = dot_nn(normed_bf, loaded['w_pa'][...])
        hid_b = dot_nn(normed_bf, loaded['w_pb'][...])
        grad_hidden = dot_nt(grad_new_bf, loaded['w_po'][...])
        hidden, grad_a, grad_b = swiglu_grad(hid_a, hid_b, grad_hidden)
        grad_a = grad_a.astype(BF)
        grad_b = grad_b.astype(BF)
        gab_s[block, :, :TRANS_P] = grad_a
        gab_s[block, :, TRANS_P:] = grad_b
        acc_po[...] += dot_tn(grad_new_bf, hidden.astype(BF))
        acc_ab[:, :TRANS_P] += dot_tn(normed_bf, grad_a)
        acc_ab[:, TRANS_P:] += dot_tn(normed_bf, grad_b)

    put_tiles(grads, 'pa', acc_ab[:, :TRANS_P])
    put_tiles(grads, 'pb', acc_ab[:, TRANS_P:])
    put_tiles(grads, 'po', jnp.transpose(acc_po[...]))
    act_on(SINGLE_END)
    finish_single()

    @pl.loop(0, NUM_BLOCKS)
    def _(block):
        act_in_loop(block, DZ_BLOCK)
        at = block * BLOCK_I
        normed, inv_std = layer_norm(loaded['pair_z'][pl.ds(at, BLOCK_I)].reshape(block_rows, PAIR).astype(F32))
        grad_normed = dot_nt(gab_s[block, :, :TRANS_P], loaded['w_pa'][...]) + dot_nt(gab_s[block, :, TRANS_P:], loaded['w_pb'][...])
        grad_new = new_rows[pl.ds(at, BLOCK_I)].reshape(block_rows, PAIR).astype(F32)
        result = grad_new + norm_grad(normed, inv_std, grad_normed)
        dz_in[pl.ds(at, BLOCK_I)] = result.reshape(BLOCK_I, TOKENS, PAIR).astype(BF)

    act_on(DZ_BLOCK + NUM_BLOCKS)
    for reducer in reducers:
        reducer.finish_sends()


GOT_COUNT = sum(len(LEVELS[kind][0]) for kind in CHUNK_KINDS)
MAX_STEPS = 2 * max(len(LEVELS[kind][0]) for kind in CHUNK_KINDS)


def run_main(inputs):
    any_spec = pl.BlockSpec(memory_space=pl.ANY)
    scratch = [pltpu.VMEM(value.shape, value.dtype) for value in inputs]
    scratch += [
        pltpu.VMEM((ALL_ROWS, TOKENS, PAIR), BF),
        pltpu.VMEM((ALL_ROWS, HEADS, TOKENS), F32),
        pltpu.VMEM((ALL_ROWS, HEADS, TOKENS), BF),
        pltpu.VMEM((PEERS, CPLX, ROWS, 2 * WIDTH), BF),
        pltpu.VMEM((2, 2, CPLX, ROWS, 2 * WIDTH), BF),
        pltpu.VMEM((2, CPLX, ROWS, 2 * WIDTH), BF),
        pltpu.VMEM((CPLX, ROWS, 2 * WIDTH), BF),
        pltpu.VMEM((ALL_ROWS, 2 * WIDTH), BF),
        pltpu.VMEM((PAIR, 2 * TRANS_P), F32),
        pltpu.VMEM((PAIR, TRANS_P), F32),
        pltpu.VMEM((HEADS, PAIR), F32),
        pltpu.VMEM((NUM_BLOCKS, BLOCK_I * TOKENS, 2 * TRANS_P), BF),
        pltpu.VMEM((ALL_ROWS, WIDTH), BF),
        pltpu.VMEM((ALL_ROWS, WIDTH), F32),
        pltpu.VMEM((ALL_ROWS, WIDTH), BF),
        pltpu.VMEM((ALL_ROWS, WIDTH), BF),
        pltpu.VMEM((ALL_ROWS, WIDTH), F32),
        pltpu.VMEM((ALL_ROWS, 1), F32),
        pltpu.VMEM((CPLX, ROWS * HEADS, TOKENS), F32),
        pltpu.VMEM((CPLX, ROWS * HEADS, WIDTH), BF),
        pltpu.VMEM((TILES, 16, 128), BF),
    ]
    for chunk, kind in enumerate(CHUNK_KINDS):
        for name, size in zip(LEVELS[kind][0], level_sizes(chunk)[1:]):
            scratch.append(pltpu.VMEM((len(LEVELS[kind]), GROUP[name] - 1, size, 16, 128), BF))
    dma = pltpu.SemaphoreType.DMA
    scratch += [dma((17,)), dma((3,)), dma((3,)), dma((2,)), dma((2,)), dma((len(CHUNKS),)), dma((len(CHUNKS), MAX_STEPS))]
    return pl.pallas_call(
        main_kernel,
        out_shape=(pltpu.VMEM((ALL_ROWS, TOKENS, PAIR), BF), pltpu.VMEM((CPLX, ROWS, WIDTH), BF), pltpu.VMEM((TILES, 16, 128), BF)),
        in_specs=[any_spec] * 17,
        out_specs=(pl.BlockSpec(memory_space=pltpu.VMEM),) * 3,
        scratch_shapes=scratch,
        compiler_params=pltpu.CompilerParams(collective_id=0, has_side_effects=True, vmem_limit_bytes=48 * 1024 * 1024),
        name='pairformer_tail',
    )(*(pltpu.with_memory_space_constraint(value, pltpu.HBM) for value in inputs))


UNPACK = ('pa', 'pb', 'po', 'bias', 'q', 'qb', 'kv', 'g', 'o', 'sa', 'sb', 'so')


def unpack_kernel(tiles, dz_buf, ds_buf, *refs):
    outs = dict(zip(UNPACK, refs[:12]))
    dz_out, ds_out = refs[12:14]
    stages = dict(zip(UNPACK, refs[14:26]))
    sem, pass_sem = refs[26:]
    copies = []
    for index, (buf, dst) in enumerate(((dz_buf, dz_out), (ds_buf, ds_out))):
        made = pltpu.make_async_copy(buf, dst, pass_sem.at[index])
        made.start()
        copies.append(made)

    def widen(stage, base, rows, row, cols, col):
        per_col = rows // 16
        for sub in range(cols // 128):
            part = tiles[base + sub * per_col:base + (sub + 1) * per_col].astype(F32)
            stage[row:row + rows, col + sub * 128:col + (sub + 1) * 128] = part.reshape(rows, 128)

    def send(name):
        made = pltpu.make_async_copy(stages[name], outs[name], sem.at[UNPACK.index(name)])
        made.start()
        copies.append(made)

    for name in ('kv', 'o', 'q', 'g', 'pa', 'pb', 'po', 'bias', 'qb'):
        base, rows, cols = SLOTS[name]
        if name == 'qb':
            last_tile = tiles[base].astype(F32)
            for sub in range(3):
                stages[name][pl.ds(sub * 128, 128)] = last_tile[sub]
        else:
            widen(stages[name], base, rows, 0, cols, 0)
        send(name)
    for piece in range(TRANS_S // PIECE):
        base = piece * PIECE_TILES
        third = PIECE_TILES // 3
        widen(stages['so'], base, PIECE, piece * PIECE, WIDTH, 0)
        widen(stages['sa'], base + third, WIDTH, 0, PIECE, piece * PIECE)
        widen(stages['sb'], base + 2 * third, WIDTH, 0, PIECE, piece * PIECE)
    for name in ('so', 'sa', 'sb'):
        send(name)
    for copy in copies:
        copy.wait()


def run_unpack(tiles, dz_in, ds_in):
    shapes = [(WIDTH,) if name == 'qb' else (TRANS_S, WIDTH) if name == 'so' else (WIDTH, TRANS_S) if name in ('sa', 'sb')
              else SLOTS[name][1:] for name in UNPACK]
    any_spec = pl.BlockSpec(memory_space=pl.ANY)
    return pl.pallas_call(
        unpack_kernel,
        out_shape=tuple(jax.ShapeDtypeStruct(shape, F32) for shape in shapes) + (
            jax.ShapeDtypeStruct(dz_in.shape, BF), jax.ShapeDtypeStruct(ds_in.shape, BF)),
        in_specs=[pl.BlockSpec(memory_space=pltpu.VMEM)] * 3,
        out_specs=(any_spec,) * 14,
        scratch_shapes=[pltpu.VMEM(shape, F32) for shape in shapes] + [
            pltpu.SemaphoreType.DMA((12,)), pltpu.SemaphoreType.DMA((2,))],
        compiler_params=pltpu.CompilerParams(vmem_limit_bytes=24 * 1024 * 1024),
        name='unpack_sums',
    )(*(pltpu.with_memory_space_constraint(value, pltpu.VMEM) for value in (tiles, dz_in, ds_in)))


def solution(mesh):
    pair_spec = P('dp', 'dap', None, None)
    single_spec = P('dp', 'dap', None)

    def body(pair_z, single_s, token_mask, dz_out, ds_out, w_pa, w_pb, w_po, w_bias, w_q, q_bias, w_kv, w_g, w_o, w_sa, w_sb, w_so):
        inputs = (pair_z.reshape(ALL_ROWS, TOKENS, PAIR), single_s, token_mask, dz_out.reshape(ALL_ROWS, TOKENS, PAIR), ds_out,
                  w_pa, w_pb, w_po, w_bias.T, w_q, q_bias, w_kv, w_g, w_o, w_sa, w_sb, w_so)
        dz_in, ds_in, tiles = run_main(inputs)
        *sums, dz_in, ds_in = run_unpack(tiles, dz_in, ds_in)
        sums[3] = sums[3].T
        return (dz_in.reshape(pair_z.shape), ds_in) + tuple(sums)

    in_specs = (pair_spec, single_spec, P('dp', None), pair_spec, single_spec) + (P(),) * 12
    out_specs = (pair_spec, single_spec) + (P(),) * 12
    return jax.shard_map(body, mesh=mesh, in_specs=in_specs, out_specs=out_specs, check_vma=False)
```

```python
import math
import jax
import jax.numpy as jnp
from jax import lax
from jax.experimental import pallas as pl
from jax.experimental.pallas import tpu as pltpu
from jax.sharding import PartitionSpec as P

HEAD_DIM = 24
HEADS = 16
WIDTH = 384
TRANS_S = 1536
PAIR = 128
TRANS_P = 512
TOKENS = 96
ROWS = 24
CPLX = 3
ALL_ROWS = CPLX * ROWS
SCALE = HEAD_DIM ** -0.5
EPSILON = 1e-5
MASK_BIG = 1e9
PEERS = 4
MESH_ID = pl.DeviceIdType.MESH
BF = jnp.bfloat16
F32 = jnp.float32

PIECE = 512
PIECE_TILES = 288
SLOTS = {
    'o': (864, 384, 384),
    'q': (936, 384, 384), 'g': (1008, 384, 384), 'qb': (1080, 16, 128), 'kv': (1088, 384, 768),
    'pa': (1280, 128, 512), 'pb': (1312, 128, 512), 'po': (1344, 512, 128), 'bias': (1232, 16, 128),
}
CHUNK = 128
LOCAL_END, PAIR_START, TILES = 1088, 1280, 1376
CHUNKS = tuple((base, min(CHUNK, LOCAL_END - base)) for base in range(0, LOCAL_END, CHUNK)) + (
    (LOCAL_END, PAIR_START - LOCAL_END), (PAIR_START, TILES - PAIR_START))
KV_CHUNK, PAIR_CHUNK = len(CHUNKS) - 2, len(CHUNKS) - 1
BLOCK_I = 4
NUM_BLOCKS = ALL_ROWS // BLOCK_I
FWD_BLOCK_I = 12

CHUNK_KINDS = 'amaaamaaaap'
LEVELS = {
    'a': (('core', 'x', 'y', 'z'), ('core', 'y', 'x', 'z')),
    'h': (('core', 'x', 'y', 'z0', 'z1'), ('core', 'y', 'x', 'z0', 'z1')),
    'f': (('core', 'z0', 'x', 'y', 'z1'), ('core', 'z0', 'y', 'x', 'z1')),
    'm': (('core', 'x', 'z0', 'y', 'z1'), ('core', 'y', 'z0', 'x', 'z1')),
    'n': (('core', 'x', 'z0', 'z1', 'y'), ('core', 'y', 'z0', 'z1', 'x')),
    'p': (('core', 'xy', 'z'),),
}
GROUP = {'core': 2, 'x': 2, 'y': 2, 'z': 4, 'z0': 2, 'z1': 2, 'xy': 4}

LINK_US = {
    'core': {'core': 0.003}, 'x': {'x': 0.0757}, 'y': {'y': 0.0757}, 'xy': {'x': 0.1514, 'y': 0.1514},
    'z': {'mid': 0.3024, 'end': 0.2268}, 'z0': {'end': 0.0756}, 'z1': {'mid': 0.1512, 'end': 0.0756},
}
LATENCY_US = {'core': 0.85, 'x': 3.5, 'y': 3.2, 'z': 4.15, 'z0': 3.4, 'z1': 3.9, 'xy': 3.8}
KV_LINK_US = ({'end': 4.1}, {'mid': 4.1, 'end': 2.05})
BACKLOG_US = 2.0
FIRST_BLOCK = 5
PAIR_END = FIRST_BLOCK + NUM_BLOCKS
DZ_BLOCK = PAIR_END + 1
SEGMENT_US = (1.0, 1.0, 1.0, 2.1, 1.1) + (1.22,) * NUM_BLOCKS + (0.65,) + (0.4,) * NUM_BLOCKS
SEGMENT_TILES = (288, 576, 864, 936, LOCAL_END)
KV_SEGMENT = 3


def level_sizes(chunk):
    sizes = [CHUNKS[chunk][1] // len(LEVELS[CHUNK_KINDS[chunk]])]
    for name in LEVELS[CHUNK_KINDS[chunk]][0]:
        sizes.append(sizes[-1] // GROUP[name])
    return sizes


def plan_actions():
    stage = [0] * len(CHUNKS)
    due = {}
    free = {}
    actions = [[] for _ in range(len(SEGMENT_US) + 1)]
    now, segment, kv_due, kv_step = 0.0, 0, None, 0

    def steps(chunk):
        return 2 * len(LEVELS[CHUNK_KINDS[chunk]][0])

    def occupy(links, start):
        ends = []
        for link, time in links.items():
            free[link] = max(free.get(link, 0.0), start) + time
            ends.append(free[link])
        return max(ends)

    def when(chunk):
        step, half = stage[chunk], steps(chunk) // 2
        if step > 2 * half:
            return None
        time = due.get(chunk, 0.0)
        if step == 0:
            if chunk == PAIR_CHUNK:
                able = segment >= PAIR_END
            elif chunk == KV_CHUNK:
                able = kv_step == 2
            else:
                end = sum(CHUNKS[chunk])
                able = segment > next(index for index, tiles in enumerate(SEGMENT_TILES) if end <= tiles)
            if not able:
                return None
        if step < 2 * half and chunk != PAIR_CHUNK:
            for names in LEVELS[CHUNK_KINDS[chunk]]:
                for link in LINK_US[names[min(step, 2 * half - 1 - step)]]:
                    time = max(time, free.get(link, 0.0) - BACKLOG_US)
        return time

    while True:
        if kv_due is not None and kv_due <= now and kv_step < 2:
            actions[segment].append((-1, kv_step))
            kv_step += 1
            now += 0.3
            kv_due = occupy(KV_LINK_US[1], now) + LATENCY_US['z1'] if kv_step == 1 else None
            continue
        times = {chunk: when(chunk) for chunk in range(len(CHUNKS))}
        times = {chunk: time for chunk, time in times.items() if time is not None}
        waiting = [chunk for chunk, time in times.items() if time <= now]
        if waiting:
            chunk = min(waiting, key=lambda one: (one != PAIR_CHUNK, one))
            step = stage[chunk]
            actions[segment].append((chunk, step))
            half = steps(chunk) // 2
            sizes = level_sizes(chunk)
            now += 0.015 + (0.0017 * len(LEVELS[CHUNK_KINDS[chunk]]) * sizes[step] if 0 < step <= half else 0.0)
            if step < 2 * half:
                level = min(step, 2 * half - 1 - step)
                ends = []
                for names in LEVELS[CHUNK_KINDS[chunk]]:
                    name = names[level]
                    links = {link: time * sizes[level + 1] for link, time in LINK_US[name].items()}
                    ends.append(occupy(links, now) + LATENCY_US[name])
                due[chunk] = max(ends)
            stage[chunk] = step + 1
        elif segment < len(SEGMENT_US):
            now += SEGMENT_US[segment]
            if segment == KV_SEGMENT:
                kv_due = occupy(KV_LINK_US[0], now) + LATENCY_US['z0']
            segment += 1
        else:
            later = list(times.values()) + [kv_due] * (kv_due is not None)
            if not later:
                return actions
            now = max(now, min(later))


ACTIONS = plan_actions()


def dot_nn(left, right):
    return lax.dot_general(left, right, (((1,), (0,)), ((), ())), preferred_element_type=F32)


def dot_nt(left, right):
    return lax.dot_general(left, right, (((1,), (1,)), ((), ())), preferred_element_type=F32)


def dot_tn(left, right):
    return lax.dot_general(left, right, (((0,), (0,)), ((), ())), preferred_element_type=F32)


def layer_norm(wide):
    centred = wide - jnp.mean(wide, axis=-1, keepdims=True)
    inv_std = lax.rsqrt(jnp.mean(centred * centred, axis=-1, keepdims=True) + EPSILON)
    return centred * inv_std, inv_std


def norm_grad(normed, inv_std, grad_out):
    mean_grad = jnp.mean(grad_out, axis=-1, keepdims=True)
    mean_proj = jnp.mean(grad_out * normed, axis=-1, keepdims=True)
    return inv_std * (grad_out - mean_grad - normed * mean_proj)


def sigmoid(values):
    return 0.5 * jnp.tanh(0.5 * values) + 0.5


def swiglu_grad(hid_a, hid_b, grad_hidden):
    half_a = 0.5 * hid_a
    tanh_a = jnp.tanh(half_a)
    sig_a = 0.5 * tanh_a + 0.5
    silu_a = half_a * tanh_a + half_a
    grad_a = (grad_hidden * hid_b) * (sig_a + silu_a * (1.0 - sig_a))
    return silu_a * hid_b, grad_a, grad_hidden * silu_a


def put_at(grads, base, value):
    per_col = value.shape[0] // 16
    for col in range(value.shape[1] // 128):
        start = base + col * per_col
        grads[start:start + per_col] = value[:, col * 128:(col + 1) * 128].reshape(per_col, 16, 128).astype(BF)


def put_tiles(grads, name, value):
    put_at(grads, SLOTS[name][0], value)


class Reducer:
    def __init__(self, chunk, grads, total, got, send_sem, recv_sem, place):
        self.chunk = chunk
        self.grads, self.total, self.got = grads, total, got
        self.send_sem, self.recv_sem = send_sem, recv_sem
        self.place = place
        self.levels = LEVELS[CHUNK_KINDS[chunk]]
        self.sizes = level_sizes(chunk)
        self.depth = len(self.levels[0])

    def kept(self, part, level):
        at = CHUNKS[self.chunk][0] + part * self.sizes[0]
        for name, size in zip(self.levels[part][:level], self.sizes[1:]):
            at = at + self.place['index'][name] * size
        return at

    def held(self, part, level, start, count):
        if level == 0:
            return self.grads.at[pl.ds(self.kept(part, 0) + start, count)]
        return self.got[level - 1].at[part, 0, pl.ds(start, count)]

    def start(self, step):
        level = min(step, 2 * self.depth - 1 - step)
        size = self.sizes[level + 1]
        for part in range(len(self.levels)):
            name = self.levels[part][level]
            group = GROUP[name]
            for hop in range(1, group):
                other = lax.rem(self.place['index'][name] + hop, group)
                if step < self.depth:
                    src, dst = self.held(part, level, other * size, size), self.got[level].at[part, hop - 1]
                else:
                    src = dst = self.total.at[pl.ds(self.kept(part, level + 1), size)]
                pltpu.make_async_remote_copy(
                    src_ref=src, dst_ref=dst, send_sem=self.send_sem, recv_sem=self.recv_sem.at[step],
                    device_id=self.place['peer'](name, other), device_id_type=MESH_ID).start()

    def moved(self, level):
        return len(self.levels) * (GROUP[self.levels[0][level]] - 1) * self.sizes[level + 1]

    def wait_tiles(self, count, sem):
        span = self.grads.at[pl.ds(0, count)]
        pltpu.make_async_copy(span, span, sem).wait()

    def add(self, level):
        size = self.sizes[level + 1]
        for part in range(len(self.levels)):
            name = self.levels[part][level]
            own = self.held(part, level, self.place['index'][name] * size, size)
            slots = [self.got[level].at[part, hop] for hop in range(GROUP[name] - 1)]
            dst = slots[0] if level + 1 < self.depth else self.total.at[pl.ds(self.kept(part, level + 1), size)]
            add_into(dst, [own] + slots, size)

    def step(self, step):
        if step:
            level = min(step - 1, 2 * self.depth - step)
            self.wait_tiles(self.moved(level), self.recv_sem.at[step - 1])
        if 0 < step <= self.depth:
            self.add(step - 1)
        if step < 2 * self.depth:
            self.start(step)

    def finish_sends(self):
        self.wait_tiles(2 * sum(self.moved(level) for level in range(self.depth)), self.send_sem)


def add_into(dst, terms, count):
    step = math.gcd(count, 8)

    @pl.loop(0, count // step)
    def _(index):
        at = pl.ds(index * step, step)
        total = terms[0][at].astype(F32)
        for term in terms[1:]:
            total = total + term[at].astype(F32)
        dst[at] = total.astype(BF)


def main_kernel(*refs):
    names = ('pair_z', 'single_s', 'token_mask', 'dz_out', 'ds_out', 'w_pa', 'w_pb', 'w_po', 'w_bias', 'w_q', 'q_bias',
             'w_kv', 'w_g', 'w_o', 'w_sa', 'w_sb', 'w_so')
    hbm = dict(zip(names, refs[:17]))
    dz_in, ds_in, total = refs[17:20]
    scratch = refs[20:]
    loaded = dict(zip(names, scratch[:17]))
    (new_rows, norm_rows, bias_rows, grad_bias, kv_buf, gkv_buf, gkv_got1, gkv_got2, gkv_s, acc_ab, acc_po, acc_bias, gab_s, act_s, norm_s, gq_s, ggp_s,
     gmid_s, inv_s, prob_s, qexp_s, grads) = scratch[17:39]
    got_refs = list(scratch[39:39 + GOT_COUNT])
    load_sem, kv_send, kv_recv, gkv_send, gkv_recv, ar_send, ar_recv = scratch[39 + GOT_COUNT:]

    order = ('single_s', 'w_kv', 'pair_z', 'w_pa', 'w_pb', 'w_po', 'w_bias', 'w_q', 'q_bias', 'w_g', 'token_mask', 'w_o', 'w_sa',
             'w_sb', 'ds_out', 'w_so', 'dz_out')
    loads = {}
    for index, name in enumerate(order):
        loads[name] = pltpu.make_async_copy(hbm[name], loaded[name], load_sem.at[index])
        loads[name].start()

    my_z = lax.axis_index('dap')
    my_dp = lax.axis_index('dp')
    core = lax.rem(my_dp, 2)
    bit_x = lax.rem(lax.div(my_dp, 2), 2)
    bit_y = lax.div(my_dp, 4)

    def z_peer(other):
        return (other, my_dp)

    def peer(name, other):
        if name == 'core':
            return my_z, my_dp + other - core
        if name == 'x':
            return my_z, my_dp + 2 * (other - bit_x)
        if name == 'y':
            return my_z, my_dp + 4 * (other - bit_y)
        if name == 'xy':
            return my_z, 2 * other + core
        if name == 'z':
            return other, my_dp
        low = lax.rem(my_z, 2)
        return (my_z - low + other if name == 'z0' else 2 * other + low), my_dp

    place = {'peer': peer, 'index': {
        'core': core, 'x': bit_x, 'y': bit_y, 'xy': 2 * bit_y + bit_x, 'z': my_z, 'z0': lax.rem(my_z, 2), 'z1': lax.div(my_z, 2)}}

    barrier = pltpu.get_barrier_semaphore()
    for name in ('core', 'xy', 'z'):
        for hop in range(1, GROUP[name]):
            device = peer(name, lax.rem(place['index'][name] + hop, GROUP[name]))
            pl.semaphore_signal(barrier, inc=1, device_id=device, device_id_type=MESH_ID)

    loads['single_s'].wait()
    loads['w_kv'].wait()
    s_wide = loaded['single_s'][...].astype(F32).reshape(ALL_ROWS, WIDTH)
    s_norm, s_inv = layer_norm(s_wide)
    act = s_norm.astype(BF)
    act_s[...] = act
    norm_s[...] = s_norm
    inv_s[...] = s_inv
    kv_local = dot_nn(act, loaded['w_kv'][...])
    pl.semaphore_wait(barrier, 7)
    kv_buf[my_z] = kv_local.reshape(CPLX, ROWS, 2 * WIDTH).astype(BF)

    def kv_copy(hop):
        return pltpu.make_async_remote_copy(
            src_ref=kv_buf.at[my_z], dst_ref=kv_buf.at[my_z], send_sem=kv_send.at[hop - 1], recv_sem=kv_recv.at[hop - 1],
            device_id=z_peer(lax.rem(my_z + hop, PEERS)), device_id_type=MESH_ID)

    for hop in range(1, PEERS):
        kv_copy(hop).start()

    for name in ('pair_z', 'w_pa', 'w_pb', 'w_po', 'w_bias'):
        loads[name].wait()
    block_rows = BLOCK_I * TOKENS
    fwd_rows = FWD_BLOCK_I * TOKENS

    @pl.loop(0, ALL_ROWS // FWD_BLOCK_I)
    def _(block):
        at = block * FWD_BLOCK_I
        z_wide = loaded['pair_z'][pl.ds(at, FWD_BLOCK_I)].reshape(fwd_rows, PAIR).astype(F32)
        normed, _ = layer_norm(z_wide)
        normed_bf = normed.astype(BF)
        half_a = 0.5 * dot_nn(normed_bf, loaded['w_pa'][...])
        hid_b = dot_nn(normed_bf, loaded['w_pb'][...])
        hidden = ((half_a * jnp.tanh(half_a) + half_a) * hid_b).astype(BF)
        z_new = (z_wide + dot_nn(hidden, loaded['w_po'][...])).astype(BF)
        new_rows[pl.ds(at, FWD_BLOCK_I)] = z_new.reshape(FWD_BLOCK_I, TOKENS, PAIR)
        bias_norm, _ = layer_norm(z_new.astype(F32))
        bias_bf = bias_norm.astype(BF)
        norm_rows[pl.ds(at, FWD_BLOCK_I)] = bias_bf.reshape(FWD_BLOCK_I, TOKENS, PAIR)
        for row in range(FWD_BLOCK_I):
            bias_rows[at + row] = dot_nt(loaded['w_bias'][...], bias_bf[row * TOKENS:(row + 1) * TOKENS])

    for name in ('w_q', 'q_bias', 'w_g', 'token_mask', 'w_o', 'w_sa', 'w_sb', 'ds_out', 'w_so'):
        loads[name].wait()
    queries = (dot_nn(act_s[...], loaded['w_q'][...]) + loaded['q_bias'][...].astype(F32).reshape(1, WIDTH)).astype(BF).astype(F32)
    gate = sigmoid(dot_nn(act_s[...], loaded['w_g'][...]))
    lane_head = lax.broadcasted_iota(jnp.int32, (HEADS, WIDTH), 1)
    row_head = lax.broadcasted_iota(jnp.int32, (HEADS, WIDTH), 0)
    head_mask = jnp.where((lane_head >= row_head * HEAD_DIM) & (lane_head < (row_head + 1) * HEAD_DIM), 1.0, 0.0).astype(F32)

    def spread(rows):
        wide = jnp.broadcast_to(rows.reshape(ROWS, 1, WIDTH), (ROWS, HEADS, WIDTH)) * head_mask[None]
        return wide.reshape(ROWS * HEADS, WIDTH).astype(BF)

    def gather_heads(wide):
        return jnp.sum(wide.reshape(ROWS, HEADS, WIDTH) * head_mask[None], axis=1)

    for hop in range(1, PEERS):
        kv_copy(hop).wait()

    def keys_values(cplx):
        both = kv_buf[:, cplx].astype(F32).reshape(TOKENS, 2 * WIDTH).astype(BF)
        return both[:, :WIDTH], both[:, WIDTH:]

    key_mask = MASK_BIG * (loaded['token_mask'][...].astype(F32) - 1.0)
    attended_parts = []
    for cplx in range(CPLX):
        keys, values = keys_values(cplx)
        q_exp = spread(queries[cplx * ROWS:(cplx + 1) * ROWS])
        qexp_s[cplx] = q_exp
        bias = bias_rows[cplx * ROWS:(cplx + 1) * ROWS].reshape(ROWS * HEADS, TOKENS)
        logits = dot_nt(q_exp, keys) * SCALE + bias + key_mask[cplx:cplx + 1]
        top = jnp.max(logits, axis=-1, keepdims=True)
        expd = jnp.exp(logits - top)
        prob = expd / jnp.sum(expd, axis=-1, keepdims=True)
        prob_s[cplx] = prob
        attended_parts.append(gather_heads(dot_nn(prob.astype(BF), values)))
    attended = jnp.concatenate(attended_parts, axis=0)
    gated = (gate * attended).astype(BF)
    s_mid = (s_wide + dot_nn(gated, loaded['w_o'][...])).astype(BF)
    mid_norm, mid_inv = layer_norm(s_mid.astype(F32))
    mid_act = mid_norm.astype(BF)

    reducers = []
    for index in range(len(CHUNKS)):
        depth = len(LEVELS[CHUNK_KINDS[index]][0])
        reducers.append(Reducer(index, grads, total, got_refs[:depth], ar_send.at[index], ar_recv.at[index], place))
        del got_refs[:depth]

    def act_on(number):
        for chunk, step in ACTIONS[number]:
            if chunk < 0:
                (forward_kv_grad, finish_kv_grad)[step]()
            else:
                reducers[chunk].step(step)

    ds_wide = loaded['ds_out'][...].astype(F32).reshape(ALL_ROWS, WIDTH)
    ds_bf = ds_wide.astype(BF)
    grad_mid_norm = jnp.zeros((ALL_ROWS, WIDTH), F32)
    for piece in range(TRANS_S // PIECE):
        cols = slice(piece * PIECE, (piece + 1) * PIECE)
        base = piece * PIECE_TILES
        trans_a = dot_nn(mid_act, loaded['w_sa'][:, cols])
        trans_b = dot_nn(mid_act, loaded['w_sb'][:, cols])
        grad_hidden = dot_nt(ds_bf, loaded['w_so'][cols, :])
        hidden, grad_ta, grad_tb = swiglu_grad(trans_a, trans_b, grad_hidden)
        grad_ta = grad_ta.astype(BF)
        grad_tb = grad_tb.astype(BF)
        put_at(grads, base, dot_tn(hidden.astype(BF), ds_bf))
        put_at(grads, base + PIECE_TILES // 3, dot_tn(mid_act, grad_ta))
        put_at(grads, base + 2 * (PIECE_TILES // 3), dot_tn(mid_act, grad_tb))
        act_on(piece + 1)
        grad_mid_norm = grad_mid_norm + dot_nt(grad_ta, loaded['w_sa'][:, cols]) + dot_nt(grad_tb, loaded['w_sb'][:, cols])
    grad_mid = ds_wide + norm_grad(mid_norm, mid_inv, grad_mid_norm)
    gmid_s[...] = grad_mid
    grad_mid_bf = grad_mid.astype(BF)
    put_tiles(grads, 'o', dot_tn(gated, grad_mid_bf))
    grad_gated = dot_nt(grad_mid_bf, loaded['w_o'][...])
    grad_gate_pre = (grad_gated * attended * gate * (1.0 - gate)).astype(BF)
    ggp_s[...] = grad_gate_pre
    grad_att = (grad_gated * gate).astype(BF).astype(F32)
    grad_query_parts = []
    for cplx in range(CPLX):
        keys, values = keys_values(cplx)
        ga_exp = spread(grad_att[cplx * ROWS:(cplx + 1) * ROWS])
        prob = prob_s[cplx]
        grad_prob = dot_nt(ga_exp, values)
        grad_values = dot_tn(prob.astype(BF), ga_exp)
        grad_logits = (prob * (grad_prob - jnp.sum(prob * grad_prob, axis=-1, keepdims=True))).astype(BF)
        grad_bias[cplx * ROWS:(cplx + 1) * ROWS] = grad_logits.reshape(ROWS, HEADS, TOKENS)
        grad_query_parts.append(gather_heads(dot_nn(grad_logits, keys)) * SCALE)
        grad_keys = dot_tn(grad_logits, qexp_s[cplx]) * SCALE
        grad_keys = grad_keys.reshape(PEERS, ROWS, WIDTH).astype(BF)
        grad_values = grad_values.reshape(PEERS, ROWS, WIDTH).astype(BF)
        for owner in range(PEERS):
            gkv_buf[owner % 2, owner // 2, cplx, :, :WIDTH] = grad_keys[owner]
            gkv_buf[owner % 2, owner // 2, cplx, :, WIDTH:] = grad_values[owner]

    low, high = place['index']['z0'], place['index']['z1']

    def gkv_copy(step):
        src, dst = ((gkv_buf.at[1 - low], gkv_got1), (gkv_got1.at[1 - high], gkv_got2))[step]
        return pltpu.make_async_remote_copy(
            src_ref=src, dst_ref=dst, send_sem=gkv_send.at[step], recv_sem=gkv_recv.at[step],
            device_id=peer(*(('z0', 1 - low), ('z1', 1 - high))[step]), device_id_type=MESH_ID)

    gkv_copy(0).start()
    act_on(4)
    grad_query = jnp.concatenate(grad_query_parts, axis=0)
    grad_query_bf = grad_query.astype(BF)
    gq_s[...] = grad_query_bf
    put_tiles(grads, 'q', dot_tn(act_s[...], grad_query_bf))
    put_tiles(grads, 'g', dot_tn(act_s[...], grad_gate_pre))
    d_q_bias = jnp.sum(grad_query, axis=0, keepdims=True)
    row_index = lax.broadcasted_iota(jnp.int32, (16, 128), 0)
    bias_tile = jnp.zeros((16, 128), F32)
    for sub in range(3):
        bias_tile = jnp.where(row_index == sub, jnp.broadcast_to(d_q_bias[:, sub * 128:(sub + 1) * 128], (16, 128)), bias_tile)
    grads[1080] = bias_tile.astype(BF)
    grads[1081:1088] = jnp.zeros((7, 16, 128), BF)
    grads[1233:1280] = jnp.zeros((47, 16, 128), BF)

    def forward_kv_grad():
        gkv_copy(0).wait()
        gkv_got1[...] = (gkv_got1[...].astype(F32) + gkv_buf[low].astype(F32)).astype(BF)
        gkv_copy(1).start()

    def finish_kv_grad():
        gkv_copy(1).wait()
        summed = gkv_got1[high].astype(F32) + gkv_got2[...].astype(F32)
        grad_kv = summed.reshape(ALL_ROWS, 2 * WIDTH).astype(BF)
        gkv_s[...] = grad_kv
        put_tiles(grads, 'kv', dot_tn(act_s[...], grad_kv))

    def finish_single():
        grad_act = (dot_nt(gq_s[...], loaded['w_q'][...]) + dot_nt(gkv_s[...], loaded['w_kv'][...])
                    + dot_nt(ggp_s[...], loaded['w_g'][...]))
        grad_s = gmid_s[...] + norm_grad(norm_s[...], inv_s[...], grad_act)
        ds_in[...] = grad_s.reshape(CPLX, ROWS, WIDTH).astype(BF)

    loads['dz_out'].wait()
    acc_ab[...] = jnp.zeros_like(acc_ab)
    acc_po[...] = jnp.zeros_like(acc_po)
    acc_bias[...] = jnp.zeros_like(acc_bias)

    @pl.loop(0, NUM_BLOCKS)
    def _(block):
        total_bias = acc_bias[...]
        for row in range(BLOCK_I):
            total_bias = total_bias + dot_nn(grad_bias[block * BLOCK_I + row], norm_rows[block * BLOCK_I + row])
        acc_bias[...] = total_bias

    grads[SLOTS['bias'][0]] = acc_bias[...].astype(BF)

    def act_in_loop(block, first):
        for tick in range(NUM_BLOCKS):
            if ACTIONS[first + tick]:
                @pl.when(block == tick)
                def _():
                    act_on(first + tick)

    @pl.loop(0, NUM_BLOCKS)
    def _(block):
        act_in_loop(block, FIRST_BLOCK)
        at = block * BLOCK_I
        bias_norm, bias_inv = layer_norm(new_rows[pl.ds(at, BLOCK_I)].reshape(block_rows, PAIR).astype(F32))
        parts = [dot_tn(grad_bias[at + row], loaded['w_bias'][...]) for row in range(BLOCK_I)]
        grad_norm = jnp.concatenate(parts, axis=0)
        dz_wide = loaded['dz_out'][pl.ds(at, BLOCK_I)].reshape(block_rows, PAIR).astype(F32)
        grad_new_bf = (dz_wide + norm_grad(bias_norm, bias_inv, grad_norm)).astype(BF)
        new_rows[pl.ds(at, BLOCK_I)] = grad_new_bf.reshape(BLOCK_I, TOKENS, PAIR)
        normed, _ = layer_norm(loaded['pair_z'][pl.ds(at, BLOCK_I)].reshape(block_rows, PAIR).astype(F32))
        normed_bf = normed.astype(BF)
        hid_a = dot_nn(normed_bf, loaded['w_pa'][...])
        hid_b = dot_nn(normed_bf, loaded['w_pb'][...])
        grad_hidden = dot_nt(grad_new_bf, loaded['w_po'][...])
        hidden, grad_a, grad_b = swiglu_grad(hid_a, hid_b, grad_hidden)
        grad_a = grad_a.astype(BF)
        grad_b = grad_b.astype(BF)
        gab_s[block, :, :TRANS_P] = grad_a
        gab_s[block, :, TRANS_P:] = grad_b
        acc_po[...] += dot_tn(grad_new_bf, hidden.astype(BF))
        acc_ab[:, :TRANS_P] += dot_tn(normed_bf, grad_a)
        acc_ab[:, TRANS_P:] += dot_tn(normed_bf, grad_b)

    put_tiles(grads, 'pa', acc_ab[:, :TRANS_P])
    put_tiles(grads, 'pb', acc_ab[:, TRANS_P:])
    put_tiles(grads, 'po', jnp.transpose(acc_po[...]))
    act_on(PAIR_END)
    finish_single()

    @pl.loop(0, NUM_BLOCKS)
    def _(block):
        act_in_loop(block, DZ_BLOCK)
        at = block * BLOCK_I
        normed, inv_std = layer_norm(loaded['pair_z'][pl.ds(at, BLOCK_I)].reshape(block_rows, PAIR).astype(F32))
        grad_normed = dot_nt(gab_s[block, :, :TRANS_P], loaded['w_pa'][...]) + dot_nt(gab_s[block, :, TRANS_P:], loaded['w_pb'][...])
        grad_new = new_rows[pl.ds(at, BLOCK_I)].reshape(block_rows, PAIR).astype(F32)
        result = grad_new + norm_grad(normed, inv_std, grad_normed)
        dz_in[pl.ds(at, BLOCK_I)] = result.reshape(BLOCK_I, TOKENS, PAIR).astype(BF)

    act_on(DZ_BLOCK + NUM_BLOCKS)
    for reducer in reducers:
        reducer.finish_sends()


GOT_COUNT = sum(len(LEVELS[kind][0]) for kind in CHUNK_KINDS)
MAX_STEPS = 2 * max(len(LEVELS[kind][0]) for kind in CHUNK_KINDS)


def run_main(inputs):
    any_spec = pl.BlockSpec(memory_space=pl.ANY)
    scratch = [pltpu.VMEM(value.shape, value.dtype) for value in inputs]
    scratch += [
        pltpu.VMEM((ALL_ROWS, TOKENS, PAIR), BF),
        pltpu.VMEM((ALL_ROWS, TOKENS, PAIR), BF),
        pltpu.VMEM((ALL_ROWS, HEADS, TOKENS), F32),
        pltpu.VMEM((ALL_ROWS, HEADS, TOKENS), BF),
        pltpu.VMEM((PEERS, CPLX, ROWS, 2 * WIDTH), BF),
        pltpu.VMEM((2, 2, CPLX, ROWS, 2 * WIDTH), BF),
        pltpu.VMEM((2, CPLX, ROWS, 2 * WIDTH), BF),
        pltpu.VMEM((CPLX, ROWS, 2 * WIDTH), BF),
        pltpu.VMEM((ALL_ROWS, 2 * WIDTH), BF),
        pltpu.VMEM((PAIR, 2 * TRANS_P), F32),
        pltpu.VMEM((PAIR, TRANS_P), F32),
        pltpu.VMEM((HEADS, PAIR), F32),
        pltpu.VMEM((NUM_BLOCKS, BLOCK_I * TOKENS, 2 * TRANS_P), BF),
        pltpu.VMEM((ALL_ROWS, WIDTH), BF),
        pltpu.VMEM((ALL_ROWS, WIDTH), F32),
        pltpu.VMEM((ALL_ROWS, WIDTH), BF),
        pltpu.VMEM((ALL_ROWS, WIDTH), BF),
        pltpu.VMEM((ALL_ROWS, WIDTH), F32),
        pltpu.VMEM((ALL_ROWS, 1), F32),
        pltpu.VMEM((CPLX, ROWS * HEADS, TOKENS), F32),
        pltpu.VMEM((CPLX, ROWS * HEADS, WIDTH), BF),
        pltpu.VMEM((TILES, 16, 128), BF),
    ]
    for chunk, kind in enumerate(CHUNK_KINDS):
        for name, size in zip(LEVELS[kind][0], level_sizes(chunk)[1:]):
            scratch.append(pltpu.VMEM((len(LEVELS[kind]), GROUP[name] - 1, size, 16, 128), BF))
    dma = pltpu.SemaphoreType.DMA
    scratch += [dma((17,)), dma((3,)), dma((3,)), dma((2,)), dma((2,)), dma((len(CHUNKS),)), dma((len(CHUNKS), MAX_STEPS))]
    return pl.pallas_call(
        main_kernel,
        out_shape=(pltpu.VMEM((ALL_ROWS, TOKENS, PAIR), BF), pltpu.VMEM((CPLX, ROWS, WIDTH), BF), pltpu.VMEM((TILES, 16, 128), BF)),
        in_specs=[any_spec] * 17,
        out_specs=(pl.BlockSpec(memory_space=pltpu.VMEM),) * 3,
        scratch_shapes=scratch,
        compiler_params=pltpu.CompilerParams(collective_id=0, has_side_effects=True, vmem_limit_bytes=50 * 1024 * 1024),
        name='pairformer_tail',
    )(*(pltpu.with_memory_space_constraint(value, pltpu.HBM) for value in inputs))


UNPACK = ('pa', 'pb', 'po', 'bias', 'q', 'qb', 'kv', 'g', 'o', 'sa', 'sb', 'so')


def unpack_kernel(tiles, dz_buf, ds_buf, *refs):
    outs = dict(zip(UNPACK, refs[:12]))
    dz_out, ds_out = refs[12:14]
    stages = dict(zip(UNPACK, refs[14:26]))
    sem, pass_sem = refs[26:]
    copies = []
    for index, (buf, dst) in enumerate(((dz_buf, dz_out), (ds_buf, ds_out))):
        made = pltpu.make_async_copy(buf, dst, pass_sem.at[index])
        made.start()
        copies.append(made)

    def widen(stage, base, rows, row, cols, col):
        per_col = rows // 16
        for sub in range(cols // 128):
            part = tiles[base + sub * per_col:base + (sub + 1) * per_col].astype(F32)
            stage[row:row + rows, col + sub * 128:col + (sub + 1) * 128] = part.reshape(rows, 128)

    def send(name):
        made = pltpu.make_async_copy(stages[name], outs[name], sem.at[UNPACK.index(name)])
        made.start()
        copies.append(made)

    for name in ('kv', 'o', 'q', 'g', 'pa', 'pb', 'po', 'bias', 'qb'):
        base, rows, cols = SLOTS[name]
        if name == 'qb':
            last_tile = tiles[base].astype(F32)
            for sub in range(3):
                stages[name][pl.ds(sub * 128, 128)] = last_tile[sub]
        else:
            widen(stages[name], base, rows, 0, cols, 0)
        send(name)
    for piece in range(TRANS_S // PIECE):
        base = piece * PIECE_TILES
        third = PIECE_TILES // 3
        widen(stages['so'], base, PIECE, piece * PIECE, WIDTH, 0)
        widen(stages['sa'], base + third, WIDTH, 0, PIECE, piece * PIECE)
        widen(stages['sb'], base + 2 * third, WIDTH, 0, PIECE, piece * PIECE)
    for name in ('so', 'sa', 'sb'):
        send(name)
    for copy in copies:
        copy.wait()


def run_unpack(tiles, dz_in, ds_in):
    shapes = [(WIDTH,) if name == 'qb' else (TRANS_S, WIDTH) if name == 'so' else (WIDTH, TRANS_S) if name in ('sa', 'sb')
              else SLOTS[name][1:] for name in UNPACK]
    any_spec = pl.BlockSpec(memory_space=pl.ANY)
    return pl.pallas_call(
        unpack_kernel,
        out_shape=tuple(jax.ShapeDtypeStruct(shape, F32) for shape in shapes) + (
            jax.ShapeDtypeStruct(dz_in.shape, BF), jax.ShapeDtypeStruct(ds_in.shape, BF)),
        in_specs=[pl.BlockSpec(memory_space=pltpu.VMEM)] * 3,
        out_specs=(any_spec,) * 14,
        scratch_shapes=[pltpu.VMEM(shape, F32) for shape in shapes] + [
            pltpu.SemaphoreType.DMA((12,)), pltpu.SemaphoreType.DMA((2,))],
        compiler_params=pltpu.CompilerParams(vmem_limit_bytes=24 * 1024 * 1024),
        name='unpack_sums',
    )(*(pltpu.with_memory_space_constraint(value, pltpu.VMEM) for value in (tiles, dz_in, ds_in)))


def solution(mesh):
    pair_spec = P('dp', 'dap', None, None)
    single_spec = P('dp', 'dap', None)

    def body(pair_z, single_s, token_mask, dz_out, ds_out, w_pa, w_pb, w_po, w_bias, w_q, q_bias, w_kv, w_g, w_o, w_sa, w_sb, w_so):
        inputs = (pair_z.reshape(ALL_ROWS, TOKENS, PAIR), single_s, token_mask, dz_out.reshape(ALL_ROWS, TOKENS, PAIR), ds_out,
                  w_pa, w_pb, w_po, w_bias.T, w_q, q_bias, w_kv, w_g, w_o, w_sa, w_sb, w_so)
        dz_in, ds_in, tiles = run_main(inputs)
        *sums, dz_in, ds_in = run_unpack(tiles, dz_in, ds_in)
        sums[3] = sums[3].T
        return (dz_in.reshape(pair_z.shape), ds_in) + tuple(sums)

    in_specs = (pair_spec, single_spec, P('dp', None), pair_spec, single_spec) + (P(),) * 12
    out_specs = (pair_spec, single_spec) + (P(),) * 12
    return jax.shard_map(body, mesh=mesh, in_specs=in_specs, out_specs=out_specs, check_vma=False)
```

```python
import math
import jax
import jax.numpy as jnp
from jax import lax
from jax.experimental import pallas as pl
from jax.experimental.pallas import tpu as pltpu
from jax.sharding import PartitionSpec as P

HEAD_DIM = 24
HEADS = 16
WIDTH = 384
TRANS_S = 1536
PAIR = 128
TRANS_P = 512
TOKENS = 96
ROWS = 24
CPLX = 3
ALL_ROWS = CPLX * ROWS
SCALE = HEAD_DIM ** -0.5
EPSILON = 1e-5
MASK_BIG = 1e9
PEERS = 4
MESH_ID = pl.DeviceIdType.MESH
BF = jnp.bfloat16
F32 = jnp.float32

PIECE = 512
PIECE_TILES = 288
SLOTS = {
    'o': (864, 384, 384),
    'q': (936, 384, 384), 'g': (1008, 384, 384), 'qb': (1080, 16, 128), 'kv': (1088, 384, 768),
    'pa': (1280, 128, 512), 'pb': (1312, 128, 512), 'po': (1344, 512, 128), 'bias': (1232, 16, 128),
}
CHUNK = 192
LOCAL_END, PAIR_START, TILES = 1088, 1280, 1376
CHUNKS = tuple((base, min(CHUNK, LOCAL_END - base)) for base in range(0, LOCAL_END, CHUNK)) + (
    (LOCAL_END, PAIR_START - LOCAL_END), (PAIR_START, TILES - PAIR_START))
KV_CHUNK, PAIR_CHUNK = len(CHUNKS) - 2, len(CHUNKS) - 1
BLOCK_I = 8
NUM_BLOCKS = ALL_ROWS // BLOCK_I
FWD_BLOCK_I = 12

CHUNK_KINDS = 'nahnafap'
LEVELS = {
    'a': (('core', 'x', 'y', 'z'), ('core', 'y', 'x', 'z')),
    'h': (('core', 'x', 'y', 'z0', 'z1'), ('core', 'y', 'x', 'z0', 'z1')),
    'f': (('core', 'z0', 'x', 'y', 'z1'), ('core', 'z0', 'y', 'x', 'z1')),
    'm': (('core', 'x', 'z0', 'y', 'z1'), ('core', 'y', 'z0', 'x', 'z1')),
    'n': (('core', 'x', 'z0', 'z1', 'y'), ('core', 'y', 'z0', 'z1', 'x')),
    'p': (('core', 'xy', 'z'),),
}
GROUP = {'core': 2, 'x': 2, 'y': 2, 'z': 4, 'z0': 2, 'z1': 2, 'xy': 4}

LINK_US = {
    'core': {'core': 0.003}, 'x': {'x': 0.0757}, 'y': {'y': 0.0757}, 'xy': {'x': 0.1514, 'y': 0.1514},
    'z': {'mid': 0.3024, 'end': 0.2268}, 'z0': {'end': 0.0756}, 'z1': {'mid': 0.1512, 'end': 0.0756},
}
LATENCY_US = {'core': 0.85, 'x': 3.5, 'y': 3.2, 'z': 4.15, 'z0': 3.4, 'z1': 3.9, 'xy': 3.8}
KV_LINK_US = ({'end': 4.1}, {'mid': 4.1, 'end': 2.05})
BACKLOG_US = 2.0
FIRST_BLOCK = 5
PAIR_END = FIRST_BLOCK + NUM_BLOCKS
DZ_BLOCK = PAIR_END + 1
SEGMENT_US = (1.0, 1.0, 1.0, 2.1, 1.1) + (2.3,) * NUM_BLOCKS + (0.65,) + (0.75,) * NUM_BLOCKS
SEGMENT_TILES = (288, 576, 864, 936, LOCAL_END)
KV_SEGMENT = 3


def level_sizes(chunk):
    sizes = [CHUNKS[chunk][1] // len(LEVELS[CHUNK_KINDS[chunk]])]
    for name in LEVELS[CHUNK_KINDS[chunk]][0]:
        sizes.append(sizes[-1] // GROUP[name])
    return sizes


def plan_actions():
    stage = [0] * len(CHUNKS)
    due = {}
    free = {}
    actions = [[] for _ in range(len(SEGMENT_US) + 1)]
    now, segment, kv_due, kv_step = 0.0, 0, None, 0

    def steps(chunk):
        return 2 * len(LEVELS[CHUNK_KINDS[chunk]][0])

    def occupy(links, start):
        ends = []
        for link, time in links.items():
            free[link] = max(free.get(link, 0.0), start) + time
            ends.append(free[link])
        return max(ends)

    def when(chunk):
        step, half = stage[chunk], steps(chunk) // 2
        if step > 2 * half:
            return None
        time = due.get(chunk, 0.0)
        if step == 0:
            if chunk == PAIR_CHUNK:
                able = segment >= PAIR_END
            elif chunk == KV_CHUNK:
                able = kv_step == 2
            else:
                end = sum(CHUNKS[chunk])
                able = segment > next(index for index, tiles in enumerate(SEGMENT_TILES) if end <= tiles)
            if not able:
                return None
        if step < 2 * half and chunk != PAIR_CHUNK:
            for names in LEVELS[CHUNK_KINDS[chunk]]:
                for link in LINK_US[names[min(step, 2 * half - 1 - step)]]:
                    time = max(time, free.get(link, 0.0) - BACKLOG_US)
        return time

    while True:
        if kv_due is not None and kv_due <= now and kv_step < 2:
            actions[segment].append((-1, kv_step))
            kv_step += 1
            now += 0.3
            kv_due = occupy(KV_LINK_US[1], now) + LATENCY_US['z1'] if kv_step == 1 else None
            continue
        times = {chunk: when(chunk) for chunk in range(len(CHUNKS))}
        times = {chunk: time for chunk, time in times.items() if time is not None}
        waiting = [chunk for chunk, time in times.items() if time <= now]
        if waiting:
            chunk = min(waiting, key=lambda one: (one != PAIR_CHUNK, one))
            step = stage[chunk]
            actions[segment].append((chunk, step))
            half = steps(chunk) // 2
            sizes = level_sizes(chunk)
            now += 0.015 + (0.0017 * len(LEVELS[CHUNK_KINDS[chunk]]) * sizes[step] if 0 < step <= half else 0.0)
            if step < 2 * half:
                level = min(step, 2 * half - 1 - step)
                ends = []
                for names in LEVELS[CHUNK_KINDS[chunk]]:
                    name = names[level]
                    links = {link: time * sizes[level + 1] for link, time in LINK_US[name].items()}
                    ends.append(occupy(links, now) + LATENCY_US[name])
                due[chunk] = max(ends)
            stage[chunk] = step + 1
        elif segment < len(SEGMENT_US):
            now += SEGMENT_US[segment]
            if segment == KV_SEGMENT:
                kv_due = occupy(KV_LINK_US[0], now) + LATENCY_US['z0']
            segment += 1
        else:
            later = list(times.values()) + [kv_due] * (kv_due is not None)
            if not later:
                return actions
            now = max(now, min(later))


ACTIONS = plan_actions()


def dot_nn(left, right):
    return lax.dot_general(left, right, (((1,), (0,)), ((), ())), preferred_element_type=F32)


def dot_nt(left, right):
    return lax.dot_general(left, right, (((1,), (1,)), ((), ())), preferred_element_type=F32)


def dot_tn(left, right):
    return lax.dot_general(left, right, (((0,), (0,)), ((), ())), preferred_element_type=F32)


def layer_norm(wide):
    centred = wide - jnp.mean(wide, axis=-1, keepdims=True)
    inv_std = lax.rsqrt(jnp.mean(centred * centred, axis=-1, keepdims=True) + EPSILON)
    return centred * inv_std, inv_std


def norm_grad(normed, inv_std, grad_out):
    mean_grad = jnp.mean(grad_out, axis=-1, keepdims=True)
    mean_proj = jnp.mean(grad_out * normed, axis=-1, keepdims=True)
    return inv_std * (grad_out - mean_grad - normed * mean_proj)


def sigmoid(values):
    return 0.5 * jnp.tanh(0.5 * values) + 0.5


def swiglu_grad(hid_a, hid_b, grad_hidden):
    half_a = 0.5 * hid_a
    tanh_a = jnp.tanh(half_a)
    sig_a = 0.5 * tanh_a + 0.5
    silu_a = half_a * tanh_a + half_a
    grad_a = (grad_hidden * hid_b) * (sig_a + silu_a * (1.0 - sig_a))
    return silu_a * hid_b, grad_a, grad_hidden * silu_a


def put_at(grads, base, value):
    per_col = value.shape[0] // 16
    for col in range(value.shape[1] // 128):
        start = base + col * per_col
        grads[start:start + per_col] = value[:, col * 128:(col + 1) * 128].reshape(per_col, 16, 128).astype(BF)


def put_tiles(grads, name, value):
    put_at(grads, SLOTS[name][0], value)


class Reducer:
    def __init__(self, chunk, grads, total, got, send_sem, recv_sem, place):
        self.chunk = chunk
        self.grads, self.total, self.got = grads, total, got
        self.send_sem, self.recv_sem = send_sem, recv_sem
        self.place = place
        self.levels = LEVELS[CHUNK_KINDS[chunk]]
        self.sizes = level_sizes(chunk)
        self.depth = len(self.levels[0])

    def kept(self, part, level):
        at = CHUNKS[self.chunk][0] + part * self.sizes[0]
        for name, size in zip(self.levels[part][:level], self.sizes[1:]):
            at = at + self.place['index'][name] * size
        return at

    def held(self, part, level, start, count):
        if level == 0:
            return self.grads.at[pl.ds(self.kept(part, 0) + start, count)]
        return self.got[level - 1].at[part, 0, pl.ds(start, count)]

    def start(self, step):
        level = min(step, 2 * self.depth - 1 - step)
        size = self.sizes[level + 1]
        for part in range(len(self.levels)):
            name = self.levels[part][level]
            group = GROUP[name]
            for hop in range(1, group):
                other = lax.rem(self.place['index'][name] + hop, group)
                if step < self.depth:
                    src, dst = self.held(part, level, other * size, size), self.got[level].at[part, hop - 1]
                else:
                    src = dst = self.total.at[pl.ds(self.kept(part, level + 1), size)]
                pltpu.make_async_remote_copy(
                    src_ref=src, dst_ref=dst, send_sem=self.send_sem, recv_sem=self.recv_sem.at[step],
                    device_id=self.place['peer'](name, other), device_id_type=MESH_ID).start()

    def moved(self, level):
        return len(self.levels) * (GROUP[self.levels[0][level]] - 1) * self.sizes[level + 1]

    def wait_tiles(self, count, sem):
        span = self.grads.at[pl.ds(0, count)]
        pltpu.make_async_copy(span, span, sem).wait()

    def add(self, level):
        size = self.sizes[level + 1]
        for part in range(len(self.levels)):
            name = self.levels[part][level]
            own = self.held(part, level, self.place['index'][name] * size, size)
            slots = [self.got[level].at[part, hop] for hop in range(GROUP[name] - 1)]
            dst = slots[0] if level + 1 < self.depth else self.total.at[pl.ds(self.kept(part, level + 1), size)]
            add_into(dst, [own] + slots, size)

    def step(self, step):
        if step:
            level = min(step - 1, 2 * self.depth - step)
            self.wait_tiles(self.moved(level), self.recv_sem.at[step - 1])
        if 0 < step <= self.depth:
            self.add(step - 1)
        if step < 2 * self.depth:
            self.start(step)

    def finish_sends(self):
        self.wait_tiles(2 * sum(self.moved(level) for level in range(self.depth)), self.send_sem)


def add_into(dst, terms, count):
    step = math.gcd(count, 8)

    @pl.loop(0, count // step)
    def _(index):
        at = pl.ds(index * step, step)
        total = terms[0][at].astype(F32)
        for term in terms[1:]:
            total = total + term[at].astype(F32)
        dst[at] = total.astype(BF)


def main_kernel(*refs):
    names = ('pair_z', 'single_s', 'token_mask', 'dz_out', 'ds_out', 'w_pa', 'w_pb', 'w_po', 'w_bias', 'w_q', 'q_bias',
             'w_kv', 'w_g', 'w_o', 'w_sa', 'w_sb', 'w_so')
    hbm = dict(zip(names, refs[:17]))
    dz_in, ds_in, total = refs[17:20]
    scratch = refs[20:]
    loaded = dict(zip(names, scratch[:17]))
    (new_rows, norm_rows, bias_rows, grad_bias, kv_buf, gkv_buf, gkv_got1, gkv_got2, gkv_s, acc_ab, acc_po, acc_bias, gab_s, act_s, norm_s, gq_s, ggp_s,
     gmid_s, inv_s, prob_s, qexp_s, grads) = scratch[17:39]
    got_refs = list(scratch[39:39 + GOT_COUNT])
    load_sem, kv_send, kv_recv, gkv_send, gkv_recv, ar_send, ar_recv = scratch[39 + GOT_COUNT:]

    order = ('single_s', 'w_kv', 'pair_z', 'w_pa', 'w_pb', 'w_po', 'w_bias', 'w_q', 'q_bias', 'w_g', 'token_mask', 'w_o', 'w_sa',
             'w_sb', 'ds_out', 'w_so', 'dz_out')
    loads = {}
    for index, name in enumerate(order):
        loads[name] = pltpu.make_async_copy(hbm[name], loaded[name], load_sem.at[index])
        loads[name].start()

    my_z = lax.axis_index('dap')
    my_dp = lax.axis_index('dp')
    core = lax.rem(my_dp, 2)
    bit_x = lax.rem(lax.div(my_dp, 2), 2)
    bit_y = lax.div(my_dp, 4)

    def z_peer(other):
        return (other, my_dp)

    def peer(name, other):
        if name == 'core':
            return my_z, my_dp + other - core
        if name == 'x':
            return my_z, my_dp + 2 * (other - bit_x)
        if name == 'y':
            return my_z, my_dp + 4 * (other - bit_y)
        if name == 'xy':
            return my_z, 2 * other + core
        if name == 'z':
            return other, my_dp
        low = lax.rem(my_z, 2)
        return (my_z - low + other if name == 'z0' else 2 * other + low), my_dp

    place = {'peer': peer, 'index': {
        'core': core, 'x': bit_x, 'y': bit_y, 'xy': 2 * bit_y + bit_x, 'z': my_z, 'z0': lax.rem(my_z, 2), 'z1': lax.div(my_z, 2)}}

    barrier = pltpu.get_barrier_semaphore()
    for name in ('core', 'xy', 'z'):
        for hop in range(1, GROUP[name]):
            device = peer(name, lax.rem(place['index'][name] + hop, GROUP[name]))
            pl.semaphore_signal(barrier, inc=1, device_id=device, device_id_type=MESH_ID)

    loads['single_s'].wait()
    loads['w_kv'].wait()
    s_wide = loaded['single_s'][...].astype(F32).reshape(ALL_ROWS, WIDTH)
    s_norm, s_inv = layer_norm(s_wide)
    act = s_norm.astype(BF)
    act_s[...] = act
    norm_s[...] = s_norm
    inv_s[...] = s_inv
    kv_local = dot_nn(act, loaded['w_kv'][...])
    pl.semaphore_wait(barrier, 7)
    kv_buf[my_z] = kv_local.reshape(CPLX, ROWS, 2 * WIDTH).astype(BF)

    def kv_copy(hop):
        return pltpu.make_async_remote_copy(
            src_ref=kv_buf.at[my_z], dst_ref=kv_buf.at[my_z], send_sem=kv_send.at[hop - 1], recv_sem=kv_recv.at[hop - 1],
            device_id=z_peer(lax.rem(my_z + hop, PEERS)), device_id_type=MESH_ID)

    for hop in range(1, PEERS):
        kv_copy(hop).start()

    for name in ('pair_z', 'w_pa', 'w_pb', 'w_po', 'w_bias'):
        loads[name].wait()
    block_rows = BLOCK_I * TOKENS
    fwd_rows = FWD_BLOCK_I * TOKENS

    @pl.loop(0, ALL_ROWS // FWD_BLOCK_I)
    def _(block):
        at = block * FWD_BLOCK_I
        z_wide = loaded['pair_z'][pl.ds(at, FWD_BLOCK_I)].reshape(fwd_rows, PAIR).astype(F32)
        normed, _ = layer_norm(z_wide)
        normed_bf = normed.astype(BF)
        half_a = 0.5 * dot_nn(normed_bf, loaded['w_pa'][...])
        hid_b = dot_nn(normed_bf, loaded['w_pb'][...])
        hidden = ((half_a * jnp.tanh(half_a) + half_a) * hid_b).astype(BF)
        z_new = (z_wide + dot_nn(hidden, loaded['w_po'][...])).astype(BF)
        new_rows[pl.ds(at, FWD_BLOCK_I)] = z_new.reshape(FWD_BLOCK_I, TOKENS, PAIR)
        bias_norm, _ = layer_norm(z_new.astype(F32))
        bias_bf = bias_norm.astype(BF)
        norm_rows[pl.ds(at, FWD_BLOCK_I)] = bias_bf.reshape(FWD_BLOCK_I, TOKENS, PAIR)
        for row in range(FWD_BLOCK_I):
            bias_rows[at + row] = dot_nt(loaded['w_bias'][...], bias_bf[row * TOKENS:(row + 1) * TOKENS])

    for name in ('w_q', 'q_bias', 'w_g', 'token_mask', 'w_o', 'w_sa', 'w_sb', 'ds_out', 'w_so'):
        loads[name].wait()
    queries = (dot_nn(act_s[...], loaded['w_q'][...]) + loaded['q_bias'][...].astype(F32).reshape(1, WIDTH)).astype(BF).astype(F32)
    gate = sigmoid(dot_nn(act_s[...], loaded['w_g'][...]))
    lane_head = lax.broadcasted_iota(jnp.int32, (HEADS, WIDTH), 1)
    row_head = lax.broadcasted_iota(jnp.int32, (HEADS, WIDTH), 0)
    head_mask = jnp.where((lane_head >= row_head * HEAD_DIM) & (lane_head < (row_head + 1) * HEAD_DIM), 1.0, 0.0).astype(F32)

    def spread(rows):
        wide = jnp.broadcast_to(rows.reshape(ROWS, 1, WIDTH), (ROWS, HEADS, WIDTH)) * head_mask[None]
        return wide.reshape(ROWS * HEADS, WIDTH).astype(BF)

    def gather_heads(wide):
        return jnp.sum(wide.reshape(ROWS, HEADS, WIDTH) * head_mask[None], axis=1)

    for hop in range(1, PEERS):
        kv_copy(hop).wait()

    def keys_values(cplx):
        both = kv_buf[:, cplx].astype(F32).reshape(TOKENS, 2 * WIDTH).astype(BF)
        return both[:, :WIDTH], both[:, WIDTH:]

    key_mask = MASK_BIG * (loaded['token_mask'][...].astype(F32) - 1.0)
    attended_parts = []
    for cplx in range(CPLX):
        keys, values = keys_values(cplx)
        q_exp = spread(queries[cplx * ROWS:(cplx + 1) * ROWS])
        qexp_s[cplx] = q_exp
        bias = bias_rows[cplx * ROWS:(cplx + 1) * ROWS].reshape(ROWS * HEADS, TOKENS)
        logits = dot_nt(q_exp, keys) * SCALE + bias + key_mask[cplx:cplx + 1]
        top = jnp.max(logits, axis=-1, keepdims=True)
        expd = jnp.exp(logits - top)
        prob = expd / jnp.sum(expd, axis=-1, keepdims=True)
        prob_s[cplx] = prob
        attended_parts.append(gather_heads(dot_nn(prob.astype(BF), values)))
    attended = jnp.concatenate(attended_parts, axis=0)
    gated = (gate * attended).astype(BF)
    s_mid = (s_wide + dot_nn(gated, loaded['w_o'][...])).astype(BF)
    mid_norm, mid_inv = layer_norm(s_mid.astype(F32))
    mid_act = mid_norm.astype(BF)

    reducers = []
    for index in range(len(CHUNKS)):
        depth = len(LEVELS[CHUNK_KINDS[index]][0])
        reducers.append(Reducer(index, grads, total, got_refs[:depth], ar_send.at[index], ar_recv.at[index], place))
        del got_refs[:depth]

    def act_on(number):
        for chunk, step in ACTIONS[number]:
            if chunk < 0:
                (forward_kv_grad, finish_kv_grad)[step]()
            else:
                reducers[chunk].step(step)

    ds_wide = loaded['ds_out'][...].astype(F32).reshape(ALL_ROWS, WIDTH)
    ds_bf = ds_wide.astype(BF)
    grad_mid_norm = jnp.zeros((ALL_ROWS, WIDTH), F32)
    for piece in range(TRANS_S // PIECE):
        cols = slice(piece * PIECE, (piece + 1) * PIECE)
        base = piece * PIECE_TILES
        trans_a = dot_nn(mid_act, loaded['w_sa'][:, cols])
        trans_b = dot_nn(mid_act, loaded['w_sb'][:, cols])
        grad_hidden = dot_nt(ds_bf, loaded['w_so'][cols, :])
        hidden, grad_ta, grad_tb = swiglu_grad(trans_a, trans_b, grad_hidden)
        grad_ta = grad_ta.astype(BF)
        grad_tb = grad_tb.astype(BF)
        put_at(grads, base, dot_tn(hidden.astype(BF), ds_bf))
        put_at(grads, base + PIECE_TILES // 3, dot_tn(mid_act, grad_ta))
        put_at(grads, base + 2 * (PIECE_TILES // 3), dot_tn(mid_act, grad_tb))
        act_on(piece + 1)
        grad_mid_norm = grad_mid_norm + dot_nt(grad_ta, loaded['w_sa'][:, cols]) + dot_nt(grad_tb, loaded['w_sb'][:, cols])
    grad_mid = ds_wide + norm_grad(mid_norm, mid_inv, grad_mid_norm)
    gmid_s[...] = grad_mid
    grad_mid_bf = grad_mid.astype(BF)
    put_tiles(grads, 'o', dot_tn(gated, grad_mid_bf))
    grad_gated = dot_nt(grad_mid_bf, loaded['w_o'][...])
    grad_gate_pre = (grad_gated * attended * gate * (1.0 - gate)).astype(BF)
    ggp_s[...] = grad_gate_pre
    grad_att = (grad_gated * gate).astype(BF).astype(F32)
    grad_query_parts = []
    for cplx in range(CPLX):
        keys, values = keys_values(cplx)
        ga_exp = spread(grad_att[cplx * ROWS:(cplx + 1) * ROWS])
        prob = prob_s[cplx]
        grad_prob = dot_nt(ga_exp, values)
        grad_values = dot_tn(prob.astype(BF), ga_exp)
        grad_logits = (prob * (grad_prob - jnp.sum(prob * grad_prob, axis=-1, keepdims=True))).astype(BF)
        grad_bias[cplx * ROWS:(cplx + 1) * ROWS] = grad_logits.reshape(ROWS, HEADS, TOKENS)
        grad_query_parts.append(gather_heads(dot_nn(grad_logits, keys)) * SCALE)
        grad_keys = dot_tn(grad_logits, qexp_s[cplx]) * SCALE
        grad_keys = grad_keys.reshape(PEERS, ROWS, WIDTH).astype(BF)
        grad_values = grad_values.reshape(PEERS, ROWS, WIDTH).astype(BF)
        for owner in range(PEERS):
            gkv_buf[owner % 2, owner // 2, cplx, :, :WIDTH] = grad_keys[owner]
            gkv_buf[owner % 2, owner // 2, cplx, :, WIDTH:] = grad_values[owner]

    low, high = place['index']['z0'], place['index']['z1']

    def gkv_copy(step):
        src, dst = ((gkv_buf.at[1 - low], gkv_got1), (gkv_got1.at[1 - high], gkv_got2))[step]
        return pltpu.make_async_remote_copy(
            src_ref=src, dst_ref=dst, send_sem=gkv_send.at[step], recv_sem=gkv_recv.at[step],
            device_id=peer(*(('z0', 1 - low), ('z1', 1 - high))[step]), device_id_type=MESH_ID)

    gkv_copy(0).start()
    act_on(4)
    grad_query = jnp.concatenate(grad_query_parts, axis=0)
    grad_query_bf = grad_query.astype(BF)
    gq_s[...] = grad_query_bf
    put_tiles(grads, 'q', dot_tn(act_s[...], grad_query_bf))
    put_tiles(grads, 'g', dot_tn(act_s[...], grad_gate_pre))
    d_q_bias = jnp.sum(grad_query, axis=0, keepdims=True)
    row_index = lax.broadcasted_iota(jnp.int32, (16, 128), 0)
    bias_tile = jnp.zeros((16, 128), F32)
    for sub in range(3):
        bias_tile = jnp.where(row_index == sub, jnp.broadcast_to(d_q_bias[:, sub * 128:(sub + 1) * 128], (16, 128)), bias_tile)
    grads[1080] = bias_tile.astype(BF)
    grads[1081:1088] = jnp.zeros((7, 16, 128), BF)
    grads[1233:1280] = jnp.zeros((47, 16, 128), BF)

    def forward_kv_grad():
        gkv_copy(0).wait()
        gkv_got1[...] = (gkv_got1[...].astype(F32) + gkv_buf[low].astype(F32)).astype(BF)
        gkv_copy(1).start()

    def finish_kv_grad():
        gkv_copy(1).wait()
        summed = gkv_got1[high].astype(F32) + gkv_got2[...].astype(F32)
        grad_kv = summed.reshape(ALL_ROWS, 2 * WIDTH).astype(BF)
        gkv_s[...] = grad_kv
        put_tiles(grads, 'kv', dot_tn(act_s[...], grad_kv))

    def finish_single():
        grad_act = (dot_nt(gq_s[...], loaded['w_q'][...]) + dot_nt(gkv_s[...], loaded['w_kv'][...])
                    + dot_nt(ggp_s[...], loaded['w_g'][...]))
        grad_s = gmid_s[...] + norm_grad(norm_s[...], inv_s[...], grad_act)
        ds_in[...] = grad_s.reshape(CPLX, ROWS, WIDTH).astype(BF)

    loads['dz_out'].wait()
    acc_ab[...] = jnp.zeros_like(acc_ab)
    acc_po[...] = jnp.zeros_like(acc_po)
    acc_bias[...] = jnp.zeros_like(acc_bias)

    @pl.loop(0, NUM_BLOCKS)
    def _(block):
        total_bias = acc_bias[...]
        for row in range(BLOCK_I):
            total_bias = total_bias + dot_nn(grad_bias[block * BLOCK_I + row], norm_rows[block * BLOCK_I + row])
        acc_bias[...] = total_bias

    grads[SLOTS['bias'][0]] = acc_bias[...].astype(BF)

    def act_in_loop(block, first):
        for tick in range(NUM_BLOCKS):
            if ACTIONS[first + tick]:
                @pl.when(block == tick)
                def _():
                    act_on(first + tick)

    @pl.loop(0, NUM_BLOCKS)
    def _(block):
        act_in_loop(block, FIRST_BLOCK)
        at = block * BLOCK_I
        bias_norm, bias_inv = layer_norm(new_rows[pl.ds(at, BLOCK_I)].reshape(block_rows, PAIR).astype(F32))
        parts = [dot_tn(grad_bias[at + row], loaded['w_bias'][...]) for row in range(BLOCK_I)]
        grad_norm = jnp.concatenate(parts, axis=0)
        dz_wide = loaded['dz_out'][pl.ds(at, BLOCK_I)].reshape(block_rows, PAIR).astype(F32)
        grad_new_bf = (dz_wide + norm_grad(bias_norm, bias_inv, grad_norm)).astype(BF)
        new_rows[pl.ds(at, BLOCK_I)] = grad_new_bf.reshape(BLOCK_I, TOKENS, PAIR)
        normed, _ = layer_norm(loaded['pair_z'][pl.ds(at, BLOCK_I)].reshape(block_rows, PAIR).astype(F32))
        normed_bf = normed.astype(BF)
        hid_a = dot_nn(normed_bf, loaded['w_pa'][...])
        hid_b = dot_nn(normed_bf, loaded['w_pb'][...])
        grad_hidden = dot_nt(grad_new_bf, loaded['w_po'][...])
        hidden, grad_a, grad_b = swiglu_grad(hid_a, hid_b, grad_hidden)
        grad_a = grad_a.astype(BF)
        grad_b = grad_b.astype(BF)
        gab_s[block, :, :TRANS_P] = grad_a
        gab_s[block, :, TRANS_P:] = grad_b
        acc_po[...] += dot_tn(grad_new_bf, hidden.astype(BF))
        acc_ab[:, :TRANS_P] += dot_tn(normed_bf, grad_a)
        acc_ab[:, TRANS_P:] += dot_tn(normed_bf, grad_b)

    put_tiles(grads, 'pa', acc_ab[:, :TRANS_P])
    put_tiles(grads, 'pb', acc_ab[:, TRANS_P:])
    put_tiles(grads, 'po', jnp.transpose(acc_po[...]))
    act_on(PAIR_END)
    finish_single()

    @pl.loop(0, NUM_BLOCKS)
    def _(block):
        act_in_loop(block, DZ_BLOCK)
        at = block * BLOCK_I
        normed, inv_std = layer_norm(loaded['pair_z'][pl.ds(at, BLOCK_I)].reshape(block_rows, PAIR).astype(F32))
        grad_normed = dot_nt(gab_s[block, :, :TRANS_P], loaded['w_pa'][...]) + dot_nt(gab_s[block, :, TRANS_P:], loaded['w_pb'][...])
        grad_new = new_rows[pl.ds(at, BLOCK_I)].reshape(block_rows, PAIR).astype(F32)
        result = grad_new + norm_grad(normed, inv_std, grad_normed)
        dz_in[pl.ds(at, BLOCK_I)] = result.reshape(BLOCK_I, TOKENS, PAIR).astype(BF)

    act_on(DZ_BLOCK + NUM_BLOCKS)
    for reducer in reducers:
        reducer.finish_sends()


GOT_COUNT = sum(len(LEVELS[kind][0]) for kind in CHUNK_KINDS)
MAX_STEPS = 2 * max(len(LEVELS[kind][0]) for kind in CHUNK_KINDS)


def run_main(inputs):
    any_spec = pl.BlockSpec(memory_space=pl.ANY)
    scratch = [pltpu.VMEM(value.shape, value.dtype) for value in inputs]
    scratch += [
        pltpu.VMEM((ALL_ROWS, TOKENS, PAIR), BF),
        pltpu.VMEM((ALL_ROWS, TOKENS, PAIR), BF),
        pltpu.VMEM((ALL_ROWS, HEADS, TOKENS), F32),
        pltpu.VMEM((ALL_ROWS, HEADS, TOKENS), BF),
        pltpu.VMEM((PEERS, CPLX, ROWS, 2 * WIDTH), BF),
        pltpu.VMEM((2, 2, CPLX, ROWS, 2 * WIDTH), BF),
        pltpu.VMEM((2, CPLX, ROWS, 2 * WIDTH), BF),
        pltpu.VMEM((CPLX, ROWS, 2 * WIDTH), BF),
        pltpu.VMEM((ALL_ROWS, 2 * WIDTH), BF),
        pltpu.VMEM((PAIR, 2 * TRANS_P), F32),
        pltpu.VMEM((PAIR, TRANS_P), F32),
        pltpu.VMEM((HEADS, PAIR), F32),
        pltpu.VMEM((NUM_BLOCKS, BLOCK_I * TOKENS, 2 * TRANS_P), BF),
        pltpu.VMEM((ALL_ROWS, WIDTH), BF),
        pltpu.VMEM((ALL_ROWS, WIDTH), F32),
        pltpu.VMEM((ALL_ROWS, WIDTH), BF),
        pltpu.VMEM((ALL_ROWS, WIDTH), BF),
        pltpu.VMEM((ALL_ROWS, WIDTH), F32),
        pltpu.VMEM((ALL_ROWS, 1), F32),
        pltpu.VMEM((CPLX, ROWS * HEADS, TOKENS), F32),
        pltpu.VMEM((CPLX, ROWS * HEADS, WIDTH), BF),
        pltpu.VMEM((TILES, 16, 128), BF),
    ]
    for chunk, kind in enumerate(CHUNK_KINDS):
        for name, size in zip(LEVELS[kind][0], level_sizes(chunk)[1:]):
            scratch.append(pltpu.VMEM((len(LEVELS[kind]), GROUP[name] - 1, size, 16, 128), BF))
    dma = pltpu.SemaphoreType.DMA
    scratch += [dma((17,)), dma((3,)), dma((3,)), dma((2,)), dma((2,)), dma((len(CHUNKS),)), dma((len(CHUNKS), MAX_STEPS))]
    return pl.pallas_call(
        main_kernel,
        out_shape=(pltpu.VMEM((ALL_ROWS, TOKENS, PAIR), BF), pltpu.VMEM((CPLX, ROWS, WIDTH), BF), pltpu.VMEM((TILES, 16, 128), BF)),
        in_specs=[any_spec] * 17,
        out_specs=(pl.BlockSpec(memory_space=pltpu.VMEM),) * 3,
        scratch_shapes=scratch,
        compiler_params=pltpu.CompilerParams(collective_id=0, has_side_effects=True, vmem_limit_bytes=50 * 1024 * 1024),
        name='pairformer_tail',
    )(*(pltpu.with_memory_space_constraint(value, pltpu.HBM) for value in inputs))


UNPACK = ('pa', 'pb', 'po', 'bias', 'q', 'qb', 'kv', 'g', 'o', 'sa', 'sb', 'so')


def unpack_kernel(tiles, dz_buf, ds_buf, *refs):
    outs = dict(zip(UNPACK, refs[:12]))
    dz_out, ds_out = refs[12:14]
    stages = dict(zip(UNPACK, refs[14:26]))
    sem, pass_sem = refs[26:]
    copies = []
    for index, (buf, dst) in enumerate(((dz_buf, dz_out), (ds_buf, ds_out))):
        made = pltpu.make_async_copy(buf, dst, pass_sem.at[index])
        made.start()
        copies.append(made)

    def widen(stage, base, rows, row, cols, col):
        per_col = rows // 16
        for sub in range(cols // 128):
            part = tiles[base + sub * per_col:base + (sub + 1) * per_col].astype(F32)
            stage[row:row + rows, col + sub * 128:col + (sub + 1) * 128] = part.reshape(rows, 128)

    def send(name):
        made = pltpu.make_async_copy(stages[name], outs[name], sem.at[UNPACK.index(name)])
        made.start()
        copies.append(made)

    for name in ('kv', 'o', 'q', 'g', 'pa', 'pb', 'po', 'bias', 'qb'):
        base, rows, cols = SLOTS[name]
        if name == 'qb':
            last_tile = tiles[base].astype(F32)
            for sub in range(3):
                stages[name][pl.ds(sub * 128, 128)] = last_tile[sub]
        else:
            widen(stages[name], base, rows, 0, cols, 0)
        send(name)
    for piece in range(TRANS_S // PIECE):
        base = piece * PIECE_TILES
        third = PIECE_TILES // 3
        widen(stages['so'], base, PIECE, piece * PIECE, WIDTH, 0)
        widen(stages['sa'], base + third, WIDTH, 0, PIECE, piece * PIECE)
        widen(stages['sb'], base + 2 * third, WIDTH, 0, PIECE, piece * PIECE)
    for name in ('so', 'sa', 'sb'):
        send(name)
    for copy in copies:
        copy.wait()


def run_unpack(tiles, dz_in, ds_in):
    shapes = [(WIDTH,) if name == 'qb' else (TRANS_S, WIDTH) if name == 'so' else (WIDTH, TRANS_S) if name in ('sa', 'sb')
              else SLOTS[name][1:] for name in UNPACK]
    any_spec = pl.BlockSpec(memory_space=pl.ANY)
    return pl.pallas_call(
        unpack_kernel,
        out_shape=tuple(jax.ShapeDtypeStruct(shape, F32) for shape in shapes) + (
            jax.ShapeDtypeStruct(dz_in.shape, BF), jax.ShapeDtypeStruct(ds_in.shape, BF)),
        in_specs=[pl.BlockSpec(memory_space=pltpu.VMEM)] * 3,
        out_specs=(any_spec,) * 14,
        scratch_shapes=[pltpu.VMEM(shape, F32) for shape in shapes] + [
            pltpu.SemaphoreType.DMA((12,)), pltpu.SemaphoreType.DMA((2,))],
        compiler_params=pltpu.CompilerParams(vmem_limit_bytes=24 * 1024 * 1024),
        name='unpack_sums',
    )(*(pltpu.with_memory_space_constraint(value, pltpu.VMEM) for value in (tiles, dz_in, ds_in)))


def solution(mesh):
    pair_spec = P('dp', 'dap', None, None)
    single_spec = P('dp', 'dap', None)

    def body(pair_z, single_s, token_mask, dz_out, ds_out, w_pa, w_pb, w_po, w_bias, w_q, q_bias, w_kv, w_g, w_o, w_sa, w_sb, w_so):
        inputs = (pair_z.reshape(ALL_ROWS, TOKENS, PAIR), single_s, token_mask, dz_out.reshape(ALL_ROWS, TOKENS, PAIR), ds_out,
                  w_pa, w_pb, w_po, w_bias.T, w_q, q_bias, w_kv, w_g, w_o, w_sa, w_sb, w_so)
        dz_in, ds_in, tiles = run_main(inputs)
        *sums, dz_in, ds_in = run_unpack(tiles, dz_in, ds_in)
        sums[3] = sums[3].T
        return (dz_in.reshape(pair_z.shape), ds_in) + tuple(sums)

    in_specs = (pair_spec, single_spec, P('dp', None), pair_spec, single_spec) + (P(),) * 12
    out_specs = (pair_spec, single_spec) + (P(),) * 12
    return jax.shard_map(body, mesh=mesh, in_specs=in_specs, out_specs=out_specs, check_vma=False)
```

```python
import math
import jax
import jax.numpy as jnp
from jax import lax
from jax.experimental import pallas as pl
from jax.experimental.pallas import tpu as pltpu
from jax.sharding import PartitionSpec as P

HEAD_DIM = 24
HEADS = 16
WIDTH = 384
TRANS_S = 1536
PAIR = 128
TRANS_P = 512
TOKENS = 96
ROWS = 24
CPLX = 3
ALL_ROWS = CPLX * ROWS
SCALE = HEAD_DIM ** -0.5
EPSILON = 1e-5
MASK_BIG = 1e9
PEERS = 4
MESH_ID = pl.DeviceIdType.MESH
BF = jnp.bfloat16
F32 = jnp.float32

PIECE = 512
PIECE_TILES = 288
SLOTS = {
    'o': (864, 384, 384),
    'q': (936, 384, 384), 'g': (1008, 384, 384), 'qb': (1080, 16, 128), 'kv': (1088, 384, 768),
    'pa': (1280, 128, 512), 'pb': (1312, 128, 512), 'po': (1344, 512, 128), 'bias': (1232, 16, 128),
}
CHUNK = 128
LOCAL_END, PAIR_START, TILES = 1088, 1280, 1376
CHUNKS = tuple((base, min(CHUNK, LOCAL_END - base)) for base in range(0, LOCAL_END, CHUNK)) + (
    (LOCAL_END, PAIR_START - LOCAL_END), (PAIR_START, TILES - PAIR_START))
KV_CHUNK, PAIR_CHUNK = len(CHUNKS) - 2, len(CHUNKS) - 1
BLOCK_I = 8
NUM_BLOCKS = ALL_ROWS // BLOCK_I
FWD_BLOCK_I = 12

CHUNK_KINDS = 'hhafafhaaap'
LEVELS = {
    'a': (('core', 'x', 'y', 'z'), ('core', 'y', 'x', 'z')),
    'h': (('core', 'x', 'y', 'z0', 'z1'), ('core', 'y', 'x', 'z0', 'z1')),
    'f': (('core', 'z0', 'x', 'y', 'z1'), ('core', 'z0', 'y', 'x', 'z1')),
    'm': (('core', 'x', 'z0', 'y', 'z1'), ('core', 'y', 'z0', 'x', 'z1')),
    'n': (('core', 'x', 'z0', 'z1', 'y'), ('core', 'y', 'z0', 'z1', 'x')),
    'p': (('core', 'xy', 'z'),),
}
GROUP = {'core': 2, 'x': 2, 'y': 2, 'z': 4, 'z0': 2, 'z1': 2, 'xy': 4}

LINK_US = {
    'core': {'core': 0.003}, 'x': {'x': 0.0757}, 'y': {'y': 0.0757}, 'xy': {'x': 0.1514, 'y': 0.1514},
    'z': {'mid': 0.3024, 'end': 0.2268}, 'z0': {'end': 0.0756}, 'z1': {'mid': 0.1512, 'end': 0.0756},
}
LATENCY_US = {'core': 0.85, 'x': 3.5, 'y': 3.2, 'z': 4.15, 'z0': 3.4, 'z1': 3.9, 'xy': 3.8}
KV_LINK_US = ({'end': 4.1}, {'mid': 4.1, 'end': 2.05})
BACKLOG_US = 2.0
FIRST_BLOCK = 5
MAIN_BLOCK = FIRST_BLOCK + NUM_BLOCKS
SINGLE_END = MAIN_BLOCK + NUM_BLOCKS
DZ_BLOCK = SINGLE_END + 1
SEGMENT_US = (1.0, 1.0, 1.0, 2.1, 0.4) + (0.62,) * NUM_BLOCKS + (2.03,) * NUM_BLOCKS + (0.65,) + (0.74,) * NUM_BLOCKS
SEGMENT_TILES = (288, 576, 864, 936, LOCAL_END)
KV_SEGMENT = 3


def level_sizes(chunk):
    sizes = [CHUNKS[chunk][1] // len(LEVELS[CHUNK_KINDS[chunk]])]
    for name in LEVELS[CHUNK_KINDS[chunk]][0]:
        sizes.append(sizes[-1] // GROUP[name])
    return sizes


def plan_actions():
    stage = [0] * len(CHUNKS)
    due = {}
    free = {}
    actions = [[] for _ in range(len(SEGMENT_US) + 1)]
    now, segment, kv_due, kv_step = 0.0, 0, None, 0

    def steps(chunk):
        return 2 * len(LEVELS[CHUNK_KINDS[chunk]][0])

    def occupy(links, start):
        ends = []
        for link, time in links.items():
            free[link] = max(free.get(link, 0.0), start) + time
            ends.append(free[link])
        return max(ends)

    def when(chunk):
        step, half = stage[chunk], steps(chunk) // 2
        if step > 2 * half:
            return None
        time = due.get(chunk, 0.0)
        if step == 0:
            if chunk == PAIR_CHUNK:
                able = segment >= SINGLE_END
            elif chunk == KV_CHUNK:
                able = kv_step == 2
            else:
                end = sum(CHUNKS[chunk])
                able = segment > next(index for index, tiles in enumerate(SEGMENT_TILES) if end <= tiles)
            if not able:
                return None
        if step < 2 * half and chunk != PAIR_CHUNK:
            for names in LEVELS[CHUNK_KINDS[chunk]]:
                for link in LINK_US[names[min(step, 2 * half - 1 - step)]]:
                    time = max(time, free.get(link, 0.0) - BACKLOG_US)
        return time

    while True:
        if kv_due is not None and kv_due <= now and (kv_step == 0 or segment >= MAIN_BLOCK):
            actions[segment].append((-1, kv_step))
            kv_step += 1
            now += 0.3
            kv_due = occupy(KV_LINK_US[1], now) + LATENCY_US['z1'] if kv_step == 1 else None
            continue
        times = {chunk: when(chunk) for chunk in range(len(CHUNKS))}
        times = {chunk: time for chunk, time in times.items() if time is not None}
        waiting = [chunk for chunk, time in times.items() if time <= now]
        if waiting:
            chunk = min(waiting, key=lambda one: (one != PAIR_CHUNK, one))
            step = stage[chunk]
            actions[segment].append((chunk, step))
            half = steps(chunk) // 2
            sizes = level_sizes(chunk)
            now += 0.015 + (0.0017 * len(LEVELS[CHUNK_KINDS[chunk]]) * sizes[step] if 0 < step <= half else 0.0)
            if step < 2 * half:
                level = min(step, 2 * half - 1 - step)
                ends = []
                for names in LEVELS[CHUNK_KINDS[chunk]]:
                    name = names[level]
                    links = {link: time * sizes[level + 1] for link, time in LINK_US[name].items()}
                    ends.append(occupy(links, now) + LATENCY_US[name])
                due[chunk] = max(ends)
            stage[chunk] = step + 1
        elif segment < len(SEGMENT_US):
            now += SEGMENT_US[segment]
            if segment == KV_SEGMENT:
                kv_due = occupy(KV_LINK_US[0], now) + LATENCY_US['z0']
            segment += 1
        else:
            later = list(times.values()) + [kv_due] * (kv_due is not None)
            if not later:
                return actions
            now = max(now, min(later))


ACTIONS = plan_actions()


def dot_nn(left, right):
    return lax.dot_general(left, right, (((1,), (0,)), ((), ())), preferred_element_type=F32)


def dot_nt(left, right):
    return lax.dot_general(left, right, (((1,), (1,)), ((), ())), preferred_element_type=F32)


def dot_tn(left, right):
    return lax.dot_general(left, right, (((0,), (0,)), ((), ())), preferred_element_type=F32)


def layer_norm(wide):
    centred = wide - jnp.mean(wide, axis=-1, keepdims=True)
    inv_std = lax.rsqrt(jnp.mean(centred * centred, axis=-1, keepdims=True) + EPSILON)
    return centred * inv_std, inv_std


def norm_grad(normed, inv_std, grad_out):
    mean_grad = jnp.mean(grad_out, axis=-1, keepdims=True)
    mean_proj = jnp.mean(grad_out * normed, axis=-1, keepdims=True)
    return inv_std * (grad_out - mean_grad - normed * mean_proj)


def sigmoid(values):
    return 0.5 * jnp.tanh(0.5 * values) + 0.5


def swiglu_grad(hid_a, hid_b, grad_hidden):
    half_a = 0.5 * hid_a
    tanh_a = jnp.tanh(half_a)
    sig_a = 0.5 * tanh_a + 0.5
    silu_a = half_a * tanh_a + half_a
    grad_a = (grad_hidden * hid_b) * (sig_a + silu_a * (1.0 - sig_a))
    return silu_a * hid_b, grad_a, grad_hidden * silu_a


def put_at(grads, base, value):
    per_col = value.shape[0] // 16
    for col in range(value.shape[1] // 128):
        start = base + col * per_col
        grads[start:start + per_col] = value[:, col * 128:(col + 1) * 128].reshape(per_col, 16, 128).astype(BF)


def put_tiles(grads, name, value):
    put_at(grads, SLOTS[name][0], value)


class Reducer:
    def __init__(self, chunk, grads, total, got, send_sem, recv_sem, place):
        self.chunk = chunk
        self.grads, self.total, self.got = grads, total, got
        self.send_sem, self.recv_sem = send_sem, recv_sem
        self.place = place
        self.levels = LEVELS[CHUNK_KINDS[chunk]]
        self.sizes = level_sizes(chunk)
        self.depth = len(self.levels[0])

    def kept(self, part, level):
        at = CHUNKS[self.chunk][0] + part * self.sizes[0]
        for name, size in zip(self.levels[part][:level], self.sizes[1:]):
            at = at + self.place['index'][name] * size
        return at

    def held(self, part, level, start, count):
        if level == 0:
            return self.grads.at[pl.ds(self.kept(part, 0) + start, count)]
        return self.got[level - 1].at[part, 0, pl.ds(start, count)]

    def start(self, step):
        level = min(step, 2 * self.depth - 1 - step)
        size = self.sizes[level + 1]
        for part in range(len(self.levels)):
            name = self.levels[part][level]
            group = GROUP[name]
            for hop in range(1, group):
                other = lax.rem(self.place['index'][name] + hop, group)
                if step < self.depth:
                    src, dst = self.held(part, level, other * size, size), self.got[level].at[part, hop - 1]
                else:
                    src = dst = self.total.at[pl.ds(self.kept(part, level + 1), size)]
                pltpu.make_async_remote_copy(
                    src_ref=src, dst_ref=dst, send_sem=self.send_sem, recv_sem=self.recv_sem.at[step],
                    device_id=self.place['peer'](name, other), device_id_type=MESH_ID).start()

    def moved(self, level):
        return len(self.levels) * (GROUP[self.levels[0][level]] - 1) * self.sizes[level + 1]

    def wait_tiles(self, count, sem):
        span = self.grads.at[pl.ds(0, count)]
        pltpu.make_async_copy(span, span, sem).wait()

    def add(self, level):
        size = self.sizes[level + 1]
        for part in range(len(self.levels)):
            name = self.levels[part][level]
            own = self.held(part, level, self.place['index'][name] * size, size)
            slots = [self.got[level].at[part, hop] for hop in range(GROUP[name] - 1)]
            dst = slots[0] if level + 1 < self.depth else self.total.at[pl.ds(self.kept(part, level + 1), size)]
            add_into(dst, [own] + slots, size)

    def step(self, step):
        if step:
            level = min(step - 1, 2 * self.depth - step)
            self.wait_tiles(self.moved(level), self.recv_sem.at[step - 1])
        if 0 < step <= self.depth:
            self.add(step - 1)
        if step < 2 * self.depth:
            self.start(step)

    def finish_sends(self):
        self.wait_tiles(2 * sum(self.moved(level) for level in range(self.depth)), self.send_sem)


def add_into(dst, terms, count):
    step = math.gcd(count, 8)

    @pl.loop(0, count // step)
    def _(index):
        at = pl.ds(index * step, step)
        total = terms[0][at].astype(F32)
        for term in terms[1:]:
            total = total + term[at].astype(F32)
        dst[at] = total.astype(BF)


def main_kernel(*refs):
    names = ('pair_z', 'single_s', 'token_mask', 'dz_out', 'ds_out', 'w_pa', 'w_pb', 'w_po', 'w_bias', 'w_q', 'q_bias',
             'w_kv', 'w_g', 'w_o', 'w_sa', 'w_sb', 'w_so')
    hbm = dict(zip(names, refs[:17]))
    dz_in, ds_in, total = refs[17:20]
    scratch = refs[20:]
    loaded = dict(zip(names, scratch[:17]))
    (new_rows, bias_rows, grad_bias, kv_buf, gkv_buf, gkv_got1, gkv_got2, gkv_s, acc_ab, acc_po, acc_bias, gab_s, act_s, norm_s, gq_s, ggp_s,
     gmid_s, inv_s, prob_s, qexp_s, grads) = scratch[17:38]
    got_refs = list(scratch[38:38 + GOT_COUNT])
    load_sem, kv_send, kv_recv, gkv_send, gkv_recv, ar_send, ar_recv = scratch[38 + GOT_COUNT:]

    order = ('single_s', 'w_kv', 'pair_z', 'w_pa', 'w_pb', 'w_po', 'w_bias', 'w_q', 'q_bias', 'w_g', 'token_mask', 'w_o', 'w_sa',
             'w_sb', 'ds_out', 'w_so', 'dz_out')
    loads = {}
    for index, name in enumerate(order):
        loads[name] = pltpu.make_async_copy(hbm[name], loaded[name], load_sem.at[index])
        loads[name].start()

    my_z = lax.axis_index('dap')
    my_dp = lax.axis_index('dp')
    core = lax.rem(my_dp, 2)
    bit_x = lax.rem(lax.div(my_dp, 2), 2)
    bit_y = lax.div(my_dp, 4)

    def z_peer(other):
        return (other, my_dp)

    def peer(name, other):
        if name == 'core':
            return my_z, my_dp + other - core
        if name == 'x':
            return my_z, my_dp + 2 * (other - bit_x)
        if name == 'y':
            return my_z, my_dp + 4 * (other - bit_y)
        if name == 'xy':
            return my_z, 2 * other + core
        if name == 'z':
            return other, my_dp
        low = lax.rem(my_z, 2)
        return (my_z - low + other if name == 'z0' else 2 * other + low), my_dp

    place = {'peer': peer, 'index': {
        'core': core, 'x': bit_x, 'y': bit_y, 'xy': 2 * bit_y + bit_x, 'z': my_z, 'z0': lax.rem(my_z, 2), 'z1': lax.div(my_z, 2)}}

    barrier = pltpu.get_barrier_semaphore()
    for name in ('core', 'xy', 'z'):
        for hop in range(1, GROUP[name]):
            device = peer(name, lax.rem(place['index'][name] + hop, GROUP[name]))
            pl.semaphore_signal(barrier, inc=1, device_id=device, device_id_type=MESH_ID)

    loads['single_s'].wait()
    loads['w_kv'].wait()
    s_wide = loaded['single_s'][...].astype(F32).reshape(ALL_ROWS, WIDTH)
    s_norm, s_inv = layer_norm(s_wide)
    act = s_norm.astype(BF)
    act_s[...] = act
    norm_s[...] = s_norm
    inv_s[...] = s_inv
    kv_local = dot_nn(act, loaded['w_kv'][...])
    pl.semaphore_wait(barrier, 7)
    kv_buf[my_z] = kv_local.reshape(CPLX, ROWS, 2 * WIDTH).astype(BF)

    def kv_copy(hop):
        return pltpu.make_async_remote_copy(
            src_ref=kv_buf.at[my_z], dst_ref=kv_buf.at[my_z], send_sem=kv_send.at[hop - 1], recv_sem=kv_recv.at[hop - 1],
            device_id=z_peer(lax.rem(my_z + hop, PEERS)), device_id_type=MESH_ID)

    for hop in range(1, PEERS):
        kv_copy(hop).start()

    for name in ('pair_z', 'w_pa', 'w_pb', 'w_po', 'w_bias'):
        loads[name].wait()
    block_rows = BLOCK_I * TOKENS
    fwd_rows = FWD_BLOCK_I * TOKENS

    @pl.loop(0, ALL_ROWS // FWD_BLOCK_I)
    def _(block):
        at = block * FWD_BLOCK_I
        z_wide = loaded['pair_z'][pl.ds(at, FWD_BLOCK_I)].reshape(fwd_rows, PAIR).astype(F32)
        normed, _ = layer_norm(z_wide)
        normed_bf = normed.astype(BF)
        half_a = 0.5 * dot_nn(normed_bf, loaded['w_pa'][...])
        hid_b = dot_nn(normed_bf, loaded['w_pb'][...])
        hidden = ((half_a * jnp.tanh(half_a) + half_a) * hid_b).astype(BF)
        z_new = (z_wide + dot_nn(hidden, loaded['w_po'][...])).astype(BF)
        new_rows[pl.ds(at, FWD_BLOCK_I)] = z_new.reshape(FWD_BLOCK_I, TOKENS, PAIR)
        bias_norm, _ = layer_norm(z_new.astype(F32))
        bias_bf = bias_norm.astype(BF)
        for row in range(FWD_BLOCK_I):
            bias_rows[at + row] = dot_nt(loaded['w_bias'][...], bias_bf[row * TOKENS:(row + 1) * TOKENS])

    for name in ('w_q', 'q_bias', 'w_g', 'token_mask', 'w_o', 'w_sa', 'w_sb', 'ds_out', 'w_so'):
        loads[name].wait()
    queries = (dot_nn(act_s[...], loaded['w_q'][...]) + loaded['q_bias'][...].astype(F32).reshape(1, WIDTH)).astype(BF).astype(F32)
    gate = sigmoid(dot_nn(act_s[...], loaded['w_g'][...]))
    lane_head = lax.broadcasted_iota(jnp.int32, (HEADS, WIDTH), 1)
    row_head = lax.broadcasted_iota(jnp.int32, (HEADS, WIDTH), 0)
    head_mask = jnp.where((lane_head >= row_head * HEAD_DIM) & (lane_head < (row_head + 1) * HEAD_DIM), 1.0, 0.0).astype(F32)

    def spread(rows):
        wide = jnp.broadcast_to(rows.reshape(ROWS, 1, WIDTH), (ROWS, HEADS, WIDTH)) * head_mask[None]
        return wide.reshape(ROWS * HEADS, WIDTH).astype(BF)

    def gather_heads(wide):
        return jnp.sum(wide.reshape(ROWS, HEADS, WIDTH) * head_mask[None], axis=1)

    for hop in range(1, PEERS):
        kv_copy(hop).wait()

    def keys_values(cplx):
        both = kv_buf[:, cplx].astype(F32).reshape(TOKENS, 2 * WIDTH).astype(BF)
        return both[:, :WIDTH], both[:, WIDTH:]

    key_mask = MASK_BIG * (loaded['token_mask'][...].astype(F32) - 1.0)
    attended_parts = []
    for cplx in range(CPLX):
        keys, values = keys_values(cplx)
        q_exp = spread(queries[cplx * ROWS:(cplx + 1) * ROWS])
        qexp_s[cplx] = q_exp
        bias = bias_rows[cplx * ROWS:(cplx + 1) * ROWS].reshape(ROWS * HEADS, TOKENS)
        logits = dot_nt(q_exp, keys) * SCALE + bias + key_mask[cplx:cplx + 1]
        top = jnp.max(logits, axis=-1, keepdims=True)
        expd = jnp.exp(logits - top)
        prob = expd / jnp.sum(expd, axis=-1, keepdims=True)
        prob_s[cplx] = prob
        attended_parts.append(gather_heads(dot_nn(prob.astype(BF), values)))
    attended = jnp.concatenate(attended_parts, axis=0)
    gated = (gate * attended).astype(BF)
    s_mid = (s_wide + dot_nn(gated, loaded['w_o'][...])).astype(BF)
    mid_norm, mid_inv = layer_norm(s_mid.astype(F32))
    mid_act = mid_norm.astype(BF)

    reducers = []
    for index in range(len(CHUNKS)):
        depth = len(LEVELS[CHUNK_KINDS[index]][0])
        reducers.append(Reducer(index, grads, total, got_refs[:depth], ar_send.at[index], ar_recv.at[index], place))
        del got_refs[:depth]

    def act_on(number):
        for chunk, step in ACTIONS[number]:
            if chunk < 0:
                (forward_kv_grad, finish_kv_grad)[step]()
            else:
                reducers[chunk].step(step)

    ds_wide = loaded['ds_out'][...].astype(F32).reshape(ALL_ROWS, WIDTH)
    ds_bf = ds_wide.astype(BF)
    grad_mid_norm = jnp.zeros((ALL_ROWS, WIDTH), F32)
    for piece in range(TRANS_S // PIECE):
        cols = slice(piece * PIECE, (piece + 1) * PIECE)
        base = piece * PIECE_TILES
        trans_a = dot_nn(mid_act, loaded['w_sa'][:, cols])
        trans_b = dot_nn(mid_act, loaded['w_sb'][:, cols])
        grad_hidden = dot_nt(ds_bf, loaded['w_so'][cols, :])
        hidden, grad_ta, grad_tb = swiglu_grad(trans_a, trans_b, grad_hidden)
        grad_ta = grad_ta.astype(BF)
        grad_tb = grad_tb.astype(BF)
        put_at(grads, base, dot_tn(hidden.astype(BF), ds_bf))
        put_at(grads, base + PIECE_TILES // 3, dot_tn(mid_act, grad_ta))
        put_at(grads, base + 2 * (PIECE_TILES // 3), dot_tn(mid_act, grad_tb))
        act_on(piece + 1)
        grad_mid_norm = grad_mid_norm + dot_nt(grad_ta, loaded['w_sa'][:, cols]) + dot_nt(grad_tb, loaded['w_sb'][:, cols])
    grad_mid = ds_wide + norm_grad(mid_norm, mid_inv, grad_mid_norm)
    gmid_s[...] = grad_mid
    grad_mid_bf = grad_mid.astype(BF)
    put_tiles(grads, 'o', dot_tn(gated, grad_mid_bf))
    grad_gated = dot_nt(grad_mid_bf, loaded['w_o'][...])
    grad_gate_pre = (grad_gated * attended * gate * (1.0 - gate)).astype(BF)
    ggp_s[...] = grad_gate_pre
    grad_att = (grad_gated * gate).astype(BF).astype(F32)
    grad_query_parts = []
    for cplx in range(CPLX):
        keys, values = keys_values(cplx)
        ga_exp = spread(grad_att[cplx * ROWS:(cplx + 1) * ROWS])
        prob = prob_s[cplx]
        grad_prob = dot_nt(ga_exp, values)
        grad_values = dot_tn(prob.astype(BF), ga_exp)
        grad_logits = (prob * (grad_prob - jnp.sum(prob * grad_prob, axis=-1, keepdims=True))).astype(BF)
        grad_bias[cplx * ROWS:(cplx + 1) * ROWS] = grad_logits.reshape(ROWS, HEADS, TOKENS)
        grad_query_parts.append(gather_heads(dot_nn(grad_logits, keys)) * SCALE)
        grad_keys = dot_tn(grad_logits, qexp_s[cplx]) * SCALE
        grad_keys = grad_keys.reshape(PEERS, ROWS, WIDTH).astype(BF)
        grad_values = grad_values.reshape(PEERS, ROWS, WIDTH).astype(BF)
        for owner in range(PEERS):
            gkv_buf[owner % 2, owner // 2, cplx, :, :WIDTH] = grad_keys[owner]
            gkv_buf[owner % 2, owner // 2, cplx, :, WIDTH:] = grad_values[owner]

    low, high = place['index']['z0'], place['index']['z1']

    def gkv_copy(step):
        src, dst = ((gkv_buf.at[1 - low], gkv_got1), (gkv_got1.at[1 - high], gkv_got2))[step]
        return pltpu.make_async_remote_copy(
            src_ref=src, dst_ref=dst, send_sem=gkv_send.at[step], recv_sem=gkv_recv.at[step],
            device_id=peer(*(('z0', 1 - low), ('z1', 1 - high))[step]), device_id_type=MESH_ID)

    gkv_copy(0).start()
    act_on(4)
    grad_query = jnp.concatenate(grad_query_parts, axis=0)
    grad_query_bf = grad_query.astype(BF)
    gq_s[...] = grad_query_bf
    put_tiles(grads, 'q', dot_tn(act_s[...], grad_query_bf))
    put_tiles(grads, 'g', dot_tn(act_s[...], grad_gate_pre))
    d_q_bias = jnp.sum(grad_query, axis=0, keepdims=True)
    row_index = lax.broadcasted_iota(jnp.int32, (16, 128), 0)
    bias_tile = jnp.zeros((16, 128), F32)
    for sub in range(3):
        bias_tile = jnp.where(row_index == sub, jnp.broadcast_to(d_q_bias[:, sub * 128:(sub + 1) * 128], (16, 128)), bias_tile)
    grads[1080] = bias_tile.astype(BF)
    grads[1081:1088] = jnp.zeros((7, 16, 128), BF)
    grads[1233:1280] = jnp.zeros((47, 16, 128), BF)

    def forward_kv_grad():
        gkv_copy(0).wait()
        gkv_got1[...] = (gkv_got1[...].astype(F32) + gkv_buf[low].astype(F32)).astype(BF)
        gkv_copy(1).start()

    def finish_kv_grad():
        gkv_copy(1).wait()
        summed = gkv_got1[high].astype(F32) + gkv_got2[...].astype(F32)
        grad_kv = summed.reshape(ALL_ROWS, 2 * WIDTH).astype(BF)
        gkv_s[...] = grad_kv
        put_tiles(grads, 'kv', dot_tn(act_s[...], grad_kv))

    def finish_single():
        grad_act = (dot_nt(gq_s[...], loaded['w_q'][...]) + dot_nt(gkv_s[...], loaded['w_kv'][...])
                    + dot_nt(ggp_s[...], loaded['w_g'][...]))
        grad_s = gmid_s[...] + norm_grad(norm_s[...], inv_s[...], grad_act)
        ds_in[...] = grad_s.reshape(CPLX, ROWS, WIDTH).astype(BF)

    loads['dz_out'].wait()
    acc_ab[...] = jnp.zeros_like(acc_ab)
    acc_po[...] = jnp.zeros_like(acc_po)
    acc_bias[...] = jnp.zeros_like(acc_bias)

    def act_in_loop(block, first):
        for tick in range(NUM_BLOCKS):
            if ACTIONS[first + tick]:
                @pl.when(block == tick)
                def _():
                    act_on(first + tick)

    @pl.loop(0, NUM_BLOCKS)
    def _(block):
        act_in_loop(block, FIRST_BLOCK)
        at = block * BLOCK_I
        bias_norm, bias_inv = layer_norm(new_rows[pl.ds(at, BLOCK_I)].reshape(block_rows, PAIR).astype(F32))
        bias_bf = bias_norm.astype(BF)
        bias_acc = acc_bias[...]
        parts = []
        for row in range(BLOCK_I):
            grad_row = grad_bias[at + row]
            bias_acc = bias_acc + dot_nn(grad_row, bias_bf[row * TOKENS:(row + 1) * TOKENS])
            parts.append(dot_tn(grad_row, loaded['w_bias'][...]))
        acc_bias[...] = bias_acc
        grad_norm = jnp.concatenate(parts, axis=0)
        dz_wide = loaded['dz_out'][pl.ds(at, BLOCK_I)].reshape(block_rows, PAIR).astype(F32)
        grad_new_bf = (dz_wide + norm_grad(bias_norm, bias_inv, grad_norm)).astype(BF)
        new_rows[pl.ds(at, BLOCK_I)] = grad_new_bf.reshape(BLOCK_I, TOKENS, PAIR)

    grads[SLOTS['bias'][0]] = acc_bias[...].astype(BF)

    @pl.loop(0, NUM_BLOCKS)
    def _(block):
        act_in_loop(block, MAIN_BLOCK)
        at = block * BLOCK_I
        grad_new_bf = new_rows[pl.ds(at, BLOCK_I)].reshape(block_rows, PAIR)
        normed, _ = layer_norm(loaded['pair_z'][pl.ds(at, BLOCK_I)].reshape(block_rows, PAIR).astype(F32))
        normed_bf = normed.astype(BF)
        hid_a = dot_nn(normed_bf, loaded['w_pa'][...])
        hid_b = dot_nn(normed_bf, loaded['w_pb'][...])
        grad_hidden = dot_nt(grad_new_bf, loaded['w_po'][...])
        hidden, grad_a, grad_b = swiglu_grad(hid_a, hid_b, grad_hidden)
        grad_a = grad_a.astype(BF)
        grad_b = grad_b.astype(BF)
        gab_s[block, :, :TRANS_P] = grad_a
        gab_s[block, :, TRANS_P:] = grad_b
        acc_po[...] += dot_tn(grad_new_bf, hidden.astype(BF))
        acc_ab[:, :TRANS_P] += dot_tn(normed_bf, grad_a)
        acc_ab[:, TRANS_P:] += dot_tn(normed_bf, grad_b)

    put_tiles(grads, 'pa', acc_ab[:, :TRANS_P])
    put_tiles(grads, 'pb', acc_ab[:, TRANS_P:])
    put_tiles(grads, 'po', jnp.transpose(acc_po[...]))
    act_on(SINGLE_END)
    finish_single()

    @pl.loop(0, NUM_BLOCKS)
    def _(block):
        act_in_loop(block, DZ_BLOCK)
        at = block * BLOCK_I
        normed, inv_std = layer_norm(loaded['pair_z'][pl.ds(at, BLOCK_I)].reshape(block_rows, PAIR).astype(F32))
        grad_normed = dot_nt(gab_s[block, :, :TRANS_P], loaded['w_pa'][...]) + dot_nt(gab_s[block, :, TRANS_P:], loaded['w_pb'][...])
        grad_new = new_rows[pl.ds(at, BLOCK_I)].reshape(block_rows, PAIR).astype(F32)
        result = grad_new + norm_grad(normed, inv_std, grad_normed)
        dz_in[pl.ds(at, BLOCK_I)] = result.reshape(BLOCK_I, TOKENS, PAIR).astype(BF)

    act_on(DZ_BLOCK + NUM_BLOCKS)
    for reducer in reducers:
        reducer.finish_sends()


GOT_COUNT = sum(len(LEVELS[kind][0]) for kind in CHUNK_KINDS)
MAX_STEPS = 2 * max(len(LEVELS[kind][0]) for kind in CHUNK_KINDS)


def run_main(inputs):
    any_spec = pl.BlockSpec(memory_space=pl.ANY)
    scratch = [pltpu.VMEM(value.shape, value.dtype) for value in inputs]
    scratch += [
        pltpu.VMEM((ALL_ROWS, TOKENS, PAIR), BF),
        pltpu.VMEM((ALL_ROWS, HEADS, TOKENS), F32),
        pltpu.VMEM((ALL_ROWS, HEADS, TOKENS), BF),
        pltpu.VMEM((PEERS, CPLX, ROWS, 2 * WIDTH), BF),
        pltpu.VMEM((2, 2, CPLX, ROWS, 2 * WIDTH), BF),
        pltpu.VMEM((2, CPLX, ROWS, 2 * WIDTH), BF),
        pltpu.VMEM((CPLX, ROWS, 2 * WIDTH), BF),
        pltpu.VMEM((ALL_ROWS, 2 * WIDTH), BF),
        pltpu.VMEM((PAIR, 2 * TRANS_P), F32),
        pltpu.VMEM((PAIR, TRANS_P), F32),
        pltpu.VMEM((HEADS, PAIR), F32),
        pltpu.VMEM((NUM_BLOCKS, BLOCK_I * TOKENS, 2 * TRANS_P), BF),
        pltpu.VMEM((ALL_ROWS, WIDTH), BF),
        pltpu.VMEM((ALL_ROWS, WIDTH), F32),
        pltpu.VMEM((ALL_ROWS, WIDTH), BF),
        pltpu.VMEM((ALL_ROWS, WIDTH), BF),
        pltpu.VMEM((ALL_ROWS, WIDTH), F32),
        pltpu.VMEM((ALL_ROWS, 1), F32),
        pltpu.VMEM((CPLX, ROWS * HEADS, TOKENS), F32),
        pltpu.VMEM((CPLX, ROWS * HEADS, WIDTH), BF),
        pltpu.VMEM((TILES, 16, 128), BF),
    ]
    for chunk, kind in enumerate(CHUNK_KINDS):
        for name, size in zip(LEVELS[kind][0], level_sizes(chunk)[1:]):
            scratch.append(pltpu.VMEM((len(LEVELS[kind]), GROUP[name] - 1, size, 16, 128), BF))
    dma = pltpu.SemaphoreType.DMA
    scratch += [dma((17,)), dma((3,)), dma((3,)), dma((2,)), dma((2,)), dma((len(CHUNKS),)), dma((len(CHUNKS), MAX_STEPS))]
    return pl.pallas_call(
        main_kernel,
        out_shape=(pltpu.VMEM((ALL_ROWS, TOKENS, PAIR), BF), pltpu.VMEM((CPLX, ROWS, WIDTH), BF), pltpu.VMEM((TILES, 16, 128), BF)),
        in_specs=[any_spec] * 17,
        out_specs=(pl.BlockSpec(memory_space=pltpu.VMEM),) * 3,
        scratch_shapes=scratch,
        compiler_params=pltpu.CompilerParams(collective_id=0, has_side_effects=True, vmem_limit_bytes=48 * 1024 * 1024),
        name='pairformer_tail',
    )(*(pltpu.with_memory_space_constraint(value, pltpu.HBM) for value in inputs))


UNPACK = ('pa', 'pb', 'po', 'bias', 'q', 'qb', 'kv', 'g', 'o', 'sa', 'sb', 'so')


def unpack_kernel(tiles, dz_buf, ds_buf, *refs):
    outs = dict(zip(UNPACK, refs[:12]))
    dz_out, ds_out = refs[12:14]
    stages = dict(zip(UNPACK, refs[14:26]))
    sem, pass_sem = refs[26:]
    copies = []
    for index, (buf, dst) in enumerate(((dz_buf, dz_out), (ds_buf, ds_out))):
        made = pltpu.make_async_copy(buf, dst, pass_sem.at[index])
        made.start()
        copies.append(made)

    def widen(stage, base, rows, row, cols, col):
        per_col = rows // 16
        for sub in range(cols // 128):
            part = tiles[base + sub * per_col:base + (sub + 1) * per_col].astype(F32)
            stage[row:row + rows, col + sub * 128:col + (sub + 1) * 128] = part.reshape(rows, 128)

    def send(name):
        made = pltpu.make_async_copy(stages[name], outs[name], sem.at[UNPACK.index(name)])
        made.start()
        copies.append(made)

    for name in ('kv', 'o', 'q', 'g', 'pa', 'pb', 'po', 'bias', 'qb'):
        base, rows, cols = SLOTS[name]
        if name == 'qb':
            last_tile = tiles[base].astype(F32)
            for sub in range(3):
                stages[name][pl.ds(sub * 128, 128)] = last_tile[sub]
        else:
            widen(stages[name], base, rows, 0, cols, 0)
        send(name)
    for piece in range(TRANS_S // PIECE):
        base = piece * PIECE_TILES
        third = PIECE_TILES // 3
        widen(stages['so'], base, PIECE, piece * PIECE, WIDTH, 0)
        widen(stages['sa'], base + third, WIDTH, 0, PIECE, piece * PIECE)
        widen(stages['sb'], base + 2 * third, WIDTH, 0, PIECE, piece * PIECE)
    for name in ('so', 'sa', 'sb'):
        send(name)
    for copy in copies:
        copy.wait()


def run_unpack(tiles, dz_in, ds_in):
    shapes = [(WIDTH,) if name == 'qb' else (TRANS_S, WIDTH) if name == 'so' else (WIDTH, TRANS_S) if name in ('sa', 'sb')
              else SLOTS[name][1:] for name in UNPACK]
    any_spec = pl.BlockSpec(memory_space=pl.ANY)
    return pl.pallas_call(
        unpack_kernel,
        out_shape=tuple(jax.ShapeDtypeStruct(shape, F32) for shape in shapes) + (
            jax.ShapeDtypeStruct(dz_in.shape, BF), jax.ShapeDtypeStruct(ds_in.shape, BF)),
        in_specs=[pl.BlockSpec(memory_space=pltpu.VMEM)] * 3,
        out_specs=(any_spec,) * 14,
        scratch_shapes=[pltpu.VMEM(shape, F32) for shape in shapes] + [
            pltpu.SemaphoreType.DMA((12,)), pltpu.SemaphoreType.DMA((2,))],
        compiler_params=pltpu.CompilerParams(vmem_limit_bytes=24 * 1024 * 1024),
        name='unpack_sums',
    )(*(pltpu.with_memory_space_constraint(value, pltpu.VMEM) for value in (tiles, dz_in, ds_in)))


def solution(mesh):
    pair_spec = P('dp', 'dap', None, None)
    single_spec = P('dp', 'dap', None)

    def body(pair_z, single_s, token_mask, dz_out, ds_out, w_pa, w_pb, w_po, w_bias, w_q, q_bias, w_kv, w_g, w_o, w_sa, w_sb, w_so):
        inputs = (pair_z.reshape(ALL_ROWS, TOKENS, PAIR), single_s, token_mask, dz_out.reshape(ALL_ROWS, TOKENS, PAIR), ds_out,
                  w_pa, w_pb, w_po, w_bias.T, w_q, q_bias, w_kv, w_g, w_o, w_sa, w_sb, w_so)
        dz_in, ds_in, tiles = run_main(inputs)
        *sums, dz_in, ds_in = run_unpack(tiles, dz_in, ds_in)
        sums[3] = sums[3].T
        return (dz_in.reshape(pair_z.shape), ds_in) + tuple(sums)

    in_specs = (pair_spec, single_spec, P('dp', None), pair_spec, single_spec) + (P(),) * 12
    out_specs = (pair_spec, single_spec) + (P(),) * 12
    return jax.shard_map(body, mesh=mesh, in_specs=in_specs, out_specs=out_specs, check_vma=False)
```
